32 devices in a mesh: asset: 8 (over z, y), tm: 4 (over x, core).
Axes of the slice: x: 2, y: 2, z: 4, core: 2. Of those that a mesh axis runs over, the one named last changes fastest.
Arguments:
- values: float32 [4, 1024, 16384], P(None, 'tm', 'asset'), may hold values from -64 to 64
- listed_from: int32 [16384], P('asset'), may hold values from -1024 to 1023, as said below
- listed_until: int32 [16384], P('asset'), may hold values from -960 to 3070, as said below
Outputs:
- standardized: float32 [4, 1024, 16384], P(None, 'tm', 'asset')
The draws below stay inside these ranges and needn't reach their ends.
Inputs may be any that keep to these rules, and one draw needn't show every extreme that they name: listed_until[a] - listed_from[a] is at least 64. listed_until[a] - listed_from[a] is at least 64.
All inputs are finite; a program needn't handle non-finite values.
Results may differ from the reference program's by a relative error of at most 0.00005.
Values sent between devices are 32-bit elements; how exact they have to be, the bound alone decides.
A program may use at most 128 MiB of HBM per device.

```python
import jax
import jax.numpy as jnp
from jax import lax

F = 4
WINDOW = 64
TIME = 1024
ASSETS = 16384


def listing_dates(key):
    base = jax.random.fold_in(key, 7)
    key_start, key_length = jax.random.split(base)
    first_stamp = jax.random.randint(key_start, (ASSETS,), -TIME, TIME, dtype=jnp.int32)
    length = jax.random.randint(key_length, (ASSETS,), WINDOW, 2 * TIME, dtype=jnp.int32)
    return (first_stamp, first_stamp + length)


def draw_listed_from(key, part):
    return listing_dates(key)[0]


def draw_listed_until(key, part):
    return listing_dates(key)[1]


def draw_values(key, part):
    base = jax.random.fold_in(key, 11)
    key_noise, key_scale, key_common, key_drift = jax.random.split(base, 4)
    noise_draw = jax.random.normal(key_noise, (F, TIME, ASSETS), jnp.float32)
    field_values = 8.0 * noise_draw
    return jnp.clip(field_values, -64.0, 64.0)


def setup_inputs(seed: int = 0) -> dict:
    arg_keys = jax.random.split(jax.random.key(seed), 4)
    values = draw_values(jax.random.fold_in(arg_keys[3], 71), 0)
    listed_from = draw_listed_from(jax.random.fold_in(arg_keys[3], 71), 0)
    listed_until = draw_listed_until(jax.random.fold_in(arg_keys[3], 71), 0)
    return {"values": values, "listed_from": listed_from, "listed_until": listed_until}


def standardize(field_values, weight, present):
    center = lax.optimization_barrier(jnp.sum(weight * field_values, axis=1)) / present
    deviate = (field_values - center[:, None]) * weight
    spread = lax.optimization_barrier(jnp.sum(deviate * deviate, axis=1)) / present
    return deviate / jnp.sqrt(spread + 0.1)[:, None]

def reference(values, listed_from, listed_until):
    stamps = jnp.arange(TIME, dtype=jnp.int32)[:, None]
    opened = listed_from[None, :]
    closed = listed_until[None, :]
    weight = ((stamps >= opened) & (stamps < closed)).astype(values.dtype)
    window_low = jnp.maximum(jnp.maximum(stamps - (WINDOW - 1), opened), 0)
    window_high = jnp.minimum(stamps, closed - 1)
    counted = jnp.maximum(window_high - window_low + 1, 1).astype(values.dtype)
    present = jnp.maximum(lax.optimization_barrier(jnp.sum(weight, axis=1)), 1.0)

    def one_field(field_values):
        window_sum = lax.reduce_window(field_values * weight, jnp.zeros((), field_values.dtype), lax.add, (WINDOW, 1), (1, 1), ((WINDOW - 1, 0), (0, 0)))
        rolling = window_sum / counted
        clipped = jnp.clip(standardize(rolling, weight, present), -3.0, 3.0)
        return standardize(clipped, weight, present)
    return lax.map(one_field, values)
```

```python
import functools

import jax
import jax.numpy as jnp
from jax import lax
from jax.experimental import pallas as pl
from jax.experimental.pallas import tpu as pltpu
from jax.sharding import PartitionSpec as P

WINDOW = 64
LANES = 128
CLIP = 3.0
UNROLL = 4
PIECES = 4
HELD = 2


def field_groups(fields):
    half = (fields + 1) // 2
    return [(start, min(half, fields - start)) for start in range(0, fields, half)]


def halo_pieces(fields, chunks):
    cuts = PIECES if chunks % PIECES == 0 else 1
    whole = [(f, 0, chunks) for f in range(fields - 1)]
    size = chunks // cuts
    return whole + [(fields - 1, c * size, size) for c in range(cuts)]


def kernel(
    n_tm, n_as, values, opened_hbm, closed_hbm, out,
    x, rolling, weight, inverse, opened_ref, closed_ref, part, got, totals, advice, advised,
    load_sem, halo_send, halo_recv, back_send, back_recv, advice_sem, send_sem, recv_sem,
):
    fields, rows, assets = values.shape
    blocks = rows // WINDOW
    chunks = assets // LANES
    groups = field_groups(fields)
    own = groups[0][1]
    helped = fields - own
    tm = lax.axis_index("tm")
    me = lax.axis_index("asset")
    later = lax.rem(tm + 1, n_tm)
    before = lax.rem(tm + n_tm - 1, n_tm)
    has_next = tm < n_tm - 1
    has_prev = tm > 0

    dates = [
        pltpu.make_async_copy(opened_hbm, opened_ref, load_sem.at[fields]),
        pltpu.make_async_copy(closed_hbm, closed_ref, load_sem.at[fields + 1]),
    ]
    loads = [
        pltpu.make_async_copy(values.at[f], x.at[f, pl.ds(WINDOW, rows)], load_sem.at[f])
        for f in range(fields)
    ]

    barrier = pltpu.get_barrier_semaphore()
    for other in (later, before):
        pl.semaphore_signal(barrier, inc=1, device_id={"tm": other})
    for d in range(1, n_as):
        pl.semaphore_signal(barrier, inc=1, device_id={"asset": lax.rem(me + d, n_as)})
    for copy in dates + loads:
        copy.start()
    pl.semaphore_wait(barrier, n_as + 1)

    pieces = halo_pieces(fields, chunks)
    halos = []
    for i, (f, first, size) in enumerate(pieces):
        cols = pl.ds(first * LANES, size * LANES)
        halos.append(pltpu.make_async_remote_copy(
            src_ref=values.at[f, pl.ds(rows - WINDOW, WINDOW), cols],
            dst_ref=x.at[f, pl.ds(0, WINDOW), cols],
            send_sem=halo_send.at[i],
            recv_sem=halo_recv.at[i],
            device_id={"tm": later},
        ))
    backs = [
        pltpu.make_async_remote_copy(
            src_ref=values.at[f, pl.ds(0, WINDOW)],
            dst_ref=x.at[f, pl.ds(WINDOW + rows, WINDOW)],
            send_sem=back_send.at[f - own],
            recv_sem=back_recv.at[f - own],
            device_id={"tm": before},
        )
        for f in range(own, fields)
    ]
    advising = pltpu.make_async_remote_copy(
        src_ref=advice,
        dst_ref=advised,
        send_sem=advice_sem.at[0],
        recv_sem=advice_sem.at[1],
        device_id={"tm": later},
    )
    free = len(halos) - min(HELD, len(halos) - (fields - 1))

    @pl.when(has_next)
    def _():
        for copy in halos[:free]:
            copy.start()

    @pl.when(has_prev)
    def _():
        for copy in backs:
            copy.start()

    def send(slot):
        for d in range(1, n_as):
            pltpu.make_async_remote_copy(
                src_ref=part.at[slot],
                dst_ref=got.at[slot, d - 1],
                send_sem=send_sem.at[slot],
                recv_sem=recv_sem.at[slot],
                device_id={"asset": lax.rem(me + d, n_as)},
            ).start()

    def receive(slot):
        arrived = got.at[slot]
        pltpu.make_async_copy(arrived, arrived, recv_sem.at[slot]).wait()
        totals[slot] = part[slot] + jnp.sum(got[slot], axis=0)

    def row_of(first, second):
        return jnp.sum(jnp.concatenate([first, second], axis=0).T, axis=0, keepdims=True)

    def factors(row, count):
        mean = row / jnp.maximum(count, 1.0)
        other = pltpu.roll(mean, WINDOW, 1)
        scale = 1.0 / jnp.sqrt(jnp.maximum(mean - other * other, 0.0) + 0.1)
        lane = lax.broadcasted_iota(jnp.int32, row.shape, 1)
        both = jnp.broadcast_to(jnp.where(lane < WINDOW, mean, scale), (LANES, LANES)).T
        return both[:WINDOW], both[WINDOW:]

    def columns(c):
        return pl.ds(pl.multiple_of(c * LANES, LANES), LANES)

    zero = jnp.zeros((WINDOW, LANES), jnp.float32)
    part[...] = jnp.zeros(part.shape, part.dtype)
    first_stamp = tm * rows - WINDOW
    for copy in dates:
        copy.wait()

    @pl.when(tm == 0)
    def _():
        @pl.loop(0, fields)
        def clear(f):
            x[f, pl.ds(0, WINDOW), :] = jnp.zeros((WINDOW, assets), jnp.float32)

    @pl.loop(0, blocks + 2)
    def listing(b):
        start = pl.multiple_of(b * WINDOW, WINDOW)
        stamps = first_stamp + start + lax.broadcasted_iota(jnp.int32, (WINDOW, LANES), 0)

        def chunk(c, total):
            cols = columns(c)
            opened = jnp.maximum(opened_ref[:, cols], 0)
            closed = closed_ref[:, cols]
            listed = (stamps >= opened) & (stamps < closed)
            low = jnp.maximum(stamps - (WINDOW - 1), opened)
            counted = jnp.maximum(jnp.minimum(stamps + 1, closed) - low, 1).astype(jnp.float32)
            ones = jnp.where(listed, 1.0, 0.0)
            weight[pl.ds(start, WINDOW), cols] = ones
            inverse[pl.ds(start, WINDOW), cols] = ones / counted
            return total + ones

        total = lax.fori_loop(0, chunks, chunk, zero, unroll=2)
        part[0, pl.ds(lax.rem(b + blocks + 1, blocks + 2), 1), :] = row_of(total, total)

    send(0)

    def window_means(f, b, c):
        top = pl.multiple_of(b * WINDOW, WINDOW)
        cols = columns(c)
        reach = pl.ds(top, 2 * WINDOW)
        sums = x[f, reach, cols] * weight[reach, cols]
        for step in (8, 16, 32):
            sums = sums[step:] + sums[:-step]
        for step in (1, 2, 4):
            sums = sums + pltpu.roll(sums, step, 0)
        return sums[8:] * inverse[pl.ds(top + WINDOW, WINDOW), cols]

    def roll_window(f, b):
        top = pl.multiple_of(b * WINDOW, WINDOW)

        def chunk(c, carry):
            means = window_means(f, b, c)
            rolling[f, pl.ds(top, WINDOW), columns(c)] = means
            return carry[0] + means, carry[1] + means * means

        return row_of(*lax.fori_loop(0, chunks, chunk, (zero, zero), unroll=UNROLL))

    def clip_scores(f, b, center, scale):
        top = pl.multiple_of(b * WINDOW, WINDOW)

        def chunk(c, carry):
            cols = columns(c)
            scored = (rolling[f, pl.ds(top, WINDOW), cols] - center) * scale
            clipped = jnp.minimum(jnp.maximum(scored, -CLIP), CLIP)
            masked = clipped * weight[pl.ds(top + WINDOW, WINDOW), cols]
            return carry[0] + masked, carry[1] + masked * clipped

        return row_of(*lax.fori_loop(0, chunks, chunk, (zero, zero), unroll=UNROLL))

    def standardized(means, b, cols, first, second):
        center, scale = first
        middle, factor = second
        top = pl.multiple_of(b * WINDOW, WINDOW)
        clipped = jnp.minimum(jnp.maximum((means - center) * scale, -CLIP), CLIP)
        return (clipped - middle) * weight[pl.ds(top + WINDOW, WINDOW), cols] * factor

    def finish(f, b, first, second):
        here = pl.ds(pl.multiple_of(b * WINDOW, WINDOW), WINDOW)

        @pl.loop(0, chunks, unroll=UNROLL)
        def chunk(c):
            cols = columns(c)
            out[f, here, cols] = standardized(rolling[f, here, cols], b, cols, first, second)

    def roll_finish(f, low, size, first, second):
        @pl.loop(low, low + size, unroll=min(UNROLL, size))
        def chunk(c):
            cols = columns(c)
            out[f, :WINDOW, cols] = standardized(window_means(f, 0, c), 0, cols, first, second)

    def count_row(b):
        return totals[0, pl.ds(b, 1), :]

    def total_row(slot, i):
        return totals[slot, pl.ds(i, 1), :]

    def main_items(g):
        size = groups[g][1]
        return pl.loop(jnp.where(tm == 0, 0, size), size * blocks)

    def main_first(g):
        start, size = groups[g]
        for f in range(start, start + size):
            loads[f].wait()

        @main_items(g)
        def item(i):
            f, b = start + lax.rem(i, size), lax.div(i, size)
            part[1 + 2 * g, pl.ds(i, 1), :] = roll_window(f, b)

        send(1 + 2 * g)

    def main_second(g):
        start, size = groups[g]
        slot = 1 + 2 * g
        receive(slot)

        @main_items(g)
        def item(i):
            f, b = start + lax.rem(i, size), lax.div(i, size)
            center, scale = factors(total_row(slot, i), count_row(b))
            part[slot + 1, pl.ds(i, 1), :] = clip_scores(f, b, center, scale)

        send(slot + 1)

    def main_third(g):
        start, size = groups[g]
        slot = 1 + 2 * g
        receive(slot + 1)

        @main_items(g)
        def item(i):
            f, b = start + lax.rem(i, size), lax.div(i, size)
            count = count_row(b)
            first = factors(total_row(slot, i), count)
            finish(f, b, first, factors(total_row(slot + 1, i), count))

    tail_slot = 1 + 2 * len(groups)

    def tail_first(u):
        slot = tail_slot + 2 * u

        @pl.when(has_prev)
        def _():
            halos[u].wait_recv()
            part[slot, :1, :] = roll_window(u, 0)

        if u < helped:
            @pl.when(has_next)
            def _():
                backs[u].wait_recv()
                part[slot, 1:2, :] = roll_window(own + u, blocks)

        send(slot)

    def tail_second(u):
        slot = tail_slot + 2 * u
        receive(slot)

        @pl.when(has_prev)
        def _():
            center, scale = factors(total_row(slot, 0), count_row(0))
            part[slot + 1, :1, :] = clip_scores(u, 0, center, scale)

        if u < helped:
            @pl.when(has_next)
            def _():
                center, scale = factors(total_row(slot, 1), count_row(blocks))
                part[slot + 1, 1:2, :] = clip_scores(own + u, blocks, center, scale)

        send(slot + 1)

    def tail_third(u):
        slot = tail_slot + 2 * u
        receive(slot + 1)
        if u < helped:
            advice[2 * u:2 * u + 1, :] = total_row(slot, 1)
            advice[2 * u + 1:2 * u + 2, :] = total_row(slot + 1, 1)

    def tail_finish(u):
        slot = tail_slot + 2 * u

        @pl.when(has_prev)
        def _():
            first = factors(total_row(slot, 0), count_row(0))
            finish(u, 0, first, factors(total_row(slot + 1, 0), count_row(0)))

    for g in range(len(groups)):
        main_first(g)
    receive(0)
    for g in range(len(groups)):
        main_second(g)
    for g in range(len(groups)):
        main_third(g)
    for u in range(own):
        tail_first(u)
    for u in range(own):
        tail_second(u)
    for u in range(own):
        tail_third(u)

    @pl.when(has_next)
    def _():
        advising.start()
        for copy in halos[free:]:
            copy.start()

    for u in range(own):
        tail_finish(u)

    @pl.when(has_prev)
    def _():
        advising.wait_recv()
        both = {}
        for f in range(own, fields):
            i = 2 * (f - own)
            both[f] = (
                factors(advised[i:i + 1, :], count_row(0)),
                factors(advised[i + 1:i + 2, :], count_row(0)),
            )
        for copy, (f, low, size) in list(zip(halos, pieces))[own:]:
            copy.wait_recv()
            roll_finish(f, low, size, *both[f])
        for copy in backs:
            copy.wait_send()

    @pl.when(has_next)
    def _():
        advising.wait_send()
        for copy in halos:
            copy.wait_send()

    for slot in range(part.shape[0]):
        sent = got.at[slot]
        pltpu.make_async_copy(sent, sent, send_sem.at[slot]).wait()


def per_device(n_tm, n_as, values, listed_from, listed_until):
    fields, rows, assets = values.shape
    blocks = rows // WINDOW
    groups = field_groups(fields)
    own = groups[0][1]
    stats = -(-max(own * blocks, blocks + 2) // 8) * 8
    slots = 1 + 2 * len(groups) + 2 * own
    cuts = len(halo_pieces(fields, assets // LANES))
    f32 = jnp.float32
    vmem = pltpu.VMEM
    dma = pltpu.SemaphoreType.DMA
    return pl.pallas_call(
        functools.partial(kernel, n_tm, n_as),
        out_shape=vmem((fields, rows, assets), f32),
        in_specs=[pl.BlockSpec(memory_space=pltpu.HBM)] * 3,
        out_specs=pl.BlockSpec(memory_space=vmem),
        scratch_shapes=[
            vmem((fields, WINDOW + rows + WINDOW, assets), f32),
            vmem((fields, rows + WINDOW, assets), f32),
            vmem((WINDOW + rows + WINDOW, assets), f32),
            vmem((WINDOW + rows + WINDOW, assets), f32),
            vmem((1, assets), jnp.int32),
            vmem((1, assets), jnp.int32),
            vmem((slots, stats, LANES), f32),
            vmem((slots, n_as - 1, stats, LANES), f32),
            vmem((slots, stats, LANES), f32),
            vmem((max(8, 2 * own), LANES), f32),
            vmem((max(8, 2 * own), LANES), f32),
            dma((fields + 2,)),
            dma((cuts,)),
            dma((cuts,)),
            dma((own,)),
            dma((own,)),
            dma((2,)),
            dma((slots,)),
            dma((slots,)),
        ],
        compiler_params=pltpu.CompilerParams(
            collective_id=0, has_side_effects=True, vmem_limit_bytes=48 * 2**20
        ),
    )(values, listed_from[None], listed_until[None])


def solution(mesh):
    in_specs = (P(None, "tm", "asset"), P("asset"), P("asset"))
    out_specs = P(None, "tm", "asset")
    body = functools.partial(per_device, mesh.shape["tm"], mesh.shape["asset"])
    return jax.shard_map(
        body, mesh=mesh, in_specs=in_specs, out_specs=out_specs, check_vma=False
    )
```

```python
import functools

import jax
import jax.numpy as jnp
from jax import lax
from jax.experimental import pallas as pl
from jax.experimental.pallas import tpu as pltpu
from jax.sharding import PartitionSpec as P

WINDOW = 64
LANES = 128
SUBLANES = 8
CLIP = 3.0
ROLL_UNROLL = 4
UNROLL = 4
PIECES = 8
HELD = 2


def field_groups(fields):
    half = (fields + 1) // 2
    return [(start, min(half, fields - start)) for start in range(0, fields, half)]


def halo_pieces(fields, chunks):
    cuts = PIECES if chunks % PIECES == 0 else 1
    whole = [(f, 0, chunks) for f in range(fields - 1)]
    size = chunks // cuts
    return whole + [(fields - 1, c * size, size) for c in range(cuts)]


def kernel(
    n_tm, n_as, values, opened_hbm, closed_hbm, out,
    x, rolling, weight, inverse, opened_ref, closed_ref,
    acc, columns_of, part, got, totals, counts, advice, advised,
    load_sem, halo_send, halo_recv, back_send, back_recv, advice_sem, send_sem, recv_sem,
):
    fields, rows, assets = values.shape
    blocks = rows // WINDOW
    chunks = assets // LANES
    tiles = WINDOW // SUBLANES
    groups = field_groups(fields)
    own = groups[0][1]
    helped = fields - own
    tm = lax.axis_index("tm")
    me = lax.axis_index("asset")
    later = lax.rem(tm + 1, n_tm)
    before = lax.rem(tm + n_tm - 1, n_tm)
    has_next = tm < n_tm - 1
    has_prev = tm > 0

    dates = [
        pltpu.make_async_copy(opened_hbm, opened_ref, load_sem.at[fields]),
        pltpu.make_async_copy(closed_hbm, closed_ref, load_sem.at[fields + 1]),
    ]
    loads = [
        pltpu.make_async_copy(values.at[f], x.at[f, pl.ds(WINDOW, rows)], load_sem.at[f])
        for f in range(fields)
    ]

    barrier = pltpu.get_barrier_semaphore()
    for other in (later, before):
        pl.semaphore_signal(barrier, inc=1, device_id={"tm": other})
    for d in range(1, n_as):
        pl.semaphore_signal(barrier, inc=1, device_id={"asset": lax.rem(me + d, n_as)})
    for copy in dates + loads:
        copy.start()

    pieces = halo_pieces(fields, chunks)
    halos = []
    for i, (f, first, size) in enumerate(pieces):
        cols = pl.ds(first * LANES, size * LANES)
        halos.append(pltpu.make_async_remote_copy(
            src_ref=values.at[f, pl.ds(rows - WINDOW, WINDOW), cols],
            dst_ref=x.at[f, pl.ds(0, WINDOW), cols],
            send_sem=halo_send.at[i],
            recv_sem=halo_recv.at[i],
            device_id={"tm": later},
        ))
    backs = [
        pltpu.make_async_remote_copy(
            src_ref=values.at[f, pl.ds(0, WINDOW)],
            dst_ref=x.at[f, pl.ds(WINDOW + rows, WINDOW)],
            send_sem=back_send.at[f - own],
            recv_sem=back_recv.at[f - own],
            device_id={"tm": before},
        )
        for f in range(own, fields)
    ]
    advising = pltpu.make_async_remote_copy(
        src_ref=advice,
        dst_ref=advised,
        send_sem=advice_sem.at[0],
        recv_sem=advice_sem.at[1],
        device_id={"tm": later},
    )
    free = len(halos) - min(HELD, len(halos) - (fields - 1))

    def send(slot):
        for d in range(1, n_as):
            pltpu.make_async_remote_copy(
                src_ref=part.at[slot],
                dst_ref=got.at[slot, d - 1],
                send_sem=send_sem.at[slot],
                recv_sem=recv_sem.at[slot],
                device_id={"asset": lax.rem(me + d, n_as)},
            ).start()

    def receive(slot):
        arrived = got.at[slot]
        pltpu.make_async_copy(arrived, arrived, recv_sem.at[slot]).wait()
        totals[slot] = part[slot] + jnp.sum(got[slot], axis=0)

    def columns(c):
        return pl.ds(pl.multiple_of(c * LANES, LANES), LANES)

    def reduce_items(slot, items):
        for i in range(items):
            part[slot, i:i + 1, :] = jnp.sum(acc[i].T, axis=0, keepdims=True)

    def spread_items(sums, count, items):
        mean = sums / count
        other = pltpu.roll(mean, WINDOW, 1)
        scale = 1.0 / jnp.sqrt(jnp.maximum(mean - other * other, 0.0) + 0.1)
        lane = lax.broadcasted_iota(jnp.int32, mean.shape, 1)
        row = jnp.where(lane < WINDOW, mean, scale)
        for i in range(items):
            columns_of[i] = jnp.broadcast_to(row[i:i + 1], (LANES, LANES)).T

    def column_pair(i):
        return columns_of[i, :WINDOW, :], columns_of[i, WINDOW:, :]

    zero = jnp.zeros((WINDOW, LANES), jnp.float32)
    part[...] = jnp.zeros(part.shape, part.dtype)
    acc[...] = jnp.zeros(acc.shape, acc.dtype)
    first_stamp = tm * rows - WINDOW
    for copy in dates:
        copy.wait()

    @pl.when(tm == 0)
    def _():
        @pl.loop(0, fields)
        def clear(f):
            x[f, pl.ds(0, WINDOW), :] = jnp.zeros((WINDOW, assets), jnp.float32)

    @pl.loop(0, blocks + 2)
    def listing(b):
        start = pl.multiple_of(b * WINDOW, WINDOW)
        row = lax.broadcasted_iota(jnp.int32, (WINDOW, LANES), 0)
        passed = (first_stamp + start + 1 + row).astype(jnp.float32)

        def chunk(c, total):
            cols = columns(c)
            opened = jnp.maximum(opened_ref[:, cols], 0).astype(jnp.float32)
            closed = closed_ref[:, cols].astype(jnp.float32)
            age = passed - opened
            listed = (age > 0.0) & (passed <= closed)
            ones = jnp.where(listed, 1.0, 0.0)
            weight[pl.ds(start, WINDOW), cols] = ones
            counted = jnp.minimum(jnp.maximum(age, 1.0), float(WINDOW))
            inverse[pl.ds(start, WINDOW), cols] = ones / counted
            return total + ones

        total = lax.fori_loop(0, chunks, chunk, zero, unroll=2)
        at = lax.rem(b + blocks + 1, blocks + 2)
        acc[at, :WINDOW, :] = total
        acc[at, WINDOW:, :] = total

    reduce_items(0, blocks + 1)
    pl.semaphore_wait(barrier, n_as + 1)

    @pl.when(has_next)
    def _():
        for copy in halos[:free]:
            copy.start()

    @pl.when(has_prev)
    def _():
        for copy in backs:
            copy.start()

    send(0)

    def window_means(f, b, c):
        top = pl.multiple_of(b * WINDOW, WINDOW)
        cols = columns(c)
        sublane = lax.broadcasted_iota(jnp.int32, (SUBLANES, LANES), 0)

        ends = range(2 * tiles)
        reach = pl.ds(top, 2 * WINDOW)
        masked = x[f, reach, cols] * weight[reach, cols]
        sums = {j: masked[SUBLANES * j:SUBLANES * (j + 1)] for j in ends}
        step = 1
        while step < tiles:
            sums = {j: sums[j] + sums[j - step] for j in ends if j - step in sums}
            step *= 2
        shift = 1
        while shift < SUBLANES:
            keep = sublane < SUBLANES - shift
            moved = {tiles - 1: sums[tiles - 1]}
            for j in range(tiles, 2 * tiles):
                moved[j] = jnp.where(keep, sums[j], sums[j - 1])
            sums = {j: sums[j] + pltpu.roll(moved[j], shift, 0) for j in moved}
            shift *= 2
        ending = jnp.concatenate([sums[j] for j in range(tiles, 2 * tiles)], axis=0)
        return ending * inverse[pl.ds(top + WINDOW, WINDOW), cols]

    def roll_window(f, b, i):
        top = pl.multiple_of(b * WINDOW, WINDOW)

        def chunk(c, carry):
            means = window_means(f, b, c)
            rolling[f, pl.ds(top, WINDOW), columns(c)] = means
            return carry[0] + means, carry[1] + means * means

        first, second = lax.fori_loop(0, chunks, chunk, (zero, zero), unroll=ROLL_UNROLL)
        acc[i, :WINDOW, :] = first
        acc[i, WINDOW:, :] = second

    def clip_scores(f, b, i):
        top = pl.multiple_of(b * WINDOW, WINDOW)
        center, scale = column_pair(i)

        def chunk(c, carry):
            cols = columns(c)
            here = pl.ds(top, WINDOW)
            scored = (rolling[f, here, cols] - center) * scale
            clipped = jnp.minimum(jnp.maximum(scored, -CLIP), CLIP)
            rolling[f, here, cols] = clipped
            masked = clipped * weight[pl.ds(top + WINDOW, WINDOW), cols]
            return carry[0] + masked, carry[1] + masked * clipped

        first, second = lax.fori_loop(0, chunks, chunk, (zero, zero), unroll=UNROLL)
        acc[i, :WINDOW, :] = first
        acc[i, WINDOW:, :] = second

    def finish(f, b, i):
        top = pl.multiple_of(b * WINDOW, WINDOW)
        middle, factor = column_pair(i)

        @pl.loop(0, chunks, unroll=UNROLL)
        def chunk(c):
            cols = columns(c)
            here = pl.ds(top, WINDOW)
            deviate = (rolling[f, here, cols] - middle) * weight[pl.ds(top + WINDOW, WINDOW), cols]
            out[f, here, cols] = deviate * factor

    def roll_finish(f, low, size, i):
        center, scale = column_pair(i)
        middle, factor = column_pair(i + 1)

        @pl.loop(low, low + size)
        def chunk(c):
            cols = columns(c)
            means = window_means(f, 0, c)
            clipped = jnp.minimum(jnp.maximum((means - center) * scale, -CLIP), CLIP)
            deviate = (clipped - middle) * weight[WINDOW:2 * WINDOW, cols]
            out[f, :WINDOW, cols] = deviate * factor

    def main_items(g):
        size = groups[g][1]
        return pl.loop(jnp.where(tm == 0, 0, size), size * blocks)

    def main_first(g):
        start, size = groups[g]
        for f in range(start, start + size):
            loads[f].wait()

        @main_items(g)
        def item(i):
            roll_window(start + lax.rem(i, size), lax.div(i, size), i)

        reduce_items(1 + 2 * g, size * blocks)
        send(1 + 2 * g)

    def main_counts(g):
        size = groups[g][1]
        for i in range(size * blocks):
            b = i // size
            counts[g, i:i + 1, :] = jnp.maximum(totals[0, b:b + 1, :], 1.0)

    def main_second(g):
        start, size = groups[g]
        slot = 1 + 2 * g
        receive(slot)
        spread_items(totals[slot], counts[g], size * blocks)

        @main_items(g)
        def item(i):
            clip_scores(start + lax.rem(i, size), lax.div(i, size), i)

        reduce_items(slot + 1, size * blocks)
        send(slot + 1)

    def main_third(g):
        start, size = groups[g]
        slot = 2 + 2 * g
        receive(slot)
        spread_items(totals[slot], counts[g], size * blocks)

        @main_items(g)
        def item(i):
            finish(start + lax.rem(i, size), lax.div(i, size), i)

    tail = 1 + 2 * len(groups)
    last = len(groups)

    def tail_first(u):
        @pl.when(has_prev)
        def _():
            halos[u].wait_recv()
            roll_window(u, 0, 2 * u)

        if u < helped:
            @pl.when(has_next)
            def _():
                backs[u].wait_recv()
                roll_window(own + u, blocks, 2 * u + 1)

    def tail_second(u):
        @pl.when(has_prev)
        def _():
            clip_scores(u, 0, 2 * u)

        if u < helped:
            @pl.when(has_next)
            def _():
                clip_scores(own + u, blocks, 2 * u + 1)

    for g in range(len(groups)):
        main_first(g)
    receive(0)
    for i in range(2 * own):
        b = 0 if i % 2 == 0 else blocks
        counts[last, i:i + 1, :] = jnp.maximum(totals[0, b:b + 1, :], 1.0)
    for g in range(len(groups)):
        main_counts(g)
        main_second(g)
    for g in range(len(groups)):
        main_third(g)

    for u in range(own):
        tail_first(u)
    reduce_items(tail, 2 * own)
    send(tail)
    receive(tail)
    spread_items(totals[tail], counts[last], 2 * own)
    for u in range(own):
        tail_second(u)
    reduce_items(tail + 1, 2 * own)
    send(tail + 1)
    receive(tail + 1)
    for u in range(helped):
        i = 2 * u
        advice[i:i + 1, :] = totals[tail, i + 1:i + 2, :]
        advice[i + 1:i + 2, :] = totals[tail + 1, i + 1:i + 2, :]

    @pl.when(has_next)
    def _():
        advising.start()
        for copy in halos[free:]:
            copy.start()

    @pl.when(has_prev)
    def _():
        spread_items(totals[tail + 1], counts[last], 2 * own)
        for u in range(own):
            finish(u, 0, 2 * u)
        advising.wait_recv()
        spread_items(advised[...], jnp.broadcast_to(counts[last, :1, :], advised.shape), 2 * helped)
        for copy, (f, low, size) in list(zip(halos, pieces))[own:]:
            copy.wait_recv()
            roll_finish(f, low, size, 2 * (f - own))
        for copy in backs:
            copy.wait_send()

    @pl.when(has_next)
    def _():
        advising.wait_send()
        for copy in halos:
            copy.wait_send()

    for slot in range(part.shape[0]):
        sent = got.at[slot]
        pltpu.make_async_copy(sent, sent, send_sem.at[slot]).wait()


def per_device(n_tm, n_as, values, listed_from, listed_until):
    fields, rows, assets = values.shape
    blocks = rows // WINDOW
    groups = field_groups(fields)
    own = groups[0][1]
    stats = -(-max(own * blocks, blocks + 2, 2 * own) // SUBLANES) * SUBLANES
    slots = 1 + 2 * len(groups) + 2
    cuts = len(halo_pieces(fields, assets // LANES))
    f32 = jnp.float32
    vmem = pltpu.VMEM
    dma = pltpu.SemaphoreType.DMA
    return pl.pallas_call(
        functools.partial(kernel, n_tm, n_as),
        out_shape=vmem((fields, rows, assets), f32),
        in_specs=[pl.BlockSpec(memory_space=pltpu.HBM)] * 3,
        out_specs=pl.BlockSpec(memory_space=vmem),
        scratch_shapes=[
            vmem((fields, WINDOW + rows + WINDOW, assets), f32),
            vmem((fields, rows + WINDOW, assets), f32),
            vmem((WINDOW + rows + WINDOW, assets), f32),
            vmem((WINDOW + rows + WINDOW, assets), f32),
            vmem((1, assets), jnp.int32),
            vmem((1, assets), jnp.int32),
            vmem((stats, LANES, LANES), f32),
            vmem((stats, LANES, LANES), f32),
            vmem((slots, stats, LANES), f32),
            vmem((slots, n_as - 1, stats, LANES), f32),
            vmem((slots, stats, LANES), f32),
            vmem((len(groups) + 1, stats, LANES), f32),
            vmem((stats, LANES), f32),
            vmem((stats, LANES), f32),
            dma((fields + 2,)),
            dma((cuts,)),
            dma((cuts,)),
            dma((own,)),
            dma((own,)),
            dma((2,)),
            dma((slots,)),
            dma((slots,)),
        ],
        compiler_params=pltpu.CompilerParams(
            collective_id=0, has_side_effects=True, vmem_limit_bytes=48 * 2**20
        ),
    )(values, listed_from[None], listed_until[None])


def solution(mesh):
    in_specs = (P(None, "tm", "asset"), P("asset"), P("asset"))
    out_specs = P(None, "tm", "asset")
    body = functools.partial(per_device, mesh.shape["tm"], mesh.shape["asset"])
    return jax.shard_map(
        body, mesh=mesh, in_specs=in_specs, out_specs=out_specs, check_vma=False
    )
```

```python
import functools

import jax
import jax.numpy as jnp
from jax import lax
from jax.experimental import pallas as pl
from jax.experimental.pallas import tpu as pltpu
from jax.sharding import PartitionSpec as P

WINDOW = 64
LANES = 128
SUBLANES = 8
CLIP = 3.0
ROLL_UNROLL = 4
UNROLL = 4
PIECES = 8
HELD = 2


def field_groups(fields):
    half = (fields + 1) // 2
    return [(start, min(half, fields - start)) for start in range(0, fields, half)]


def halo_pieces(fields, chunks):
    cuts = PIECES if chunks % PIECES == 0 else 1
    whole = [(f, 0, chunks) for f in range(fields - 1)]
    size = chunks // cuts
    return whole + [(fields - 1, c * size, size) for c in range(cuts)]


def greeting_rounds(n):
    if n % 2:
        return 0
    return max(n // 2 - 1, 0)


def kernel(
    n_tm, n_as, values, opened_hbm, closed_hbm, out,
    x, rolling, weight, inverse, opened_ref, closed_ref,
    acc, columns_of, part, got, totals, counts, advice, advised,
    load_sem, halo_send, halo_recv, back_send, back_recv, advice_sem, send_sem, recv_sem, hello,
):
    fields, rows, assets = values.shape
    blocks = rows // WINDOW
    chunks = assets // LANES
    tiles = WINDOW // SUBLANES
    groups = field_groups(fields)
    own = groups[0][1]
    helped = fields - own
    tm = lax.axis_index("tm")
    me = lax.axis_index("asset")
    later = lax.rem(tm + 1, n_tm)
    before = lax.rem(tm + n_tm - 1, n_tm)
    has_next = tm < n_tm - 1
    has_prev = tm > 0

    dates = [
        pltpu.make_async_copy(opened_hbm, opened_ref, load_sem.at[fields]),
        pltpu.make_async_copy(closed_hbm, closed_ref, load_sem.at[fields + 1]),
    ]
    loads = [
        pltpu.make_async_copy(values.at[f], x.at[f, pl.ds(WINDOW, rows)], load_sem.at[f])
        for f in range(fields)
    ]

    barrier = pltpu.get_barrier_semaphore()
    rounds = greeting_rounds(n_as)

    @pl.when(has_next)
    def _():
        pl.semaphore_signal(barrier, inc=1, device_id={"tm": later})

    @pl.when(has_prev)
    def _():
        pl.semaphore_signal(barrier, inc=1, device_id={"tm": before})

    def greet(semaphore):
        if n_as % 2:
            for d in range(1, n_as):
                pl.semaphore_signal(semaphore, inc=1, device_id={"asset": lax.rem(me + d, n_as)})
            return n_as - 1
        beside = me + 1 - 2 * lax.rem(me, 2)
        pl.semaphore_signal(semaphore, inc=1, device_id={"asset": beside})

        @pl.when(me >= 2)
        def _():
            pl.semaphore_signal(semaphore, inc=1, device_id={"asset": me - 2})

        @pl.when(me + 2 < n_as)
        def _():
            pl.semaphore_signal(semaphore, inc=1, device_id={"asset": me + 2})

        return 1 + jnp.where(me >= 2, 1, 0) + jnp.where(me + 2 < n_as, 1, 0)

    near = greet(barrier)
    expected = near + jnp.where(has_next, 1, 0) + jnp.where(has_prev, 1, 0)
    for copy in dates + loads:
        copy.start()

    pieces = halo_pieces(fields, chunks)
    halos = []
    for i, (f, first, size) in enumerate(pieces):
        cols = pl.ds(first * LANES, size * LANES)
        halos.append(pltpu.make_async_remote_copy(
            src_ref=values.at[f, pl.ds(rows - WINDOW, WINDOW), cols],
            dst_ref=x.at[f, pl.ds(0, WINDOW), cols],
            send_sem=halo_send.at[i],
            recv_sem=halo_recv.at[i],
            device_id={"tm": later},
        ))
    backs = [
        pltpu.make_async_remote_copy(
            src_ref=values.at[f, pl.ds(0, WINDOW)],
            dst_ref=x.at[f, pl.ds(WINDOW + rows, WINDOW)],
            send_sem=back_send.at[f - own],
            recv_sem=back_recv.at[f - own],
            device_id={"tm": before},
        )
        for f in range(own, fields)
    ]
    advising = pltpu.make_async_remote_copy(
        src_ref=advice,
        dst_ref=advised,
        send_sem=advice_sem.at[0],
        recv_sem=advice_sem.at[1],
        device_id={"tm": later},
    )
    free = len(halos) - min(HELD, len(halos) - (fields - 1))

    def send(slot):
        for d in range(1, n_as):
            pltpu.make_async_remote_copy(
                src_ref=part.at[slot],
                dst_ref=got.at[slot, d - 1],
                send_sem=send_sem.at[slot],
                recv_sem=recv_sem.at[slot],
                device_id={"asset": lax.rem(me + d, n_as)},
            ).start()

    def receive(slot):
        arrived = got.at[slot]
        pltpu.make_async_copy(arrived, arrived, recv_sem.at[slot]).wait()
        totals[slot] = part[slot] + jnp.sum(got[slot], axis=0)

    def columns(c):
        return pl.ds(pl.multiple_of(c * LANES, LANES), LANES)

    def reduce_items(slot, items):
        for i in range(items):
            part[slot, i:i + 1, :] = jnp.sum(acc[i].T, axis=0, keepdims=True)

    def spread_items(sums, count, items):
        mean = sums / count
        other = pltpu.roll(mean, WINDOW, 1)
        scale = 1.0 / jnp.sqrt(jnp.maximum(mean - other * other, 0.0) + 0.1)
        lane = lax.broadcasted_iota(jnp.int32, mean.shape, 1)
        row = jnp.where(lane < WINDOW, mean, scale)
        for i in range(items):
            columns_of[i] = jnp.broadcast_to(row[i:i + 1], (LANES, LANES)).T

    def column_pair(i):
        return columns_of[i, :WINDOW, :], columns_of[i, WINDOW:, :]

    zero = jnp.zeros((WINDOW, LANES), jnp.float32)
    part[...] = jnp.zeros(part.shape, part.dtype)
    acc[...] = jnp.zeros(acc.shape, acc.dtype)
    first_stamp = tm * rows - WINDOW
    for copy in dates:
        copy.wait()

    @pl.when(tm == 0)
    def _():
        @pl.loop(0, fields)
        def clear(f):
            x[f, pl.ds(0, WINDOW), :] = jnp.zeros((WINDOW, assets), jnp.float32)

    def listing(b):
        start = pl.multiple_of(b * WINDOW, WINDOW)
        row = lax.broadcasted_iota(jnp.int32, (WINDOW, LANES), 0)
        passed = (first_stamp + start + 1 + row).astype(jnp.float32)

        def chunk(c, total):
            cols = columns(c)
            opened = jnp.maximum(opened_ref[:, cols], 0).astype(jnp.float32)
            closed = closed_ref[:, cols].astype(jnp.float32)
            age = passed - opened
            listed = (age > 0.0) & (passed <= closed)
            ones = jnp.where(listed, 1.0, 0.0)
            weight[pl.ds(start, WINDOW), cols] = ones
            counted = jnp.minimum(jnp.maximum(age, 1.0), float(WINDOW))
            inverse[pl.ds(start, WINDOW), cols] = ones / counted
            return total + ones

        total = lax.fori_loop(0, chunks, chunk, zero, unroll=2)
        at = lax.rem(b + blocks + 1, blocks + 2)
        acc[at, :WINDOW, :] = total
        acc[at, WINDOW:, :] = total

    def listing_blocks(low, high):
        pl.loop(low, high)(listing)

    ahead = min(2, blocks)
    listing_blocks(0, ahead)
    pl.semaphore_wait(barrier, expected)

    @pl.when(has_next)
    def _():
        for copy in halos[:free]:
            copy.start()

    @pl.when(has_prev)
    def _():
        for copy in backs:
            copy.start()

    for r in range(rounds):
        greet(hello.at[r])
        if r == 0:
            listing_blocks(ahead, blocks)
        if r == 1:
            listing_blocks(blocks, blocks + 2)
        if r < rounds - 1:
            pl.semaphore_wait(hello.at[r], near)
    if rounds < 1:
        listing_blocks(ahead, blocks)
    if rounds < 2:
        listing_blocks(blocks, blocks + 2)
    reduce_items(0, blocks + 1)

    def window_means(f, b, c):
        top = pl.multiple_of(b * WINDOW, WINDOW)
        cols = columns(c)
        sublane = lax.broadcasted_iota(jnp.int32, (SUBLANES, LANES), 0)

        ends = range(2 * tiles)
        reach = pl.ds(top, 2 * WINDOW)
        masked = x[f, reach, cols] * weight[reach, cols]
        sums = {j: masked[SUBLANES * j:SUBLANES * (j + 1)] for j in ends}
        step = 1
        while step < tiles:
            sums = {j: sums[j] + sums[j - step] for j in ends if j - step in sums}
            step *= 2
        shift = 1
        while shift < SUBLANES:
            keep = sublane < SUBLANES - shift
            moved = {tiles - 1: sums[tiles - 1]}
            for j in range(tiles, 2 * tiles):
                moved[j] = jnp.where(keep, sums[j], sums[j - 1])
            sums = {j: sums[j] + pltpu.roll(moved[j], shift, 0) for j in moved}
            shift *= 2
        ending = jnp.concatenate([sums[j] for j in range(tiles, 2 * tiles)], axis=0)
        return ending * inverse[pl.ds(top + WINDOW, WINDOW), cols]

    def roll_window(f, b, i):
        top = pl.multiple_of(b * WINDOW, WINDOW)

        def chunk(c, carry):
            means = window_means(f, b, c)
            rolling[f, pl.ds(top, WINDOW), columns(c)] = means
            return carry[0] + means, carry[1] + means * means

        first, second = lax.fori_loop(0, chunks, chunk, (zero, zero), unroll=ROLL_UNROLL)
        acc[i, :WINDOW, :] = first
        acc[i, WINDOW:, :] = second

    def clip_scores(f, b, i):
        top = pl.multiple_of(b * WINDOW, WINDOW)
        center, scale = column_pair(i)

        def chunk(c, carry):
            cols = columns(c)
            here = pl.ds(top, WINDOW)
            scored = (rolling[f, here, cols] - center) * scale
            clipped = jnp.minimum(jnp.maximum(scored, -CLIP), CLIP)
            rolling[f, here, cols] = clipped
            masked = clipped * weight[pl.ds(top + WINDOW, WINDOW), cols]
            return carry[0] + masked, carry[1] + masked * clipped

        first, second = lax.fori_loop(0, chunks, chunk, (zero, zero), unroll=UNROLL)
        acc[i, :WINDOW, :] = first
        acc[i, WINDOW:, :] = second

    def finish(f, b, i):
        top = pl.multiple_of(b * WINDOW, WINDOW)
        middle, factor = column_pair(i)

        @pl.loop(0, chunks, unroll=UNROLL)
        def chunk(c):
            cols = columns(c)
            here = pl.ds(top, WINDOW)
            deviate = (rolling[f, here, cols] - middle) * weight[pl.ds(top + WINDOW, WINDOW), cols]
            out[f, here, cols] = deviate * factor

    def roll_finish(f, low, size, i):
        center, scale = column_pair(i)
        middle, factor = column_pair(i + 1)

        @pl.loop(low, low + size)
        def chunk(c):
            cols = columns(c)
            means = window_means(f, 0, c)
            clipped = jnp.minimum(jnp.maximum((means - center) * scale, -CLIP), CLIP)
            deviate = (clipped - middle) * weight[WINDOW:2 * WINDOW, cols]
            out[f, :WINDOW, cols] = deviate * factor

    def main_items(g):
        size = groups[g][1]
        return pl.loop(jnp.where(tm == 0, 0, size), size * blocks)

    def main_first(g):
        start, size = groups[g]
        for f in range(start, start + size):
            loads[f].wait()

        @main_items(g)
        def item(i):
            roll_window(start + lax.rem(i, size), lax.div(i, size), i)

        reduce_items(1 + 2 * g, size * blocks)
        if g == 0:
            if rounds:
                pl.semaphore_wait(hello.at[rounds - 1], near)
            send(0)
        send(1 + 2 * g)

    def main_counts(g):
        size = groups[g][1]
        for i in range(size * blocks):
            b = i // size
            counts[g, i:i + 1, :] = jnp.maximum(totals[0, b:b + 1, :], 1.0)

    def main_second(g):
        start, size = groups[g]
        slot = 1 + 2 * g
        receive(slot)
        spread_items(totals[slot], counts[g], size * blocks)

        @main_items(g)
        def item(i):
            clip_scores(start + lax.rem(i, size), lax.div(i, size), i)

        reduce_items(slot + 1, size * blocks)
        send(slot + 1)

    def main_third(g):
        start, size = groups[g]
        slot = 2 + 2 * g
        receive(slot)
        spread_items(totals[slot], counts[g], size * blocks)

        @main_items(g)
        def item(i):
            finish(start + lax.rem(i, size), lax.div(i, size), i)

    tail = 1 + 2 * len(groups)
    last = len(groups)

    def tail_first(u):
        @pl.when(has_prev)
        def _():
            halos[u].wait_recv()
            roll_window(u, 0, 2 * u)

        if u < helped:
            @pl.when(has_next)
            def _():
                backs[u].wait_recv()
                roll_window(own + u, blocks, 2 * u + 1)

    def tail_second(u):
        @pl.when(has_prev)
        def _():
            clip_scores(u, 0, 2 * u)

        if u < helped:
            @pl.when(has_next)
            def _():
                clip_scores(own + u, blocks, 2 * u + 1)

    def tail_exchange():
        reduce_items(tail, 2 * own)
        send(tail)

    def tail_scores():
        receive(tail)
        spread_items(totals[tail], counts[last], 2 * own)
        for u in range(own):
            tail_second(u)
        reduce_items(tail + 1, 2 * own)
        send(tail + 1)

    for g in range(len(groups)):
        main_first(g)
    receive(0)
    for i in range(2 * own):
        b = 0 if i % 2 == 0 else blocks
        counts[last, i:i + 1, :] = jnp.maximum(totals[0, b:b + 1, :], 1.0)
    for g in range(len(groups)):
        main_counts(g)
        main_second(g)
    for u in range(own):
        tail_first(u)
    tail_exchange()
    for g in range(len(groups) - 1):
        main_third(g)
    tail_scores()
    main_third(len(groups) - 1)
    receive(tail + 1)
    for u in range(helped):
        i = 2 * u
        advice[i:i + 1, :] = totals[tail, i + 1:i + 2, :]
        advice[i + 1:i + 2, :] = totals[tail + 1, i + 1:i + 2, :]

    @pl.when(has_next)
    def _():
        advising.start()
        for copy in halos[free:]:
            copy.start()

    @pl.when(has_prev)
    def _():
        spread_items(totals[tail + 1], counts[last], 2 * own)
        for u in range(own):
            finish(u, 0, 2 * u)
        advising.wait_recv()
        spread_items(advised[...], jnp.broadcast_to(counts[last, :1, :], advised.shape), 2 * helped)
        for copy, (f, low, size) in list(zip(halos, pieces))[own:]:
            copy.wait_recv()
            roll_finish(f, low, size, 2 * (f - own))
        for copy in backs:
            copy.wait_send()

    @pl.when(has_next)
    def _():
        advising.wait_send()
        for copy in halos:
            copy.wait_send()

    for slot in range(part.shape[0]):
        sent = got.at[slot]
        pltpu.make_async_copy(sent, sent, send_sem.at[slot]).wait()


def per_device(n_tm, n_as, values, listed_from, listed_until):
    fields, rows, assets = values.shape
    blocks = rows // WINDOW
    groups = field_groups(fields)
    own = groups[0][1]
    stats = -(-max(own * blocks, blocks + 2, 2 * own) // SUBLANES) * SUBLANES
    slots = 1 + 2 * len(groups) + 2
    cuts = len(halo_pieces(fields, assets // LANES))
    f32 = jnp.float32
    vmem = pltpu.VMEM
    dma = pltpu.SemaphoreType.DMA
    return pl.pallas_call(
        functools.partial(kernel, n_tm, n_as),
        out_shape=vmem((fields, rows, assets), f32),
        in_specs=[pl.BlockSpec(memory_space=pltpu.HBM)] * 3,
        out_specs=pl.BlockSpec(memory_space=vmem),
        scratch_shapes=[
            vmem((fields, WINDOW + rows + WINDOW, assets), f32),
            vmem((fields, rows + WINDOW, assets), f32),
            vmem((WINDOW + rows + WINDOW, assets), f32),
            vmem((WINDOW + rows + WINDOW, assets), f32),
            vmem((1, assets), jnp.int32),
            vmem((1, assets), jnp.int32),
            vmem((stats, LANES, LANES), f32),
            vmem((stats, LANES, LANES), f32),
            vmem((slots, stats, LANES), f32),
            vmem((slots, n_as - 1, stats, LANES), f32),
            vmem((slots, stats, LANES), f32),
            vmem((len(groups) + 1, stats, LANES), f32),
            vmem((stats, LANES), f32),
            vmem((stats, LANES), f32),
            dma((fields + 2,)),
            dma((cuts,)),
            dma((cuts,)),
            dma((own,)),
            dma((own,)),
            dma((2,)),
            dma((slots,)),
            dma((slots,)),
            pltpu.SemaphoreType.REGULAR((max(greeting_rounds(n_as), 1),)),
        ],
        compiler_params=pltpu.CompilerParams(
            collective_id=0, has_side_effects=True, vmem_limit_bytes=48 * 2**20
        ),
    )(values, listed_from[None], listed_until[None])


def solution(mesh):
    in_specs = (P(None, "tm", "asset"), P("asset"), P("asset"))
    out_specs = P(None, "tm", "asset")
    body = functools.partial(per_device, mesh.shape["tm"], mesh.shape["asset"])
    return jax.shard_map(
        body, mesh=mesh, in_specs=in_specs, out_specs=out_specs, check_vma=False
    )
```

```python
import functools

import jax
import jax.numpy as jnp
from jax import lax
from jax.experimental import pallas as pl
from jax.experimental.pallas import tpu as pltpu
from jax.sharding import PartitionSpec as P

WINDOW = 64
LANES = 128
SUBLANES = 8
CLIP = 3.0
ROLL_UNROLL = 4
UNROLL = 4
PIECES = 8
HELD = 2


def field_groups(fields):
    half = (fields + 1) // 2
    return [(start, min(half, fields - start)) for start in range(0, fields, half)]


def halo_pieces(fields, chunks):
    cuts = PIECES if chunks % PIECES == 0 else 1
    whole = [(f, 0, chunks) for f in range(fields - 1)]
    size = chunks // cuts
    return whole + [(fields - 1, c * size, size) for c in range(cuts)]


def greeting_rounds(n):
    if n % 2:
        return 0
    return max(n // 2 - 1, 0)


def kernel(
    n_tm, n_as, values, opened_hbm, closed_hbm, out,
    x, rolling, weight, inverse, opened_ref, closed_ref,
    acc, columns_of, part, got, totals, counts, advice, advised,
    load_sem, halo_send, halo_recv, back_send, back_recv, advice_sem, send_sem, recv_sem, hello,
):
    fields, rows, assets = values.shape
    blocks = rows // WINDOW
    chunks = assets // LANES
    tiles = WINDOW // SUBLANES
    groups = field_groups(fields)
    own = groups[0][1]
    helped = fields - own
    stats = part.shape[1]
    tm = lax.axis_index("tm")
    me = lax.axis_index("asset")
    later = lax.rem(tm + 1, n_tm)
    before = lax.rem(tm + n_tm - 1, n_tm)
    has_next = tm < n_tm - 1
    has_prev = tm > 0

    dates = [
        pltpu.make_async_copy(opened_hbm, opened_ref, load_sem.at[fields]),
        pltpu.make_async_copy(closed_hbm, closed_ref, load_sem.at[fields + 1]),
    ]
    loads = [
        pltpu.make_async_copy(
            values.at[f], x.at[f, pl.ds(WINDOW, rows), pl.ds(0, assets)], load_sem.at[f]
        )
        for f in range(fields)
    ]

    barrier = pltpu.get_barrier_semaphore()
    rounds = greeting_rounds(n_as)

    @pl.when(has_next)
    def _():
        pl.semaphore_signal(barrier, inc=1, device_id={"tm": later})

    @pl.when(has_prev)
    def _():
        pl.semaphore_signal(barrier, inc=1, device_id={"tm": before})

    def greet(semaphore):
        if n_as % 2:
            for d in range(1, n_as):
                pl.semaphore_signal(semaphore, inc=1, device_id={"asset": lax.rem(me + d, n_as)})
            return n_as - 1
        beside = me + 1 - 2 * lax.rem(me, 2)
        pl.semaphore_signal(semaphore, inc=1, device_id={"asset": beside})

        @pl.when(me >= 2)
        def _():
            pl.semaphore_signal(semaphore, inc=1, device_id={"asset": me - 2})

        @pl.when(me + 2 < n_as)
        def _():
            pl.semaphore_signal(semaphore, inc=1, device_id={"asset": me + 2})

        return 1 + jnp.where(me >= 2, 1, 0) + jnp.where(me + 2 < n_as, 1, 0)

    near = greet(barrier)
    expected = near + jnp.where(has_next, 1, 0) + jnp.where(has_prev, 1, 0)
    for copy in dates + loads:
        copy.start()

    pieces = halo_pieces(fields, chunks)
    halos = []
    for i, (f, first, size) in enumerate(pieces):
        cols = pl.ds(first * LANES, size * LANES)
        halos.append(pltpu.make_async_remote_copy(
            src_ref=values.at[f, pl.ds(rows - WINDOW, WINDOW), cols],
            dst_ref=x.at[f, pl.ds(0, WINDOW), cols],
            send_sem=halo_send.at[i],
            recv_sem=halo_recv.at[i],
            device_id={"tm": later},
        ))
    backs = [
        pltpu.make_async_remote_copy(
            src_ref=values.at[f, pl.ds(0, WINDOW)],
            dst_ref=x.at[f, pl.ds(WINDOW + rows, WINDOW), pl.ds(0, assets)],
            send_sem=back_send.at[f - own],
            recv_sem=back_recv.at[f - own],
            device_id={"tm": before},
        )
        for f in range(own, fields)
    ]
    advising = pltpu.make_async_remote_copy(
        src_ref=advice,
        dst_ref=advised,
        send_sem=advice_sem.at[0],
        recv_sem=advice_sem.at[1],
        device_id={"tm": later},
    )
    free = len(halos) - min(HELD, len(halos) - (fields - 1))

    def send(slot):
        for d in range(1, n_as):
            pltpu.make_async_remote_copy(
                src_ref=part.at[slot],
                dst_ref=got.at[slot, d - 1],
                send_sem=send_sem.at[slot],
                recv_sem=recv_sem.at[slot],
                device_id={"asset": lax.rem(me + d, n_as)},
            ).start()

    def receive(slot):
        arrived = got.at[slot]
        pltpu.make_async_copy(arrived, arrived, recv_sem.at[slot]).wait()
        totals[slot] = part[slot] + jnp.sum(got[slot], axis=0)

    def columns(c):
        return pl.ds(pl.multiple_of(c * LANES, LANES), LANES)

    def reduce_items(slot, items, first=0):
        for i in range(items):
            part[slot, i:i + 1, :] = jnp.sum(acc[first + i].T, axis=0, keepdims=True)

    def spread_items(sums, count, items, first=0):
        mean = sums / count
        other = pltpu.roll(mean, WINDOW, 1)
        scale = 1.0 / jnp.sqrt(jnp.maximum(mean - other * other, 0.0) + 0.1)
        lane = lax.broadcasted_iota(jnp.int32, mean.shape, 1)
        row = jnp.where(lane < WINDOW, mean, scale)
        for i in range(items):
            columns_of[first + i] = jnp.broadcast_to(row[i:i + 1], (LANES, LANES)).T

    def column_pair(i):
        return columns_of[i, :WINDOW, :], columns_of[i, WINDOW:, :]

    zero = jnp.zeros((WINDOW, LANES), jnp.float32)
    part[...] = jnp.zeros(part.shape, part.dtype)
    acc[...] = jnp.zeros(acc.shape, acc.dtype)
    first_stamp = tm * rows - WINDOW
    for copy in dates:
        copy.wait()

    @pl.when(tm == 0)
    def _():
        @pl.loop(0, fields)
        def clear(f):
            x[f, pl.ds(0, WINDOW), pl.ds(0, assets)] = jnp.zeros((WINDOW, assets), jnp.float32)

    def listing(b):
        start = pl.multiple_of(b * WINDOW, WINDOW)
        row = lax.broadcasted_iota(jnp.int32, (WINDOW, LANES), 0)
        passed = (first_stamp + start + 1 + row).astype(jnp.float32)

        def chunk(c, total):
            cols = columns(c)
            opened = jnp.maximum(opened_ref[:, cols], 0).astype(jnp.float32)
            closed = closed_ref[:, cols].astype(jnp.float32)
            age = passed - opened
            listed = (age > 0.0) & (passed <= closed)
            ones = jnp.where(listed, 1.0, 0.0)
            weight[pl.ds(start, WINDOW), cols] = ones
            counted = jnp.minimum(jnp.maximum(age, 1.0), float(WINDOW))
            inverse[pl.ds(start, WINDOW), cols] = ones / counted
            return total + ones

        total = lax.fori_loop(0, chunks, chunk, zero, unroll=2)
        at = lax.rem(b + blocks + 1, blocks + 2)
        acc[at, :WINDOW, :] = total
        acc[at, WINDOW:, :] = total

    def listing_blocks(low, high):
        pl.loop(low, high)(listing)

    ahead = min(2, blocks)
    listing_blocks(0, ahead)
    pl.semaphore_wait(barrier, expected)

    @pl.when(has_next)
    def _():
        for copy in halos[:free]:
            copy.start()

    @pl.when(has_prev)
    def _():
        for copy in backs:
            copy.start()

    for r in range(rounds):
        greet(hello.at[r])
        if r == 0:
            listing_blocks(ahead, blocks)
        if r == 1:
            listing_blocks(blocks, blocks + 2)
        if r < rounds - 1:
            pl.semaphore_wait(hello.at[r], near)
    if rounds < 1:
        listing_blocks(ahead, blocks)
    if rounds < 2:
        listing_blocks(blocks, blocks + 2)
    reduce_items(0, blocks + 1)

    def window_means(f, b, c):
        top = pl.multiple_of(b * WINDOW, WINDOW)
        cols = columns(c)
        sublane = lax.broadcasted_iota(jnp.int32, (SUBLANES, LANES), 0)

        ends = range(2 * tiles)
        reach = pl.ds(top, 2 * WINDOW)
        masked = x[f, reach, cols] * weight[reach, cols]
        sums = {j: masked[SUBLANES * j:SUBLANES * (j + 1)] for j in ends}
        step = 1
        while step < tiles:
            sums = {j: sums[j] + sums[j - step] for j in ends if j - step in sums}
            step *= 2
        shift = 1
        while shift < SUBLANES:
            keep = sublane < SUBLANES - shift
            moved = {tiles - 1: sums[tiles - 1]}
            for j in range(tiles, 2 * tiles):
                moved[j] = jnp.where(keep, sums[j], sums[j - 1])
            sums = {j: sums[j] + pltpu.roll(moved[j], shift, 0) for j in moved}
            shift *= 2
        ending = jnp.concatenate([sums[j] for j in range(tiles, 2 * tiles)], axis=0)
        return ending * inverse[pl.ds(top + WINDOW, WINDOW), cols]

    def roll_window(f, b, i):
        top = pl.multiple_of(b * WINDOW, WINDOW)

        def chunk(c, carry):
            means = window_means(f, b, c)
            rolling[f, pl.ds(top, WINDOW), columns(c)] = means
            return carry[0] + means, carry[1] + means * means

        first, second = lax.fori_loop(0, chunks, chunk, (zero, zero), unroll=ROLL_UNROLL)
        acc[i, :WINDOW, :] = first
        acc[i, WINDOW:, :] = second

    def clip_scores(f, b, i):
        top = pl.multiple_of(b * WINDOW, WINDOW)
        center, scale = column_pair(i)

        def chunk(c, carry):
            cols = columns(c)
            here = pl.ds(top, WINDOW)
            scored = (rolling[f, here, cols] - center) * scale
            clipped = jnp.minimum(jnp.maximum(scored, -CLIP), CLIP)
            rolling[f, here, cols] = clipped
            masked = clipped * weight[pl.ds(top + WINDOW, WINDOW), cols]
            return carry[0] + masked, carry[1] + masked * clipped

        first, second = lax.fori_loop(0, chunks, chunk, (zero, zero), unroll=UNROLL)
        acc[i, :WINDOW, :] = first
        acc[i, WINDOW:, :] = second

    def finish(f, b, i):
        top = pl.multiple_of(b * WINDOW, WINDOW)
        middle, factor = column_pair(i)

        @pl.loop(0, chunks, unroll=UNROLL)
        def chunk(c):
            cols = columns(c)
            here = pl.ds(top, WINDOW)
            deviate = (rolling[f, here, cols] - middle) * weight[pl.ds(top + WINDOW, WINDOW), cols]
            out[f, here, cols] = deviate * factor

    def standardized(means, cols, first, second):
        center, scale = first
        middle, factor = second
        clipped = jnp.minimum(jnp.maximum((means - center) * scale, -CLIP), CLIP)
        return (clipped - middle) * weight[WINDOW:2 * WINDOW, cols] * factor

    def roll_only(f, low, size):
        @pl.loop(low, low + size, unroll=min(2, size))
        def chunk(c):
            rolling[f, :WINDOW, columns(c)] = window_means(f, 0, c)

    def score_finish(f, low, size, i):
        first, second = column_pair(i), column_pair(i + 1)

        @pl.loop(low, low + size, unroll=min(2, size))
        def chunk(c):
            cols = columns(c)
            out[f, :WINDOW, cols] = standardized(rolling[f, :WINDOW, cols], cols, first, second)

    def roll_finish(f, low, size, i):
        first, second = column_pair(i), column_pair(i + 1)

        @pl.loop(low, low + size, unroll=min(2, size))
        def chunk(c):
            cols = columns(c)
            out[f, :WINDOW, cols] = standardized(window_means(f, 0, c), cols, first, second)

    def main_items(g):
        size = groups[g][1]
        return pl.loop(jnp.where(tm == 0, 0, size), size * blocks)

    def main_first(g):
        start, size = groups[g]
        for f in range(start, start + size):
            loads[f].wait()

        @main_items(g)
        def item(i):
            roll_window(start + lax.rem(i, size), lax.div(i, size), i)

        reduce_items(1 + 2 * g, size * blocks)
        if g == 0:
            if rounds:
                pl.semaphore_wait(hello.at[rounds - 1], near)
            send(0)
        send(1 + 2 * g)

    def main_counts(g):
        size = groups[g][1]
        for i in range(size * blocks):
            b = i // size
            counts[g, i:i + 1, :] = jnp.maximum(totals[0, b:b + 1, :], 1.0)

    def main_second(g):
        start, size = groups[g]
        slot = 1 + 2 * g
        receive(slot)
        spread_items(totals[slot], counts[g], size * blocks)

        @main_items(g)
        def item(i):
            clip_scores(start + lax.rem(i, size), lax.div(i, size), i)

        reduce_items(slot + 1, size * blocks)
        send(slot + 1)

    def main_third(g):
        start, size = groups[g]
        slot = 2 + 2 * g
        receive(slot)
        spread_items(totals[slot], counts[g], size * blocks)

        @main_items(g)
        def item(i):
            finish(start + lax.rem(i, size), lax.div(i, size), i)

    tail = 1 + 2 * len(groups)
    last = len(groups)

    def tail_first(u):
        @pl.when(has_prev)
        def _():
            halos[u].wait_recv()
            roll_window(u, 0, stats + 2 * u)

        if u < helped:
            @pl.when(has_next)
            def _():
                backs[u].wait_recv()
                roll_window(own + u, blocks, stats + 2 * u + 1)

    def tail_second(u):
        @pl.when(has_prev)
        def _():
            clip_scores(u, 0, stats + 2 * u)

        if u < helped:
            @pl.when(has_next)
            def _():
                clip_scores(own + u, blocks, stats + 2 * u + 1)

    def tail_exchange():
        reduce_items(tail, 2 * own, stats)
        send(tail)

    def tail_scores():
        receive(tail)
        spread_items(totals[tail], counts[last], 2 * own, stats)
        for u in range(own):
            tail_second(u)
        reduce_items(tail + 1, 2 * own, stats)
        send(tail + 1)

    for g in range(len(groups)):
        main_first(g)
    tail_first(0)

    @pl.when(tm == 0)
    def _():
        for u in range(1, own):
            tail_first(u)
        tail_exchange()

    receive(0)
    for i in range(2 * own):
        b = 0 if i % 2 == 0 else blocks
        counts[last, i:i + 1, :] = jnp.maximum(totals[0, b:b + 1, :], 1.0)
    for g in range(len(groups)):
        main_counts(g)
        main_second(g)

    @pl.when(tm == 0)
    def _():
        tail_scores()

    @pl.when(has_prev)
    def _():
        for u in range(1, own):
            tail_first(u)
        tail_exchange()

    for g in range(len(groups) - 1):
        main_third(g)

    @pl.when(has_prev)
    def _():
        tail_scores()

    main_third(len(groups) - 1)
    receive(tail + 1)
    for u in range(helped):
        i = 2 * u
        advice[i:i + 1, :] = totals[tail, i + 1:i + 2, :]
        advice[i + 1:i + 2, :] = totals[tail + 1, i + 1:i + 2, :]

    @pl.when(has_next)
    def _():
        advising.start()
        for copy in halos[free:]:
            copy.start()

    @pl.when(has_prev)
    def _():
        spread_items(totals[tail + 1], counts[last], 2 * own)
        for u in range(own):
            finish(u, 0, 2 * u)
        landing = list(zip(halos, pieces))[own:]
        early = landing[:len(landing) - (len(halos) - free)]
        for copy, (f, low, size) in early:
            copy.wait_recv()
            roll_only(f, low, size)
        advising.wait_recv()
        spread_items(advised[...], jnp.broadcast_to(counts[last, :1, :], advised.shape), 2 * helped)
        for copy, (f, low, size) in early:
            score_finish(f, low, size, 2 * (f - own))
        for copy, (f, low, size) in landing[len(early):]:
            copy.wait_recv()
            roll_finish(f, low, size, 2 * (f - own))
        for copy in backs:
            copy.wait_send()

    @pl.when(has_next)
    def _():
        advising.wait_send()
        for copy in halos:
            copy.wait_send()

    for slot in range(part.shape[0]):
        sent = got.at[slot]
        pltpu.make_async_copy(sent, sent, send_sem.at[slot]).wait()


def per_device(n_tm, n_as, values, listed_from, listed_until):
    fields, rows, assets = values.shape
    blocks = rows // WINDOW
    groups = field_groups(fields)
    own = groups[0][1]
    stats = -(-max(own * blocks, blocks + 2, 2 * own) // SUBLANES) * SUBLANES
    slots = 1 + 2 * len(groups) + 2
    cuts = len(halo_pieces(fields, assets // LANES))
    f32 = jnp.float32
    vmem = pltpu.VMEM
    dma = pltpu.SemaphoreType.DMA
    return pl.pallas_call(
        functools.partial(kernel, n_tm, n_as),
        out_shape=vmem((fields, rows, assets), f32),
        in_specs=[pl.BlockSpec(memory_space=pltpu.HBM)] * 3,
        out_specs=pl.BlockSpec(memory_space=vmem),
        scratch_shapes=[
            vmem((fields, WINDOW + rows + WINDOW, assets + LANES), f32),
            vmem((fields, rows + WINDOW, assets + LANES), f32),
            vmem((WINDOW + rows + WINDOW, assets + LANES), f32),
            vmem((WINDOW + rows + WINDOW, assets + LANES), f32),
            vmem((1, assets), jnp.int32),
            vmem((1, assets), jnp.int32),
            vmem((stats + 2 * own, LANES, LANES), f32),
            vmem((stats + 2 * own, LANES, LANES), f32),
            vmem((slots, stats, LANES), f32),
            vmem((slots, n_as - 1, stats, LANES), f32),
            vmem((slots, stats, LANES), f32),
            vmem((len(groups) + 1, stats, LANES), f32),
            vmem((stats, LANES), f32),
            vmem((stats, LANES), f32),
            dma((fields + 2,)),
            dma((cuts,)),
            dma((cuts,)),
            dma((own,)),
            dma((own,)),
            dma((2,)),
            dma((slots,)),
            dma((slots,)),
            pltpu.SemaphoreType.REGULAR((max(greeting_rounds(n_as), 1),)),
        ],
        compiler_params=pltpu.CompilerParams(
            collective_id=0, has_side_effects=True, vmem_limit_bytes=48 * 2**20
        ),
    )(values, listed_from[None], listed_until[None])


def solution(mesh):
    in_specs = (P(None, "tm", "asset"), P("asset"), P("asset"))
    out_specs = P(None, "tm", "asset")
    body = functools.partial(per_device, mesh.shape["tm"], mesh.shape["asset"])
    return jax.shard_map(
        body, mesh=mesh, in_specs=in_specs, out_specs=out_specs, check_vma=False
    )
```

```python
import functools

import jax
import jax.numpy as jnp
from jax import lax
from jax.experimental import pallas as pl
from jax.experimental.pallas import tpu as pltpu
from jax.sharding import PartitionSpec as P

WINDOW = 64
LANES = 128
SUBLANES = 8
CLIP = 3.0
ROLL_UNROLL = 4
UNROLL = 4
HELD = 1


def field_groups(fields):
    half = (fields + 1) // 2
    return [(start, min(half, fields - start)) for start in range(0, fields, half)]


def halo_pieces(fields, chunks):
    pieces = [(f, 0, chunks) for f in range(fields - 1)]
    first, left = 0, chunks
    while left > 0:
        size = max(left // 2, 1)
        pieces.append((fields - 1, first, size))
        first, left = first + size, left - size
    return pieces


def greeting_rounds(n):
    if n % 2:
        return 0
    return max(n // 2 - 1, 0)


def kernel(
    n_tm, n_as, values, opened_hbm, closed_hbm, out,
    x, rolling, weight, inverse, opened_ref, closed_ref,
    acc, columns_of, part, got, totals, counts, advice, advised,
    load_sem, halo_send, halo_recv, back_send, back_recv, advice_sem, send_sem, recv_sem, hello,
):
    fields, rows, assets = values.shape
    blocks = rows // WINDOW
    chunks = assets // LANES
    tiles = WINDOW // SUBLANES
    groups = field_groups(fields)
    own = groups[0][1]
    helped = fields - own
    stats = part.shape[1]
    tail = 1 + 2 * len(groups)
    last = len(groups)
    tm = lax.axis_index("tm")
    me = lax.axis_index("asset")
    later = lax.rem(tm + 1, n_tm)
    before = lax.rem(tm + n_tm - 1, n_tm)
    has_next = tm < n_tm - 1
    has_prev = tm > 0

    dates = [
        pltpu.make_async_copy(opened_hbm, opened_ref, load_sem.at[fields]),
        pltpu.make_async_copy(closed_hbm, closed_ref, load_sem.at[fields + 1]),
    ]
    loads = [
        pltpu.make_async_copy(
            values.at[f], x.at[f, pl.ds(WINDOW, rows), pl.ds(0, assets)], load_sem.at[f]
        )
        for f in range(fields)
    ]

    barrier = pltpu.get_barrier_semaphore()
    rounds = greeting_rounds(n_as)

    @pl.when(has_next)
    def _():
        pl.semaphore_signal(barrier, inc=1, device_id={"tm": later})

    @pl.when(has_prev)
    def _():
        pl.semaphore_signal(barrier, inc=1, device_id={"tm": before})

    def greet(semaphore):
        if n_as % 2:
            for d in range(1, n_as):
                pl.semaphore_signal(semaphore, inc=1, device_id={"asset": lax.rem(me + d, n_as)})
            return n_as - 1
        beside = me + 1 - 2 * lax.rem(me, 2)
        pl.semaphore_signal(semaphore, inc=1, device_id={"asset": beside})

        @pl.when(me >= 2)
        def _():
            pl.semaphore_signal(semaphore, inc=1, device_id={"asset": me - 2})

        @pl.when(me + 2 < n_as)
        def _():
            pl.semaphore_signal(semaphore, inc=1, device_id={"asset": me + 2})

        return 1 + jnp.where(me >= 2, 1, 0) + jnp.where(me + 2 < n_as, 1, 0)

    near = greet(barrier)
    expected = near + jnp.where(has_next, 1, 0) + jnp.where(has_prev, 1, 0)
    for copy in dates + loads:
        copy.start()

    pieces = halo_pieces(fields, chunks)
    halos = []
    for i, (f, first, size) in enumerate(pieces):
        cols = pl.ds(first * LANES, size * LANES)
        halos.append(pltpu.make_async_remote_copy(
            src_ref=values.at[f, pl.ds(rows - WINDOW, WINDOW), cols],
            dst_ref=x.at[f, pl.ds(0, WINDOW), cols],
            send_sem=halo_send.at[i],
            recv_sem=halo_recv.at[i],
            device_id={"tm": later},
        ))
    backs = [
        pltpu.make_async_remote_copy(
            src_ref=values.at[f, pl.ds(0, WINDOW)],
            dst_ref=x.at[f, pl.ds(WINDOW + rows, WINDOW), pl.ds(0, assets)],
            send_sem=back_send.at[f - own],
            recv_sem=back_recv.at[f - own],
            device_id={"tm": before},
        )
        for f in range(own, fields)
    ]
    advising = pltpu.make_async_remote_copy(
        src_ref=advice,
        dst_ref=advised,
        send_sem=advice_sem.at[0],
        recv_sem=advice_sem.at[1],
        device_id={"tm": later},
    )
    free = len(halos) - min(HELD, len(halos) - (fields - 1))

    def rows_of(slot):
        return pl.ds(0, 2 * own if slot >= tail else stats)

    def send(slot):
        for d in range(1, n_as):
            pltpu.make_async_remote_copy(
                src_ref=part.at[slot, rows_of(slot)],
                dst_ref=got.at[slot, d - 1, rows_of(slot)],
                send_sem=send_sem.at[slot],
                recv_sem=recv_sem.at[slot],
                device_id={"asset": lax.rem(me + d, n_as)},
            ).start()

    def receive(slot):
        arrived = got.at[slot, :, rows_of(slot)]
        pltpu.make_async_copy(arrived, arrived, recv_sem.at[slot]).wait()
        totals[slot] = part[slot] + jnp.sum(got[slot], axis=0)

    def columns(c):
        return pl.ds(pl.multiple_of(c * LANES, LANES), LANES)

    def reduce_items(slot, items, first=0):
        for i in range(items):
            part[slot, i:i + 1, :] = jnp.sum(acc[first + i].T, axis=0, keepdims=True)

    def spread_items(sums, count, items, first=0):
        mean = sums / count
        other = pltpu.roll(mean, WINDOW, 1)
        scale = 1.0 / jnp.sqrt(jnp.maximum(mean - other * other, 0.0) + 0.1)
        lane = lax.broadcasted_iota(jnp.int32, mean.shape, 1)
        row = jnp.where(lane < WINDOW, mean, scale)
        for i in range(items):
            columns_of[first + i] = jnp.broadcast_to(row[i:i + 1], (LANES, LANES)).T

    def column_pair(i):
        return columns_of[i, :WINDOW, :], columns_of[i, WINDOW:, :]

    zero = jnp.zeros((WINDOW, LANES), jnp.float32)
    part[...] = jnp.zeros(part.shape, part.dtype)
    acc[...] = jnp.zeros(acc.shape, acc.dtype)
    first_stamp = tm * rows - WINDOW
    for copy in dates:
        copy.wait()

    @pl.when(tm == 0)
    def _():
        @pl.loop(0, fields)
        def clear(f):
            x[f, pl.ds(0, WINDOW), pl.ds(0, assets)] = jnp.zeros((WINDOW, assets), jnp.float32)

    def listing(b):
        start = pl.multiple_of(b * WINDOW, WINDOW)
        row = lax.broadcasted_iota(jnp.int32, (WINDOW, LANES), 0)
        passed = (first_stamp + start + 1 + row).astype(jnp.float32)

        def chunk(c, total):
            cols = columns(c)
            opened = jnp.maximum(opened_ref[:, cols], 0).astype(jnp.float32)
            closed = closed_ref[:, cols].astype(jnp.float32)
            age = passed - opened
            listed = (age > 0.0) & (passed <= closed)
            ones = jnp.where(listed, 1.0, 0.0)
            weight[pl.ds(start, WINDOW), cols] = ones
            counted = jnp.minimum(jnp.maximum(age, 1.0), float(WINDOW))
            inverse[pl.ds(start, WINDOW), cols] = ones / counted
            return total + ones

        total = lax.fori_loop(0, chunks, chunk, zero, unroll=2)
        at = lax.rem(b + blocks + 1, blocks + 2)
        acc[at, :WINDOW, :] = total
        acc[at, WINDOW:, :] = total

    def listing_blocks(low, high):
        pl.loop(low, high)(listing)

    ahead = min(2, blocks)
    listing_blocks(0, ahead)
    pl.semaphore_wait(barrier, expected)

    for i in range(free):
        @pl.when(has_next)
        def _():
            halos[i].start()

        if i < helped:
            @pl.when(has_prev)
            def _():
                backs[i].start()

    for r in range(rounds):
        greet(hello.at[r])
        if r == 0:
            listing_blocks(ahead, blocks)
        if r == 1:
            listing_blocks(blocks, blocks + 2)
        if r < rounds - 1:
            pl.semaphore_wait(hello.at[r], near)
    if rounds < 1:
        listing_blocks(ahead, blocks)
    if rounds < 2:
        listing_blocks(blocks, blocks + 2)
    reduce_items(0, blocks + 1)

    def window_means(f, b, c):
        top = pl.multiple_of(b * WINDOW, WINDOW)
        cols = columns(c)
        sublane = lax.broadcasted_iota(jnp.int32, (SUBLANES, LANES), 0)

        ends = range(2 * tiles)
        reach = pl.ds(top, 2 * WINDOW)
        masked = x[f, reach, cols] * weight[reach, cols]
        sums = {j: masked[SUBLANES * j:SUBLANES * (j + 1)] for j in ends}
        step = 1
        while step < tiles:
            sums = {j: sums[j] + sums[j - step] for j in ends if j - step in sums}
            step *= 2
        shift = 1
        while shift < SUBLANES:
            keep = sublane < SUBLANES - shift
            moved = {tiles - 1: sums[tiles - 1]}
            for j in range(tiles, 2 * tiles):
                moved[j] = jnp.where(keep, sums[j], sums[j - 1])
            sums = {j: sums[j] + pltpu.roll(moved[j], shift, 0) for j in moved}
            shift *= 2
        ending = jnp.concatenate([sums[j] for j in range(tiles, 2 * tiles)], axis=0)
        return ending * inverse[pl.ds(top + WINDOW, WINDOW), cols]

    def roll_window(f, b, i):
        top = pl.multiple_of(b * WINDOW, WINDOW)

        def chunk(c, carry):
            means = window_means(f, b, c)
            rolling[f, pl.ds(top, WINDOW), columns(c)] = means
            return carry[0] + means, carry[1] + means * means

        first, second = lax.fori_loop(0, chunks, chunk, (zero, zero), unroll=ROLL_UNROLL)
        acc[i, :WINDOW, :] = first
        acc[i, WINDOW:, :] = second

    def clip_scores(f, b, i):
        top = pl.multiple_of(b * WINDOW, WINDOW)
        center, scale = column_pair(i)

        def chunk(c, carry):
            cols = columns(c)
            here = pl.ds(top, WINDOW)
            scored = (rolling[f, here, cols] - center) * scale
            clipped = jnp.minimum(jnp.maximum(scored, -CLIP), CLIP)
            rolling[f, here, cols] = clipped
            masked = clipped * weight[pl.ds(top + WINDOW, WINDOW), cols]
            return carry[0] + masked, carry[1] + masked * clipped

        first, second = lax.fori_loop(0, chunks, chunk, (zero, zero), unroll=UNROLL)
        acc[i, :WINDOW, :] = first
        acc[i, WINDOW:, :] = second

    def finish(f, b, i):
        top = pl.multiple_of(b * WINDOW, WINDOW)
        middle, factor = column_pair(i)

        @pl.loop(0, chunks, unroll=UNROLL)
        def chunk(c):
            cols = columns(c)
            here = pl.ds(top, WINDOW)
            deviate = (rolling[f, here, cols] - middle) * weight[pl.ds(top + WINDOW, WINDOW), cols]
            out[f, here, cols] = deviate * factor

    def standardized(means, cols, first, second):
        center, scale = first
        middle, factor = second
        clipped = jnp.minimum(jnp.maximum((means - center) * scale, -CLIP), CLIP)
        return (clipped - middle) * weight[WINDOW:2 * WINDOW, cols] * factor

    def roll_only(f, low, size):
        @pl.loop(low, low + size, unroll=min(2, size))
        def chunk(c):
            rolling[f, :WINDOW, columns(c)] = window_means(f, 0, c)

    def score_finish(f, low, size, i):
        first, second = column_pair(i), column_pair(i + 1)

        @pl.loop(low, low + size, unroll=min(2, size))
        def chunk(c):
            cols = columns(c)
            out[f, :WINDOW, cols] = standardized(rolling[f, :WINDOW, cols], cols, first, second)

    def roll_finish(f, low, size, i):
        first, second = column_pair(i), column_pair(i + 1)

        @pl.loop(low, low + size, unroll=min(2, size))
        def chunk(c):
            cols = columns(c)
            out[f, :WINDOW, cols] = standardized(window_means(f, 0, c), cols, first, second)

    def main_items(g):
        size = groups[g][1]
        return pl.loop(jnp.where(tm == 0, 0, size), size * blocks)

    def main_first(g):
        start, size = groups[g]
        for f in range(start, start + size):
            loads[f].wait()

        @main_items(g)
        def item(i):
            roll_window(start + lax.rem(i, size), lax.div(i, size), i)

        reduce_items(1 + 2 * g, size * blocks)
        if g == 0:
            if rounds:
                pl.semaphore_wait(hello.at[rounds - 1], near)
            send(0)
        send(1 + 2 * g)

    def main_counts(g):
        size = groups[g][1]
        for i in range(size * blocks):
            b = i // size
            counts[g, i:i + 1, :] = jnp.maximum(totals[0, b:b + 1, :], 1.0)

    def main_second(g):
        start, size = groups[g]
        slot = 1 + 2 * g
        receive(slot)
        spread_items(totals[slot], counts[g], size * blocks)

        @main_items(g)
        def item(i):
            clip_scores(start + lax.rem(i, size), lax.div(i, size), i)

        reduce_items(slot + 1, size * blocks)
        send(slot + 1)

    def main_third(g):
        start, size = groups[g]
        slot = 2 + 2 * g
        receive(slot)
        spread_items(totals[slot], counts[g], size * blocks)

        @main_items(g)
        def item(i):
            finish(start + lax.rem(i, size), lax.div(i, size), i)

    def tail_first(u):
        @pl.when(has_prev)
        def _():
            halos[u].wait_recv()
            roll_window(u, 0, stats + 2 * u)

        if u < helped:
            @pl.when(has_next)
            def _():
                backs[u].wait_recv()
                roll_window(own + u, blocks, stats + 2 * u + 1)

    def tail_second(u):
        @pl.when(has_prev)
        def _():
            clip_scores(u, 0, stats + 2 * u)

        if u < helped:
            @pl.when(has_next)
            def _():
                clip_scores(own + u, blocks, stats + 2 * u + 1)

    def tail_exchange():
        reduce_items(tail, 2 * own, stats)
        send(tail)

    def tail_scores():
        receive(tail)
        spread_items(totals[tail], counts[last], 2 * own, stats)
        for u in range(own):
            tail_second(u)
        reduce_items(tail + 1, 2 * own, stats)
        send(tail + 1)

    for g in range(len(groups)):
        main_first(g)
    tail_first(0)

    @pl.when(tm == 0)
    def _():
        for u in range(1, own):
            tail_first(u)
        tail_exchange()

    receive(0)
    for i in range(2 * own):
        b = 0 if i % 2 == 0 else blocks
        counts[last, i:i + 1, :] = jnp.maximum(totals[0, b:b + 1, :], 1.0)
    main_counts(0)
    main_second(0)

    @pl.when(has_prev)
    def _():
        for u in range(1, own):
            tail_first(u)
        tail_exchange()

    for g in range(1, len(groups)):
        main_counts(g)
        main_second(g)

    @pl.when(tm == 0)
    def _():
        tail_scores()

    for g in range(len(groups) - 1):
        main_third(g)

    @pl.when(has_prev)
    def _():
        tail_scores()

    main_third(len(groups) - 1)
    landing = list(zip(halos, pieces))[own:]
    early = landing[:len(landing) - (len(halos) - free)]
    sooner = [entry for entry in early if entry[1][0] < fields - 1]

    @pl.when(has_prev)
    def _():
        for copy, (f, low, size) in sooner:
            copy.wait_recv()
            roll_only(f, low, size)

    receive(tail + 1)
    for u in range(helped):
        i = 2 * u
        advice[i:i + 1, :] = totals[tail, i + 1:i + 2, :]
        advice[i + 1:i + 2, :] = totals[tail + 1, i + 1:i + 2, :]

    @pl.when(has_next)
    def _():
        advising.start()
        for copy in halos[free:]:
            copy.start()

    @pl.when(has_prev)
    def _():
        spread_items(totals[tail + 1], counts[last], 2 * own)
        for u in range(own):
            finish(u, 0, 2 * u)
        for copy, (f, low, size) in early[len(sooner):]:
            copy.wait_recv()
            roll_only(f, low, size)
        advising.wait_recv()
        spread_items(advised[...], jnp.broadcast_to(counts[last, :1, :], advised.shape), 2 * helped)
        for copy, (f, low, size) in early:
            score_finish(f, low, size, 2 * (f - own))
        for copy, (f, low, size) in landing[len(early):]:
            copy.wait_recv()
            roll_finish(f, low, size, 2 * (f - own))
        for copy in backs:
            copy.wait_send()

    @pl.when(has_next)
    def _():
        advising.wait_send()
        for copy in halos:
            copy.wait_send()

    for slot in range(part.shape[0]):
        sent = got.at[slot, :, rows_of(slot)]
        pltpu.make_async_copy(sent, sent, send_sem.at[slot]).wait()


def per_device(n_tm, n_as, values, listed_from, listed_until):
    fields, rows, assets = values.shape
    blocks = rows // WINDOW
    groups = field_groups(fields)
    own = groups[0][1]
    stats = -(-max(own * blocks, blocks + 2, 2 * own) // SUBLANES) * SUBLANES
    slots = 1 + 2 * len(groups) + 2
    cuts = len(halo_pieces(fields, assets // LANES))
    f32 = jnp.float32
    vmem = pltpu.VMEM
    dma = pltpu.SemaphoreType.DMA
    return pl.pallas_call(
        functools.partial(kernel, n_tm, n_as),
        out_shape=vmem((fields, rows, assets), f32),
        in_specs=[pl.BlockSpec(memory_space=pltpu.HBM)] * 3,
        out_specs=pl.BlockSpec(memory_space=vmem),
        scratch_shapes=[
            vmem((fields, WINDOW + rows + WINDOW, assets + LANES), f32),
            vmem((fields, rows + WINDOW, assets + LANES), f32),
            vmem((WINDOW + rows + WINDOW, assets + LANES), f32),
            vmem((WINDOW + rows + WINDOW, assets + LANES), f32),
            vmem((1, assets), jnp.int32),
            vmem((1, assets), jnp.int32),
            vmem((stats + 2 * own, LANES, LANES), f32),
            vmem((stats + 2 * own, LANES, LANES), f32),
            vmem((slots, stats, LANES), f32),
            vmem((slots, n_as - 1, stats, LANES), f32),
            vmem((slots, stats, LANES), f32),
            vmem((len(groups) + 1, stats, LANES), f32),
            vmem((stats, LANES), f32),
            vmem((stats, LANES), f32),
            dma((fields + 2,)),
            dma((cuts,)),
            dma((cuts,)),
            dma((own,)),
            dma((own,)),
            dma((2,)),
            dma((slots,)),
            dma((slots,)),
            pltpu.SemaphoreType.REGULAR((max(greeting_rounds(n_as), 1),)),
        ],
        compiler_params=pltpu.CompilerParams(
            collective_id=0, has_side_effects=True, vmem_limit_bytes=48 * 2**20
        ),
    )(values, listed_from[None], listed_until[None])


def solution(mesh):
    in_specs = (P(None, "tm", "asset"), P("asset"), P("asset"))
    out_specs = P(None, "tm", "asset")
    body = functools.partial(per_device, mesh.shape["tm"], mesh.shape["asset"])
    return jax.shard_map(
        body, mesh=mesh, in_specs=in_specs, out_specs=out_specs, check_vma=False
    )
```

```python
import functools

import jax
import jax.numpy as jnp
from jax import lax
from jax.experimental import pallas as pl
from jax.experimental.pallas import tpu as pltpu
from jax.sharding import PartitionSpec as P

WINDOW = 64
LANES = 128
SUBLANES = 8
CLIP = 3.0
ROLL_UNROLL = 4
UNROLL = 4
HELD = 0
CUTS = 4


def field_groups(fields):
    half = (fields + 1) // 2
    return [(start, min(half, fields - start)) for start in range(0, fields, half)]


def lane_pieces(chunks, cuts):
    if cuts and chunks % cuts == 0:
        size = chunks // cuts
        return [(c * size, size) for c in range(cuts)]
    if cuts:
        return [(0, chunks)]
    pieces, first = [], 0
    while first < chunks:
        size = max((chunks - first) // 2, 1)
        pieces.append((first, size))
        first += size
    return pieces


def halo_pieces(fields, own, chunks):
    cuts = [CUTS if f == own - 1 else 1 for f in range(fields)]
    if fields > own:
        cuts[fields - 1] = 0
    return [(f, *piece) for f in range(fields) for piece in lane_pieces(chunks, cuts[f])]


def back_pieces(fields, own, chunks):
    cuts = [CUTS if f == fields - 1 else 1 for f in range(fields)]
    return [(f, *piece) for f in range(own, fields) for piece in lane_pieces(chunks, cuts[f])]


def greeting_rounds(n):
    if n % 2:
        return 0
    return max(n // 2 - 1, 0)


def kernel(
    n_tm, n_as, values, opened_hbm, closed_hbm, out,
    x, rolling, weight, inverse, opened_ref, closed_ref,
    acc, columns_of, part, got, totals, counts, advice, advised,
    load_sem, halo_send, halo_recv, back_send, back_recv, advice_send, advice_recv, send_sem, recv_sem, hello,
):
    fields, rows, assets = values.shape
    blocks = rows // WINDOW
    chunks = assets // LANES
    tiles = WINDOW // SUBLANES
    groups = field_groups(fields)
    own = groups[0][1]
    helped = fields - own
    stats = part.shape[1]
    tail = 1 + 2 * len(groups)
    last = len(groups)
    tm = lax.axis_index("tm")
    me = lax.axis_index("asset")
    later = lax.rem(tm + 1, n_tm)
    before = lax.rem(tm + n_tm - 1, n_tm)
    has_next = tm < n_tm - 1
    has_prev = tm > 0

    dates = [
        pltpu.make_async_copy(opened_hbm, opened_ref, load_sem.at[fields]),
        pltpu.make_async_copy(closed_hbm, closed_ref, load_sem.at[fields + 1]),
    ]
    loads = [
        pltpu.make_async_copy(
            values.at[f], x.at[f, pl.ds(WINDOW, rows), pl.ds(0, assets)], load_sem.at[f]
        )
        for f in range(fields)
    ]

    barrier = pltpu.get_barrier_semaphore()
    rounds = greeting_rounds(n_as)

    @pl.when(has_next)
    def _():
        pl.semaphore_signal(barrier, inc=1, device_id={"tm": later})

    @pl.when(has_prev)
    def _():
        pl.semaphore_signal(barrier, inc=1, device_id={"tm": before})

    def greet(semaphore):
        if n_as % 2:
            for d in range(1, n_as):
                pl.semaphore_signal(semaphore, inc=1, device_id={"asset": lax.rem(me + d, n_as)})
            return n_as - 1
        beside = me + 1 - 2 * lax.rem(me, 2)
        pl.semaphore_signal(semaphore, inc=1, device_id={"asset": beside})

        @pl.when(me >= 2)
        def _():
            pl.semaphore_signal(semaphore, inc=1, device_id={"asset": me - 2})

        @pl.when(me + 2 < n_as)
        def _():
            pl.semaphore_signal(semaphore, inc=1, device_id={"asset": me + 2})

        return 1 + jnp.where(me >= 2, 1, 0) + jnp.where(me + 2 < n_as, 1, 0)

    near = greet(barrier)
    expected = near + jnp.where(has_next, 1, 0) + jnp.where(has_prev, 1, 0)
    for copy in dates + loads:
        copy.start()

    landing = {f: [] for f in range(fields)}
    halos = []
    for i, (f, first, size) in enumerate(halo_pieces(fields, own, chunks)):
        cols = pl.ds(first * LANES, size * LANES)
        halos.append(pltpu.make_async_remote_copy(
            src_ref=values.at[f, pl.ds(rows - WINDOW, WINDOW), cols],
            dst_ref=x.at[f, pl.ds(0, WINDOW), cols],
            send_sem=halo_send.at[i],
            recv_sem=halo_recv.at[i],
            device_id={"tm": later},
        ))
        landing[f].append((halos[-1], first, size))
    returning = {f: [] for f in range(own, fields)}
    backs = []
    for i, (f, first, size) in enumerate(back_pieces(fields, own, chunks)):
        cols = pl.ds(first * LANES, size * LANES)
        backs.append(pltpu.make_async_remote_copy(
            src_ref=values.at[f, pl.ds(0, WINDOW), cols],
            dst_ref=x.at[f, pl.ds(WINDOW + rows, WINDOW), cols],
            send_sem=back_send.at[i],
            recv_sem=back_recv.at[i],
            device_id={"tm": before},
        ))
        returning[f].append((backs[-1], first, size))
    advising = [
        pltpu.make_async_remote_copy(
            src_ref=advice.at[u],
            dst_ref=advised.at[u],
            send_sem=advice_send.at[u],
            recv_sem=advice_recv.at[u],
            device_id={"tm": later},
        )
        for u in range(helped)
    ]
    free = len(halos) - min(HELD, len(landing[fields - 1]) - 1)
    odd = lax.rem(tm, 2) == 1

    def rows_of(slot):
        return pl.ds(0, 2 if slot >= tail else stats)

    def send(slot):
        for d in range(1, n_as):
            pltpu.make_async_remote_copy(
                src_ref=part.at[slot, rows_of(slot)],
                dst_ref=got.at[slot, d - 1, rows_of(slot)],
                send_sem=send_sem.at[slot],
                recv_sem=recv_sem.at[slot],
                device_id={"asset": lax.rem(me + d, n_as)},
            ).start()

    def receive(slot):
        arrived = got.at[slot, :, rows_of(slot)]
        pltpu.make_async_copy(arrived, arrived, recv_sem.at[slot]).wait()
        totals[slot] = part[slot] + jnp.sum(got[slot], axis=0)

    def columns(c):
        return pl.ds(pl.multiple_of(c * LANES, LANES), LANES)

    def reduce_items(slot, items, first=0):
        for i in range(items):
            part[slot, i:i + 1, :] = jnp.sum(acc[first + i].T, axis=0, keepdims=True)

    def spread_items(sums, count, items, first=0):
        mean = sums / count
        other = pltpu.roll(mean, WINDOW, 1)
        scale = 1.0 / jnp.sqrt(jnp.maximum(mean - other * other, 0.0) + 0.1)
        lane = lax.broadcasted_iota(jnp.int32, mean.shape, 1)
        row = jnp.where(lane < WINDOW, mean, scale)
        for i in range(items):
            columns_of[first + i] = jnp.broadcast_to(row[i:i + 1], (LANES, LANES)).T

    def column_pair(i):
        return columns_of[i, :WINDOW, :], columns_of[i, WINDOW:, :]

    pl.semaphore_wait(barrier, expected)

    @pl.when(has_prev & ~odd)
    def _():
        for copy in backs:
            copy.start()

    @pl.when(has_next)
    def _():
        for copy in halos[:free]:
            copy.start()

    @pl.when(has_prev & odd)
    def _():
        for copy in backs:
            copy.start()

    zero = jnp.zeros((WINDOW, LANES), jnp.float32)
    first_stamp = tm * rows - WINDOW

    def start_listing():
        part[...] = jnp.zeros(part.shape, part.dtype)
        acc[...] = jnp.zeros(acc.shape, acc.dtype)
        for copy in dates:
            copy.wait()

        @pl.when(tm == 0)
        def _():
            @pl.loop(0, fields)
            def clear(f):
                x[f, pl.ds(0, WINDOW), pl.ds(0, assets)] = jnp.zeros((WINDOW, assets), jnp.float32)

    def listing(b):
        start = pl.multiple_of(b * WINDOW, WINDOW)
        row = lax.broadcasted_iota(jnp.int32, (WINDOW, LANES), 0)
        passed = (first_stamp + start + 1 + row).astype(jnp.float32)

        def chunk(c, total):
            cols = columns(c)
            opened = jnp.maximum(opened_ref[:, cols], 0).astype(jnp.float32)
            closed = closed_ref[:, cols].astype(jnp.float32)
            age = passed - opened
            listed = (age > 0.0) & (passed <= closed)
            ones = jnp.where(listed, 1.0, 0.0)
            weight[pl.ds(start, WINDOW), cols] = ones
            counted = jnp.minimum(jnp.maximum(age, 1.0), float(WINDOW))
            inverse[pl.ds(start, WINDOW), cols] = ones / counted
            return total + ones

        total = lax.fori_loop(0, chunks, chunk, zero, unroll=2)
        at = lax.rem(b + blocks + 1, blocks + 2)
        acc[at, :WINDOW, :] = total
        acc[at, WINDOW:, :] = total

    def listing_blocks(low, high):
        pl.loop(low, high)(listing)

    ahead = min(2, blocks)

    for r in range(rounds):
        greet(hello.at[r])
        if r == 0:
            start_listing()
            listing_blocks(0, ahead)
        if r == 1:
            listing_blocks(ahead, blocks)
        if r == 2:
            listing_blocks(blocks, blocks + 2)
        if r < rounds - 1:
            pl.semaphore_wait(hello.at[r], near)
    if rounds < 1:
        start_listing()
        listing_blocks(0, ahead)
    if rounds < 2:
        listing_blocks(ahead, blocks)
    if rounds < 3:
        listing_blocks(blocks, blocks + 2)
    reduce_items(0, blocks + 1)

    def window_means(f, b, c):
        top = pl.multiple_of(b * WINDOW, WINDOW)
        cols = columns(c)
        sublane = lax.broadcasted_iota(jnp.int32, (SUBLANES, LANES), 0)

        ends = range(2 * tiles)
        reach = pl.ds(top, 2 * WINDOW)
        masked = x[f, reach, cols] * weight[reach, cols]
        sums = {j: masked[SUBLANES * j:SUBLANES * (j + 1)] for j in ends}
        step = 1
        while step < tiles:
            sums = {j: sums[j] + sums[j - step] for j in ends if j - step in sums}
            step *= 2
        shift = 1
        while shift < SUBLANES:
            keep = sublane < SUBLANES - shift
            moved = {tiles - 1: sums[tiles - 1]}
            for j in range(tiles, 2 * tiles):
                moved[j] = jnp.where(keep, sums[j], sums[j - 1])
            sums = {j: sums[j] + pltpu.roll(moved[j], shift, 0) for j in moved}
            shift *= 2
        ending = jnp.concatenate([sums[j] for j in range(tiles, 2 * tiles)], axis=0)
        return ending * inverse[pl.ds(top + WINDOW, WINDOW), cols]

    def roll_window(f, b, i, low=0, size=chunks):
        top = pl.multiple_of(b * WINDOW, WINDOW)

        def chunk(c, carry):
            means = window_means(f, b, c)
            rolling[f, pl.ds(top, WINDOW), columns(c)] = means
            return carry[0] + means, carry[1] + means * means

        carry = (zero, zero) if low == 0 else (acc[i, :WINDOW, :], acc[i, WINDOW:, :])
        first, second = lax.fori_loop(
            low, low + size, chunk, carry, unroll=min(ROLL_UNROLL, size)
        )
        acc[i, :WINDOW, :] = first
        acc[i, WINDOW:, :] = second

    def clip_scores(f, b, i):
        top = pl.multiple_of(b * WINDOW, WINDOW)
        center, scale = column_pair(i)

        def chunk(c, carry):
            cols = columns(c)
            here = pl.ds(top, WINDOW)
            scored = (rolling[f, here, cols] - center) * scale
            clipped = jnp.minimum(jnp.maximum(scored, -CLIP), CLIP)
            rolling[f, here, cols] = clipped
            masked = clipped * weight[pl.ds(top + WINDOW, WINDOW), cols]
            return carry[0] + masked, carry[1] + masked * clipped

        first, second = lax.fori_loop(0, chunks, chunk, (zero, zero), unroll=UNROLL)
        acc[i, :WINDOW, :] = first
        acc[i, WINDOW:, :] = second

    def finish(f, b, i):
        top = pl.multiple_of(b * WINDOW, WINDOW)
        middle, factor = column_pair(i)

        @pl.loop(0, chunks, unroll=UNROLL)
        def chunk(c):
            cols = columns(c)
            here = pl.ds(top, WINDOW)
            deviate = (rolling[f, here, cols] - middle) * weight[pl.ds(top + WINDOW, WINDOW), cols]
            out[f, here, cols] = deviate * factor

    def standardized(means, cols, first, second):
        center, scale = first
        middle, factor = second
        clipped = jnp.minimum(jnp.maximum((means - center) * scale, -CLIP), CLIP)
        return (clipped - middle) * weight[WINDOW:2 * WINDOW, cols] * factor

    def roll_only(f, low, size):
        @pl.loop(low, low + size, unroll=min(2, size))
        def chunk(c):
            rolling[f, :WINDOW, columns(c)] = window_means(f, 0, c)

    def score_finish(f, low, size, i):
        first, second = column_pair(i), column_pair(i + 1)

        @pl.loop(low, low + size, unroll=min(UNROLL, size))
        def chunk(c):
            cols = columns(c)
            out[f, :WINDOW, cols] = standardized(rolling[f, :WINDOW, cols], cols, first, second)

    def roll_finish(f, low, size, i):
        first, second = column_pair(i), column_pair(i + 1)

        @pl.loop(low, low + size, unroll=min(2, size))
        def chunk(c):
            cols = columns(c)
            out[f, :WINDOW, cols] = standardized(window_means(f, 0, c), cols, first, second)

    def main_items(g):
        size = groups[g][1]
        return pl.loop(jnp.where(tm == 0, 0, size), size * blocks)

    def main_first(g):
        start, size = groups[g]
        for f in range(start, start + size):
            loads[f].wait()

        @main_items(g)
        def item(i):
            roll_window(start + lax.rem(i, size), lax.div(i, size), i)

        reduce_items(1 + 2 * g, size * blocks)
        if g == 0:
            if rounds:
                pl.semaphore_wait(hello.at[rounds - 1], near)
            send(0)
        send(1 + 2 * g)

    def main_counts(g):
        size = groups[g][1]
        for i in range(size * blocks):
            b = i // size
            counts[g, i:i + 1, :] = jnp.maximum(totals[0, b:b + 1, :], 1.0)

    def main_second(g):
        start, size = groups[g]
        slot = 1 + 2 * g
        receive(slot)
        spread_items(totals[slot], counts[g], size * blocks)

        @main_items(g)
        def item(i):
            clip_scores(start + lax.rem(i, size), lax.div(i, size), i)

        reduce_items(slot + 1, size * blocks)
        send(slot + 1)

    def main_third(g):
        start, size = groups[g]
        slot = 2 + 2 * g
        receive(slot)
        spread_items(totals[slot], counts[g], size * blocks)

        @main_items(g)
        def item(i):
            finish(start + lax.rem(i, size), lax.div(i, size), i)

    def tail_own(u):
        for copy, low, size in landing[u]:
            copy.wait_recv()
            roll_window(u, 0, stats + 2 * u, low, size)

    def tail_help(u):
        for copy, low, size in returning[own + u]:
            copy.wait_recv()
            roll_window(own + u, blocks, stats + 2 * u + 1, low, size)

    def tail_first(u):
        pl.when(has_prev & odd)(functools.partial(tail_own, u))
        if u < helped:
            pl.when(has_next)(functools.partial(tail_help, u))
        pl.when(has_prev & ~odd)(functools.partial(tail_own, u))

    def tail_second(u):
        @pl.when(has_prev)
        def _():
            clip_scores(u, 0, stats + 2 * u)

        if u < helped:
            @pl.when(has_next)
            def _():
                clip_scores(own + u, blocks, stats + 2 * u + 1)

    def tail_exchange(u):
        reduce_items(tail + 2 * u, 2, stats + 2 * u)
        send(tail + 2 * u)

    def tail_scores(u):
        slot = tail + 2 * u
        receive(slot)
        spread_items(totals[slot], counts[last], 2, stats + 2 * u)
        tail_second(u)
        reduce_items(slot + 1, 2, stats + 2 * u)
        send(slot + 1)

    def tail_last(u):
        slot = tail + 2 * u
        receive(slot + 1)
        if u < helped:
            advice[u, :1, :] = totals[slot, 1:2, :]
            advice[u, 1:2, :] = totals[slot + 1, 1:2, :]

            @pl.when(has_next)
            def _():
                advising[u].start()

        @pl.when(has_prev)
        def _():
            spread_items(totals[slot + 1], counts[last], 1, stats + 2 * u)
            finish(u, 0, stats + 2 * u)

    def split_pieces(f):
        held = len(halos) - free if f == fields - 1 else 0
        return landing[f][:len(landing[f]) - held], landing[f][len(landing[f]) - held:]

    def last_rolls(u):
        for copy, low, size in split_pieces(own + u)[0]:
            copy.wait_recv()
            roll_only(own + u, low, size)

    def last_fields():
        count = jnp.broadcast_to(counts[last, :1, :], advised.shape[1:])
        for u in range(helped):
            advising[u].wait_recv()
            spread_items(advised[u], count, 2, 2 * u)
        for u in range(helped):
            rolled, landed = split_pieces(own + u)
            score_finish(own + u, 0, sum(size for _, _, size in rolled), 2 * u)
            for copy, low, size in landed:
                copy.wait_recv()
                roll_finish(own + u, low, size, 2 * u)

    late = own - 1
    for g in range(len(groups)):
        main_first(g)
    for u in range(late):
        tail_first(u)
        tail_exchange(u)

    @pl.when(tm == 0)
    def _():
        tail_first(late)
        tail_exchange(late)

    receive(0)
    for i in range(2):
        b = 0 if i == 0 else blocks
        counts[last, i:i + 1, :] = jnp.maximum(totals[0, b:b + 1, :], 1.0)
    main_counts(0)
    main_second(0)

    @pl.when(has_prev)
    def _():
        tail_first(late)
        tail_exchange(late)

    for g in range(1, len(groups)):
        main_counts(g)
        main_second(g)
    for u in range(late):
        tail_scores(u)

    @pl.when(tm == 0)
    def _():
        tail_scores(late)

    for g in range(len(groups) - 1):
        main_third(g)

    @pl.when(has_prev)
    def _():
        tail_scores(late)

    @pl.when(has_prev)
    def _():
        main_third(len(groups) - 1)

    for u in range(late):
        tail_last(u)

    @pl.when(has_prev)
    def _():
        for u in range(helped - 1):
            last_rolls(u)

    tail_last(late)

    @pl.when(has_next)
    def _():
        for copy in halos[free:]:
            copy.start()

    @pl.when(tm == 0)
    def _():
        main_third(len(groups) - 1)

    @pl.when(has_prev)
    def _():
        for u in range(helped - 1, helped):
            last_rolls(u)
        last_fields()

    @pl.when(has_prev)
    def _():
        for copy in backs:
            copy.wait_send()

    @pl.when(has_next)
    def _():
        for copy in advising + halos:
            copy.wait_send()

    for slot in range(part.shape[0]):
        sent = got.at[slot, :, rows_of(slot)]
        pltpu.make_async_copy(sent, sent, send_sem.at[slot]).wait()


def per_device(n_tm, n_as, values, listed_from, listed_until):
    fields, rows, assets = values.shape
    blocks = rows // WINDOW
    groups = field_groups(fields)
    own = groups[0][1]
    stats = -(-max(own * blocks, blocks + 2) // SUBLANES) * SUBLANES
    slots = 1 + 2 * len(groups) + 2 * own
    cuts = len(halo_pieces(fields, own, assets // LANES))
    back_cuts = max(len(back_pieces(fields, own, assets // LANES)), 1)
    f32 = jnp.float32
    vmem = pltpu.VMEM
    dma = pltpu.SemaphoreType.DMA
    return pl.pallas_call(
        functools.partial(kernel, n_tm, n_as),
        out_shape=vmem((fields, rows, assets), f32),
        in_specs=[pl.BlockSpec(memory_space=pltpu.HBM)] * 3,
        out_specs=pl.BlockSpec(memory_space=vmem),
        scratch_shapes=[
            vmem((fields, WINDOW + rows + WINDOW, assets + LANES), f32),
            vmem((fields, rows + WINDOW, assets + LANES), f32),
            vmem((WINDOW + rows + WINDOW, assets + LANES), f32),
            vmem((WINDOW + rows + WINDOW, assets + LANES), f32),
            vmem((1, assets), jnp.int32),
            vmem((1, assets), jnp.int32),
            vmem((stats + 2 * own, LANES, LANES), f32),
            vmem((stats + 2 * own, LANES, LANES), f32),
            vmem((slots, stats, LANES), f32),
            vmem((slots, n_as - 1, stats, LANES), f32),
            vmem((slots, stats, LANES), f32),
            vmem((len(groups) + 1, stats, LANES), f32),
            vmem((own, SUBLANES, LANES), f32),
            vmem((own, SUBLANES, LANES), f32),
            dma((fields + 2,)),
            dma((cuts,)),
            dma((cuts,)),
            dma((back_cuts,)),
            dma((back_cuts,)),
            dma((own,)),
            dma((own,)),
            dma((slots,)),
            dma((slots,)),
            pltpu.SemaphoreType.REGULAR((max(greeting_rounds(n_as), 1),)),
        ],
        compiler_params=pltpu.CompilerParams(
            collective_id=0, has_side_effects=True, vmem_limit_bytes=48 * 2**20
        ),
    )(values, listed_from[None], listed_until[None])


def solution(mesh):
    in_specs = (P(None, "tm", "asset"), P("asset"), P("asset"))
    out_specs = P(None, "tm", "asset")
    body = functools.partial(per_device, mesh.shape["tm"], mesh.shape["asset"])
    return jax.shard_map(
        body, mesh=mesh, in_specs=in_specs, out_specs=out_specs, check_vma=False
    )
```

```python
import functools

import jax
import jax.numpy as jnp
from jax import lax
from jax.experimental import pallas as pl
from jax.experimental.pallas import tpu as pltpu
from jax.sharding import PartitionSpec as P

WINDOW = 64
LANES = 128
SUBLANES = 8
CLIP = 3.0
ROLL_UNROLL = 4
UNROLL = 4
CUTS = 4


def field_groups(fields):
    half = (fields + 1) // 2
    return [(start, min(half, fields - start)) for start in range(0, fields, half)]


def lane_pieces(chunks, cuts):
    if cuts and chunks % cuts == 0:
        size = chunks // cuts
        return [(c * size, size) for c in range(cuts)]
    if cuts:
        return [(0, chunks)]
    pieces, first = [], 0
    while first < chunks:
        size = max((chunks - first) // 2, 1)
        pieces.append((first, size))
        first += size
    return pieces


def halo_pieces(fields, own, chunks):
    cuts = [CUTS if f == own - 1 else 1 for f in range(fields)]
    if fields > own:
        cuts[fields - 1] = 0
    return [(f, *piece) for f in range(fields) for piece in lane_pieces(chunks, cuts[f])]


def back_pieces(fields, own, chunks):
    cuts = [CUTS if f == fields - 1 else 1 for f in range(fields)]
    return [(f, *piece) for f in range(own, fields) for piece in lane_pieces(chunks, cuts[f])]


def greeting_rounds(n):
    if n % 2:
        return 0
    return max(n // 2 - 1, 0)


def spread(columns_of, sums, count, items, first=0):
    mean = sums / count
    other = pltpu.roll(mean, WINDOW, 1)
    scale = 1.0 / jnp.sqrt(jnp.maximum(mean - other * other, 0.0) + 0.1)
    lane = lax.broadcasted_iota(jnp.int32, mean.shape, 1)
    row = jnp.where(lane < WINDOW, mean, scale)
    for i in range(items):
        columns_of[first + i] = jnp.broadcast_to(row[i:i + 1], (LANES, LANES)).T


def chunk_columns(c):
    return pl.ds(pl.multiple_of(c * LANES, LANES), LANES)


def kernel(
    n_tm, n_as, values, opened_hbm, closed_hbm,
    out, rolled, head_weight, advised, head_count,
    x, rolling, weight, inverse, opened_ref, closed_ref,
    acc, columns_of, part, got, totals, counts, advice,
    load_sem, halo_send, halo_recv, back_send, back_recv, advice_send, advice_recv, send_sem, recv_sem, hello,
):
    fields, rows, assets = values.shape
    blocks = rows // WINDOW
    chunks = assets // LANES
    tiles = WINDOW // SUBLANES
    groups = field_groups(fields)
    own = groups[0][1]
    helped = fields - own
    stats = part.shape[1]
    tail = 1 + 2 * len(groups)
    last = len(groups)
    tm = lax.axis_index("tm")
    me = lax.axis_index("asset")
    later = lax.rem(tm + 1, n_tm)
    before = lax.rem(tm + n_tm - 1, n_tm)
    has_next = tm < n_tm - 1
    has_prev = tm > 0

    dates = [
        pltpu.make_async_copy(opened_hbm, opened_ref, load_sem.at[fields]),
        pltpu.make_async_copy(closed_hbm, closed_ref, load_sem.at[fields + 1]),
    ]
    loads = [
        pltpu.make_async_copy(
            values.at[f], x.at[f, pl.ds(WINDOW, rows), pl.ds(0, assets)], load_sem.at[f]
        )
        for f in range(fields)
    ]

    barrier = pltpu.get_barrier_semaphore()
    rounds = greeting_rounds(n_as)

    @pl.when(has_next)
    def _():
        pl.semaphore_signal(barrier, inc=1, device_id={"tm": later})

    @pl.when(has_prev)
    def _():
        pl.semaphore_signal(barrier, inc=1, device_id={"tm": before})

    def greet(semaphore):
        if n_as % 2:
            for d in range(1, n_as):
                pl.semaphore_signal(semaphore, inc=1, device_id={"asset": lax.rem(me + d, n_as)})
            return n_as - 1
        beside = me + 1 - 2 * lax.rem(me, 2)
        pl.semaphore_signal(semaphore, inc=1, device_id={"asset": beside})

        @pl.when(me >= 2)
        def _():
            pl.semaphore_signal(semaphore, inc=1, device_id={"asset": me - 2})

        @pl.when(me + 2 < n_as)
        def _():
            pl.semaphore_signal(semaphore, inc=1, device_id={"asset": me + 2})

        return 1 + jnp.where(me >= 2, 1, 0) + jnp.where(me + 2 < n_as, 1, 0)

    near = greet(barrier)
    expected = near + jnp.where(has_next, 1, 0) + jnp.where(has_prev, 1, 0)
    for copy in dates + loads:
        copy.start()

    landing = {f: [] for f in range(fields)}
    halos = []
    for i, (f, first, size) in enumerate(halo_pieces(fields, own, chunks)):
        cols = pl.ds(first * LANES, size * LANES)
        halos.append(pltpu.make_async_remote_copy(
            src_ref=values.at[f, pl.ds(rows - WINDOW, WINDOW), cols],
            dst_ref=x.at[f, pl.ds(0, WINDOW), cols],
            send_sem=halo_send.at[i],
            recv_sem=halo_recv.at[i],
            device_id={"tm": later},
        ))
        landing[f].append((halos[-1], first, size))
    returning = {f: [] for f in range(own, fields)}
    backs = []
    for i, (f, first, size) in enumerate(back_pieces(fields, own, chunks)):
        cols = pl.ds(first * LANES, size * LANES)
        backs.append(pltpu.make_async_remote_copy(
            src_ref=values.at[f, pl.ds(0, WINDOW), cols],
            dst_ref=x.at[f, pl.ds(WINDOW + rows, WINDOW), cols],
            send_sem=back_send.at[i],
            recv_sem=back_recv.at[i],
            device_id={"tm": before},
        ))
        returning[f].append((backs[-1], first, size))
    advising = [
        pltpu.make_async_remote_copy(
            src_ref=advice.at[u],
            dst_ref=advised.at[u],
            send_sem=advice_send.at[u],
            recv_sem=advice_recv.at[u],
            device_id={"tm": later},
        )
        for u in range(helped)
    ]
    odd = lax.rem(tm, 2) == 1

    def rows_of(slot):
        return pl.ds(0, 2 if slot >= tail else stats)

    def send(slot):
        for d in range(1, n_as):
            pltpu.make_async_remote_copy(
                src_ref=part.at[slot, rows_of(slot)],
                dst_ref=got.at[slot, d - 1, rows_of(slot)],
                send_sem=send_sem.at[slot],
                recv_sem=recv_sem.at[slot],
                device_id={"asset": lax.rem(me + d, n_as)},
            ).start()

    def receive(slot):
        arrived = got.at[slot, :, rows_of(slot)]
        pltpu.make_async_copy(arrived, arrived, recv_sem.at[slot]).wait()
        totals[slot] = part[slot] + jnp.sum(got[slot], axis=0)

    def reduce_items(slot, items, first=0):
        for i in range(items):
            part[slot, i:i + 1, :] = jnp.sum(acc[first + i].T, axis=0, keepdims=True)

    def spread_items(sums, count, items, first=0):
        spread(columns_of, sums, count, items, first)

    def column_pair(i):
        return columns_of[i, :WINDOW, :], columns_of[i, WINDOW:, :]

    pl.semaphore_wait(barrier, expected)

    @pl.when(has_prev & ~odd)
    def _():
        for copy in backs:
            copy.start()

    @pl.when(has_next)
    def _():
        for copy in halos:
            copy.start()

    @pl.when(has_prev & odd)
    def _():
        for copy in backs:
            copy.start()

    zero = jnp.zeros((WINDOW, LANES), jnp.float32)
    first_stamp = tm * rows - WINDOW

    def start_listing():
        part[...] = jnp.zeros(part.shape, part.dtype)
        acc[...] = jnp.zeros(acc.shape, acc.dtype)
        for copy in dates:
            copy.wait()

        @pl.when(tm == 0)
        def _():
            @pl.loop(0, fields)
            def clear(f):
                x[f, pl.ds(0, WINDOW), pl.ds(0, assets)] = jnp.zeros((WINDOW, assets), jnp.float32)

    def listing(b):
        start = pl.multiple_of(b * WINDOW, WINDOW)
        row = lax.broadcasted_iota(jnp.int32, (WINDOW, LANES), 0)
        passed = (first_stamp + start + 1 + row).astype(jnp.float32)

        def chunk(c, total):
            cols = chunk_columns(c)
            opened = jnp.maximum(opened_ref[:, cols], 0).astype(jnp.float32)
            closed = closed_ref[:, cols].astype(jnp.float32)
            age = passed - opened
            listed = (age > 0.0) & (passed <= closed)
            ones = jnp.where(listed, 1.0, 0.0)
            weight[pl.ds(start, WINDOW), cols] = ones
            counted = jnp.minimum(jnp.maximum(age, 1.0), float(WINDOW))
            inverse[pl.ds(start, WINDOW), cols] = ones / counted
            return total + ones

        total = lax.fori_loop(0, chunks, chunk, zero, unroll=2)
        at = lax.rem(b + blocks + 1, blocks + 2)
        acc[at, :WINDOW, :] = total
        acc[at, WINDOW:, :] = total

    def listing_blocks(low, high):
        pl.loop(low, high)(listing)

    ahead = min(2, blocks)

    for r in range(rounds):
        greet(hello.at[r])
        if r == 0:
            start_listing()
            listing_blocks(0, ahead)
        if r == 1:
            listing_blocks(ahead, blocks)
        if r == 2:
            listing_blocks(blocks, blocks + 2)
        if r < rounds - 1:
            pl.semaphore_wait(hello.at[r], near)
    if rounds < 1:
        start_listing()
        listing_blocks(0, ahead)
    if rounds < 2:
        listing_blocks(ahead, blocks)
    if rounds < 3:
        listing_blocks(blocks, blocks + 2)
    reduce_items(0, blocks + 1)

    def window_means(f, b, c):
        top = pl.multiple_of(b * WINDOW, WINDOW)
        cols = chunk_columns(c)
        sublane = lax.broadcasted_iota(jnp.int32, (SUBLANES, LANES), 0)

        ends = range(2 * tiles)
        reach = pl.ds(top, 2 * WINDOW)
        masked = x[f, reach, cols] * weight[reach, cols]
        sums = {j: masked[SUBLANES * j:SUBLANES * (j + 1)] for j in ends}
        step = 1
        while step < tiles:
            sums = {j: sums[j] + sums[j - step] for j in ends if j - step in sums}
            step *= 2
        shift = 1
        while shift < SUBLANES:
            keep = sublane < SUBLANES - shift
            moved = {tiles - 1: sums[tiles - 1]}
            for j in range(tiles, 2 * tiles):
                moved[j] = jnp.where(keep, sums[j], sums[j - 1])
            sums = {j: sums[j] + pltpu.roll(moved[j], shift, 0) for j in moved}
            shift *= 2
        ending = jnp.concatenate([sums[j] for j in range(tiles, 2 * tiles)], axis=0)
        return ending * inverse[pl.ds(top + WINDOW, WINDOW), cols]

    def roll_window(f, b, i, low=0, size=chunks):
        top = pl.multiple_of(b * WINDOW, WINDOW)

        def chunk(c, carry):
            means = window_means(f, b, c)
            rolling[f, pl.ds(top, WINDOW), chunk_columns(c)] = means
            return carry[0] + means, carry[1] + means * means

        carry = (zero, zero) if low == 0 else (acc[i, :WINDOW, :], acc[i, WINDOW:, :])
        first, second = lax.fori_loop(
            low, low + size, chunk, carry, unroll=min(ROLL_UNROLL, size)
        )
        acc[i, :WINDOW, :] = first
        acc[i, WINDOW:, :] = second

    def clip_scores(f, b, i):
        top = pl.multiple_of(b * WINDOW, WINDOW)
        center, scale = column_pair(i)

        def chunk(c, carry):
            cols = chunk_columns(c)
            here = pl.ds(top, WINDOW)
            scored = (rolling[f, here, cols] - center) * scale
            clipped = jnp.minimum(jnp.maximum(scored, -CLIP), CLIP)
            rolling[f, here, cols] = clipped
            masked = clipped * weight[pl.ds(top + WINDOW, WINDOW), cols]
            return carry[0] + masked, carry[1] + masked * clipped

        first, second = lax.fori_loop(0, chunks, chunk, (zero, zero), unroll=UNROLL)
        acc[i, :WINDOW, :] = first
        acc[i, WINDOW:, :] = second

    def finish(f, b, i):
        top = pl.multiple_of(b * WINDOW, WINDOW)
        middle, factor = column_pair(i)

        @pl.loop(0, chunks, unroll=UNROLL)
        def chunk(c):
            cols = chunk_columns(c)
            here = pl.ds(top, WINDOW)
            deviate = (rolling[f, here, cols] - middle) * weight[pl.ds(top + WINDOW, WINDOW), cols]
            out[f, here, cols] = deviate * factor

    def roll_only(u, low, size):
        @pl.loop(low, low + size, unroll=min(2, size))
        def chunk(c):
            cols = chunk_columns(c)
            rolled[u, :, cols] = window_means(own + u, 0, c)
            if u == 0:
                head_weight[:, cols] = weight[WINDOW:2 * WINDOW, cols]

    def main_items(g):
        size = groups[g][1]
        return pl.loop(jnp.where(tm == 0, 0, size), size * blocks)

    def main_first(g):
        start, size = groups[g]
        for f in range(start, start + size):
            loads[f].wait()

        @main_items(g)
        def item(i):
            roll_window(start + lax.rem(i, size), lax.div(i, size), i)

        reduce_items(1 + 2 * g, size * blocks)
        if g == 0:
            if rounds:
                pl.semaphore_wait(hello.at[rounds - 1], near)
            send(0)
        send(1 + 2 * g)

    def main_counts(g):
        size = groups[g][1]
        for i in range(size * blocks):
            b = i // size
            counts[g, i:i + 1, :] = jnp.maximum(totals[0, b:b + 1, :], 1.0)

    def main_second(g):
        start, size = groups[g]
        slot = 1 + 2 * g
        receive(slot)
        spread_items(totals[slot], counts[g], size * blocks)

        @main_items(g)
        def item(i):
            clip_scores(start + lax.rem(i, size), lax.div(i, size), i)

        reduce_items(slot + 1, size * blocks)
        send(slot + 1)

    def main_third(g):
        start, size = groups[g]
        slot = 2 + 2 * g
        receive(slot)
        spread_items(totals[slot], counts[g], size * blocks)

        @main_items(g)
        def item(i):
            finish(start + lax.rem(i, size), lax.div(i, size), i)

    def tail_own(u):
        for copy, low, size in landing[u]:
            copy.wait_recv()
            roll_window(u, 0, stats + 2 * u, low, size)

    def tail_help(u):
        for copy, low, size in returning[own + u]:
            copy.wait_recv()
            roll_window(own + u, blocks, stats + 2 * u + 1, low, size)

    def tail_first(u):
        pl.when(has_prev & odd)(functools.partial(tail_own, u))
        if u < helped:
            pl.when(has_next)(functools.partial(tail_help, u))
        pl.when(has_prev & ~odd)(functools.partial(tail_own, u))

    def tail_second(u):
        @pl.when(has_prev)
        def _():
            clip_scores(u, 0, stats + 2 * u)

        if u < helped:
            @pl.when(has_next)
            def _():
                clip_scores(own + u, blocks, stats + 2 * u + 1)

    def tail_exchange(u):
        reduce_items(tail + 2 * u, 2, stats + 2 * u)
        send(tail + 2 * u)

    def tail_scores(u):
        slot = tail + 2 * u
        receive(slot)
        spread_items(totals[slot], counts[last], 2, stats + 2 * u)
        tail_second(u)
        reduce_items(slot + 1, 2, stats + 2 * u)
        send(slot + 1)

    def tail_last(u):
        slot = tail + 2 * u
        receive(slot + 1)
        if u < helped:
            advice[u, :1, :] = totals[slot, 1:2, :]
            advice[u, 1:2, :] = totals[slot + 1, 1:2, :]

            @pl.when(has_next)
            def _():
                advising[u].start()

        @pl.when(has_prev)
        def _():
            spread_items(totals[slot + 1], counts[last], 1, stats + 2 * u)
            finish(u, 0, stats + 2 * u)

    def last_rolls(u):
        for copy, low, size in landing[own + u]:
            copy.wait_recv()
            roll_only(u, low, size)

    late = own - 1
    for g in range(len(groups)):
        main_first(g)
    for u in range(late):
        tail_first(u)
        tail_exchange(u)

    @pl.when(tm == 0)
    def _():
        tail_first(late)
        tail_exchange(late)

    receive(0)
    for i in range(2):
        b = 0 if i == 0 else blocks
        counts[last, i:i + 1, :] = jnp.maximum(totals[0, b:b + 1, :], 1.0)
    main_counts(0)
    main_second(0)

    @pl.when(has_prev)
    def _():
        tail_first(late)
        tail_exchange(late)

    for g in range(1, len(groups)):
        main_counts(g)
        main_second(g)
    for u in range(late):
        tail_scores(u)

    @pl.when(tm == 0)
    def _():
        tail_scores(late)

    for g in range(len(groups) - 1):
        main_third(g)

    @pl.when(has_prev)
    def _():
        tail_scores(late)

    @pl.when(has_prev)
    def _():
        main_third(len(groups) - 1)

    for u in range(late):
        tail_last(u)

    @pl.when(has_prev)
    def _():
        for u in range(helped - 1):
            last_rolls(u)

    tail_last(late)

    @pl.when(tm == 0)
    def _():
        main_third(len(groups) - 1)

    @pl.when(has_prev)
    def _():
        for u in range(helped - 1, helped):
            last_rolls(u)
        head_count[...] = jnp.broadcast_to(counts[last, :1, :], head_count.shape)
        for copy in advising:
            copy.wait_recv()

    @pl.when(has_prev)
    def _():
        for copy in backs:
            copy.wait_send()

    @pl.when(has_next)
    def _():
        for copy in advising + halos:
            copy.wait_send()

    for slot in range(part.shape[0]):
        sent = got.at[slot, :, rows_of(slot)]
        pltpu.make_async_copy(sent, sent, send_sem.at[slot]).wait()


def finisher(
    own, out, rolled, head_weight, advised, head_count, result, head, columns_of, sem,
):
    fields, rows, assets = out.shape
    helped = fields - own
    below = pl.ds(WINDOW, rows - WINDOW)
    tm = lax.axis_index("tm")
    copies = [
        pltpu.make_async_copy(out.at[f, below], result.at[f, below], sem.at[0, f])
        for f in range(fields)
    ]
    done = [
        pltpu.make_async_copy(out.at[f, :WINDOW], result.at[f, :WINDOW], sem.at[1, f])
        for f in range(fields)
    ]
    finished = [
        pltpu.make_async_copy(head.at[u], result.at[own + u, :WINDOW], sem.at[1, own + u])
        for u in range(helped)
    ]
    for copy in copies + done[:own]:
        copy.start()

    @pl.when(tm == 0)
    def _():
        for copy in done[own:]:
            copy.start()

    @pl.when(tm > 0)
    def _():
        for u in range(helped):
            spread(columns_of, advised[u], head_count[...], 2, 2 * u)
        for u in range(helped):
            center, scale = columns_of[2 * u, :WINDOW, :], columns_of[2 * u, WINDOW:, :]
            middle, factor = columns_of[2 * u + 1, :WINDOW, :], columns_of[2 * u + 1, WINDOW:, :]

            @pl.loop(0, assets // LANES, unroll=2)
            def chunk(c):
                cols = chunk_columns(c)
                scored = (rolled[u, :, cols] - center) * scale
                clipped = jnp.minimum(jnp.maximum(scored, -CLIP), CLIP)
                head[u, :, cols] = (clipped - middle) * head_weight[:, cols] * factor

            finished[u].start()

    for copy in copies + done:
        copy.wait()


def per_device(n_tm, n_as, values, listed_from, listed_until):
    fields, rows, assets = values.shape
    blocks = rows // WINDOW
    groups = field_groups(fields)
    own = groups[0][1]
    stats = -(-max(own * blocks, blocks + 2) // SUBLANES) * SUBLANES
    slots = 1 + 2 * len(groups) + 2 * own
    cuts = len(halo_pieces(fields, own, assets // LANES))
    back_cuts = max(len(back_pieces(fields, own, assets // LANES)), 1)
    f32 = jnp.float32
    vmem = pltpu.VMEM
    dma = pltpu.SemaphoreType.DMA
    helped = max(fields - own, 1)
    parts = (
        vmem((fields, rows, assets), f32),
        vmem((helped, WINDOW, assets + LANES), f32),
        vmem((WINDOW, assets + LANES), f32),
        vmem((own, SUBLANES, LANES), f32),
        vmem((SUBLANES, LANES), f32),
    )
    in_vmem = [pl.BlockSpec(memory_space=vmem)] * len(parts)
    outputs = pl.pallas_call(
        functools.partial(kernel, n_tm, n_as),
        out_shape=parts,
        in_specs=[pl.BlockSpec(memory_space=pltpu.HBM)] * 3,
        out_specs=in_vmem,
        scratch_shapes=[
            vmem((fields, WINDOW + rows + WINDOW, assets + LANES), f32),
            vmem((fields, rows + WINDOW, assets + LANES), f32),
            vmem((WINDOW + rows + WINDOW, assets + LANES), f32),
            vmem((WINDOW + rows + WINDOW, assets + LANES), f32),
            vmem((1, assets), jnp.int32),
            vmem((1, assets), jnp.int32),
            vmem((stats + 2 * own, LANES, LANES), f32),
            vmem((stats + 2 * own, LANES, LANES), f32),
            vmem((slots, stats, LANES), f32),
            vmem((slots, n_as - 1, stats, LANES), f32),
            vmem((slots, stats, LANES), f32),
            vmem((len(groups) + 1, stats, LANES), f32),
            vmem((own, SUBLANES, LANES), f32),
            dma((fields + 2,)),
            dma((cuts,)),
            dma((cuts,)),
            dma((back_cuts,)),
            dma((back_cuts,)),
            dma((own,)),
            dma((own,)),
            dma((slots,)),
            dma((slots,)),
            pltpu.SemaphoreType.REGULAR((max(greeting_rounds(n_as), 1),)),
        ],
        compiler_params=pltpu.CompilerParams(
            collective_id=0, has_side_effects=True, vmem_limit_bytes=48 * 2**20
        ),
    )(values, listed_from[None], listed_until[None])
    return pl.pallas_call(
        functools.partial(finisher, own),
        out_shape=jax.ShapeDtypeStruct((fields, rows, assets), f32),
        in_specs=in_vmem,
        out_specs=pl.BlockSpec(memory_space=pltpu.HBM),
        scratch_shapes=[
            vmem((helped, WINDOW, assets), f32),
            vmem((2 * own, LANES, LANES), f32),
            dma((2, fields)),
        ],
        compiler_params=pltpu.CompilerParams(vmem_limit_bytes=4 * 2**20),
    )(*outputs)


def solution(mesh):
    in_specs = (P(None, "tm", "asset"), P("asset"), P("asset"))
    out_specs = P(None, "tm", "asset")
    body = functools.partial(per_device, mesh.shape["tm"], mesh.shape["asset"])
    return jax.shard_map(
        body, mesh=mesh, in_specs=in_specs, out_specs=out_specs, check_vma=False
    )
```

```python
import functools

import jax
import jax.numpy as jnp
from jax import lax
from jax.experimental import pallas as pl
from jax.experimental.pallas import tpu as pltpu
from jax.sharding import PartitionSpec as P

WINDOW = 64
LANES = 128
SUBLANES = 8
CLIP = 3.0
ROLL_UNROLL = 8
UNROLL = 4
CUTS = 4


def field_groups(fields):
    half = (fields + 1) // 2
    return [(start, min(half, fields - start)) for start in range(0, fields, half)]


def lane_pieces(fields, split, chunks):
    pieces = []
    for f in fields:
        cuts = CUTS if f in split and chunks % CUTS == 0 else 1
        size = chunks // cuts
        pieces += [(f, c * size, size) for c in range(cuts)]
    return pieces


def halo_pieces(fields, own, chunks):
    return lane_pieces(range(fields), (own - 1, fields - 1), chunks)


def back_pieces(fields, own, chunks):
    return lane_pieces(range(own, fields), (fields - 1,), chunks)


def greeting_rounds(n):
    if n % 2:
        return 0
    return max(n // 2 - 1, 0)


def spread(columns_of, sums, count, items, first=0):
    mean = sums / count
    other = pltpu.roll(mean, WINDOW, 1)
    scale = 1.0 / jnp.sqrt(jnp.maximum(mean - other * other, 0.0) + 0.1)
    lane = lax.broadcasted_iota(jnp.int32, mean.shape, 1)
    row = jnp.where(lane < WINDOW, mean, scale)
    for i in range(items):
        columns_of[first + i] = jnp.broadcast_to(row[i:i + 1], (LANES, LANES)).T


def chunk_columns(c):
    return pl.ds(pl.multiple_of(c * LANES, LANES), LANES)


def kernel(
    n_tm, n_as, values, opened_hbm, closed_hbm,
    out, rolled, head_weight, advised, head_count,
    x, rolling, weight, inverse, opened_ref, closed_ref,
    acc, columns_of, part, got, totals, counts, advice,
    load_sem, sent_sem, halo_recv, back_recv, recv_sem, hello,
):
    fields, rows, assets = values.shape
    blocks = rows // WINDOW
    chunks = assets // LANES
    tiles = WINDOW // SUBLANES
    groups = field_groups(fields)
    own = groups[0][1]
    helped = fields - own
    stats = part.shape[1]
    tail = 1 + 2 * len(groups)
    last = len(groups)
    tm = lax.axis_index("tm")
    me = lax.axis_index("asset")
    later = lax.rem(tm + 1, n_tm)
    before = lax.rem(tm + n_tm - 1, n_tm)
    has_next = tm < n_tm - 1
    has_prev = tm > 0

    def wait_for(ref, semaphore):
        pltpu.make_async_copy(ref, ref, semaphore).wait()

    dates = [
        pltpu.make_async_copy(opened_hbm, opened_ref, load_sem.at[len(groups)]),
        pltpu.make_async_copy(closed_hbm, closed_ref, load_sem.at[len(groups) + 1]),
    ]
    loads = [
        pltpu.make_async_copy(
            values.at[f], x.at[f, pl.ds(WINDOW, rows), pl.ds(0, assets)], load_sem.at[f // own]
        )
        for f in range(fields)
    ]

    barrier = pltpu.get_barrier_semaphore()
    rounds = greeting_rounds(n_as)

    @pl.when(has_next)
    def _():
        pl.semaphore_signal(barrier, inc=1, device_id={"tm": later})

    @pl.when(has_prev)
    def _():
        pl.semaphore_signal(barrier, inc=1, device_id={"tm": before})

    def greet(semaphore):
        if n_as % 2:
            for d in range(1, n_as):
                pl.semaphore_signal(semaphore, inc=1, device_id={"asset": lax.rem(me + d, n_as)})
            return n_as - 1
        beside = me + 1 - 2 * lax.rem(me, 2)
        pl.semaphore_signal(semaphore, inc=1, device_id={"asset": beside})

        @pl.when(me >= 2)
        def _():
            pl.semaphore_signal(semaphore, inc=1, device_id={"asset": me - 2})

        @pl.when(me + 2 < n_as)
        def _():
            pl.semaphore_signal(semaphore, inc=1, device_id={"asset": me + 2})

        return 1 + jnp.where(me >= 2, 1, 0) + jnp.where(me + 2 < n_as, 1, 0)

    near = greet(barrier)
    expected = near + jnp.where(has_next, 1, 0) + jnp.where(has_prev, 1, 0)
    for copy in dates + loads:
        copy.start()

    landing = {f: [] for f in range(fields)}
    halos = []
    for i, (f, first, size) in enumerate(halo_pieces(fields, own, chunks)):
        cols = pl.ds(first * LANES, size * LANES)
        halos.append(pltpu.make_async_remote_copy(
            src_ref=values.at[f, pl.ds(rows - WINDOW, WINDOW), cols],
            dst_ref=x.at[f, pl.ds(0, WINDOW), cols],
            send_sem=sent_sem.at[0],
            recv_sem=halo_recv.at[i],
            device_id={"tm": later},
        ))
        landing[f].append((halos[-1], first, size))
    returning = {f: [] for f in range(own, fields)}
    backs = []
    for i, (f, first, size) in enumerate(back_pieces(fields, own, chunks)):
        cols = pl.ds(first * LANES, size * LANES)
        backs.append(pltpu.make_async_remote_copy(
            src_ref=values.at[f, pl.ds(0, WINDOW), cols],
            dst_ref=x.at[f, pl.ds(WINDOW + rows, WINDOW), cols],
            send_sem=sent_sem.at[1],
            recv_sem=back_recv.at[i],
            device_id={"tm": before},
        ))
        returning[f].append((backs[-1], first, size))
    advising = [
        pltpu.make_async_remote_copy(
            src_ref=advice.at[u],
            dst_ref=advised.at[u],
            send_sem=sent_sem.at[2],
            recv_sem=sent_sem.at[3],
            device_id={"tm": later},
        )
        for u in range(helped)
    ]
    odd = lax.rem(tm, 2) == 1

    def rows_of(slot):
        return pl.ds(0, 2 if slot >= tail else stats)

    def send(slot):
        for d in range(1, n_as):
            pltpu.make_async_remote_copy(
                src_ref=part.at[slot, rows_of(slot)],
                dst_ref=got.at[slot, d - 1, rows_of(slot)],
                send_sem=sent_sem.at[5 if slot >= tail else 4],
                recv_sem=recv_sem.at[slot],
                device_id={"asset": lax.rem(me + d, n_as)},
            ).start()

    def receive(slot):
        arrived = got.at[slot, :, rows_of(slot)]
        wait_for(arrived, recv_sem.at[slot])
        totals[slot] = part[slot] + jnp.sum(got[slot], axis=0)

    def reduce_items(slot, items, first=0):
        for i in range(items):
            part[slot, i:i + 1, :] = jnp.sum(acc[first + i].T, axis=0, keepdims=True)

    def spread_items(sums, count, items, first=0):
        spread(columns_of, sums, count, items, first)

    def column_pair(i):
        return columns_of[i, :WINDOW, :], columns_of[i, WINDOW:, :]

    zero = jnp.zeros((WINDOW, LANES), jnp.float32)
    first_stamp = tm * rows - WINDOW

    def start_listing():
        part[...] = jnp.zeros(part.shape, part.dtype)
        acc[...] = jnp.zeros(acc.shape, acc.dtype)
        for copy in dates:
            copy.wait()

        @pl.when(tm == 0)
        def _():
            @pl.loop(0, fields)
            def clear(f):
                x[f, pl.ds(0, WINDOW), pl.ds(0, assets)] = jnp.zeros((WINDOW, assets), jnp.float32)

    def listing(b):
        start = pl.multiple_of(b * WINDOW, WINDOW)
        row = lax.broadcasted_iota(jnp.int32, (WINDOW, LANES), 0)
        passed = (first_stamp + start + 1 + row).astype(jnp.float32)

        def chunk(c, total):
            cols = chunk_columns(c)
            opened = jnp.maximum(opened_ref[:, cols], 0).astype(jnp.float32)
            closed = closed_ref[:, cols].astype(jnp.float32)
            age = passed - opened
            listed = (age > 0.0) & (passed <= closed)
            ones = jnp.where(listed, 1.0, 0.0)
            weight[pl.ds(start, WINDOW), cols] = ones
            counted = jnp.minimum(jnp.maximum(age, 1.0), float(WINDOW))
            inverse[pl.ds(start, WINDOW), cols] = ones / counted
            return total + ones

        total = lax.fori_loop(0, chunks, chunk, zero, unroll=2)
        at = lax.rem(b + blocks + 1, blocks + 2)
        acc[at, :WINDOW, :] = total
        acc[at, WINDOW:, :] = total

    def listing_blocks(low, high):
        pl.loop(low, high)(listing)

    @pl.when(tm == 0)
    def _():
        start_listing()
        listing_blocks(0, blocks)

    pl.semaphore_wait(barrier, expected)

    @pl.when(has_prev & ~odd)
    def _():
        for copy in backs:
            copy.start()

    @pl.when(has_next)
    def _():
        for copy in halos:
            copy.start()

    @pl.when(has_prev & odd)
    def _():
        for copy in backs:
            copy.start()

    if rounds:
        greet(hello.at[0])

    @pl.when(has_prev)
    def _():
        start_listing()
        listing_blocks(0, blocks)

    listing_blocks(blocks, blocks + 2)

    def next_round(r):
        pl.semaphore_wait(hello.at[r], near)
        if r + 1 < rounds:
            greet(hello.at[r + 1])

    for r in range(rounds - 2):
        next_round(r)
    reduce_items(0, blocks + 1)

    def window_means(f, b, c):
        top = pl.multiple_of(b * WINDOW, WINDOW)
        cols = chunk_columns(c)
        sublane = lax.broadcasted_iota(jnp.int32, (SUBLANES, LANES), 0)

        ends = range(2 * tiles)
        reach = pl.ds(top, 2 * WINDOW)
        masked = x[f, reach, cols] * weight[reach, cols]
        sums = {j: masked[SUBLANES * j:SUBLANES * (j + 1)] for j in ends}
        step = 1
        while step < tiles:
            sums = {j: sums[j] + sums[j - step] for j in ends if j - step in sums}
            step *= 2
        shift = 1
        while shift < SUBLANES:
            keep = sublane < SUBLANES - shift
            moved = {tiles - 1: sums[tiles - 1]}
            for j in range(tiles, 2 * tiles):
                moved[j] = jnp.where(keep, sums[j], sums[j - 1])
            sums = {j: sums[j] + pltpu.roll(moved[j], shift, 0) for j in moved}
            shift *= 2
        ending = jnp.concatenate([sums[j] for j in range(tiles, 2 * tiles)], axis=0)
        return ending * inverse[pl.ds(top + WINDOW, WINDOW), cols]

    def roll_window(f, b, i, low=0, size=chunks):
        top = pl.multiple_of(b * WINDOW, WINDOW)

        def chunk(c, carry):
            means = window_means(f, b, c)
            rolling[f, pl.ds(top, WINDOW), chunk_columns(c)] = means
            return carry[0] + means, carry[1] + means * means

        carry = (zero, zero) if low == 0 else (acc[i, :WINDOW, :], acc[i, WINDOW:, :])
        first, second = lax.fori_loop(
            low, low + size, chunk, carry, unroll=min(ROLL_UNROLL, size)
        )
        acc[i, :WINDOW, :] = first
        acc[i, WINDOW:, :] = second

    def clip_scores(f, b, i):
        top = pl.multiple_of(b * WINDOW, WINDOW)
        center, scale = column_pair(i)

        def chunk(c, carry):
            cols = chunk_columns(c)
            here = pl.ds(top, WINDOW)
            scored = (rolling[f, here, cols] - center) * scale
            clipped = jnp.minimum(jnp.maximum(scored, -CLIP), CLIP)
            rolling[f, here, cols] = clipped
            masked = clipped * weight[pl.ds(top + WINDOW, WINDOW), cols]
            return carry[0] + masked, carry[1] + masked * clipped

        first, second = lax.fori_loop(0, chunks, chunk, (zero, zero), unroll=UNROLL)
        acc[i, :WINDOW, :] = first
        acc[i, WINDOW:, :] = second

    def finish(f, b, i):
        top = pl.multiple_of(b * WINDOW, WINDOW)
        middle, factor = column_pair(i)

        @pl.loop(0, chunks, unroll=UNROLL)
        def chunk(c):
            cols = chunk_columns(c)
            here = pl.ds(top, WINDOW)
            deviate = (rolling[f, here, cols] - middle) * weight[pl.ds(top + WINDOW, WINDOW), cols]
            out[f, here, cols] = deviate * factor

    def roll_only(u, low, size):
        @pl.loop(low, low + size, unroll=min(2, size))
        def chunk(c):
            cols = chunk_columns(c)
            rolled[u, :, cols] = window_means(own + u, 0, c)
            if u == 0:
                head_weight[:, cols] = weight[WINDOW:2 * WINDOW, cols]

    def main_items(g):
        size = groups[g][1]
        return pl.loop(jnp.where(tm == 0, 0, size), size * blocks)

    def main_first(g):
        start, size = groups[g]
        block = x.at[pl.ds(start, size), pl.ds(WINDOW, rows), pl.ds(0, assets)]
        wait_for(block, load_sem.at[g])

        @main_items(g)
        def item(i):
            roll_window(start + lax.rem(i, size), lax.div(i, size), i)
            if g == 0 and rounds > 1:
                pl.when(i == (size + size * blocks) // 2)(lambda: next_round(rounds - 2))

        reduce_items(1 + 2 * g, size * blocks)
        if g == 0:
            if rounds:
                next_round(rounds - 1)
            send(0)
        send(1 + 2 * g)

    def main_counts(g):
        size = groups[g][1]
        for i in range(size * blocks):
            b = i // size
            counts[g, i:i + 1, :] = jnp.maximum(totals[0, b:b + 1, :], 1.0)

    def main_second(g):
        start, size = groups[g]
        slot = 1 + 2 * g
        receive(slot)
        spread_items(totals[slot], counts[g], size * blocks)

        @main_items(g)
        def item(i):
            clip_scores(start + lax.rem(i, size), lax.div(i, size), i)

        reduce_items(slot + 1, size * blocks)
        send(slot + 1)

    def main_third(g):
        start, size = groups[g]
        slot = 2 + 2 * g
        receive(slot)
        spread_items(totals[slot], counts[g], size * blocks)

        @main_items(g)
        def item(i):
            finish(start + lax.rem(i, size), lax.div(i, size), i)

    def tail_own(u):
        for copy, low, size in landing[u]:
            copy.wait_recv()
            roll_window(u, 0, stats + 2 * u, low, size)

    def tail_help(u):
        for copy, low, size in returning[own + u]:
            copy.wait_recv()
            roll_window(own + u, blocks, stats + 2 * u + 1, low, size)

    def tail_first(u):
        pl.when(has_prev & odd)(functools.partial(tail_own, u))
        if u < helped:
            pl.when(has_next)(functools.partial(tail_help, u))
        pl.when(has_prev & ~odd)(functools.partial(tail_own, u))

    def tail_second(u):
        @pl.when(has_prev)
        def _():
            clip_scores(u, 0, stats + 2 * u)

        if u < helped:
            @pl.when(has_next)
            def _():
                clip_scores(own + u, blocks, stats + 2 * u + 1)

    def tail_exchange(u):
        reduce_items(tail + 2 * u, 2, stats + 2 * u)
        send(tail + 2 * u)

    def tail_scores(u):
        slot = tail + 2 * u
        receive(slot)
        spread_items(totals[slot], counts[last], 2, stats + 2 * u)
        tail_second(u)
        reduce_items(slot + 1, 2, stats + 2 * u)
        send(slot + 1)

    def tail_last(u):
        slot = tail + 2 * u
        receive(slot + 1)
        if u < helped:
            advice[u, :1, :] = totals[slot, 1:2, :]
            advice[u, 1:2, :] = totals[slot + 1, 1:2, :]

            @pl.when(has_next)
            def _():
                advising[u].start()

        @pl.when(has_prev)
        def _():
            spread_items(totals[slot + 1], counts[last], 1, stats + 2 * u)
            finish(u, 0, stats + 2 * u)

    def last_rolls(u):
        for copy, low, size in landing[own + u]:
            copy.wait_recv()
            roll_only(u, low, size)

    late = own - 1
    for g in range(len(groups)):
        main_first(g)
    for u in range(late):
        tail_first(u)
        tail_exchange(u)

    @pl.when(tm == 0)
    def _():
        tail_first(late)
        tail_exchange(late)

    receive(0)
    for i in range(2):
        b = 0 if i == 0 else blocks
        counts[last, i:i + 1, :] = jnp.maximum(totals[0, b:b + 1, :], 1.0)
    main_counts(0)
    main_second(0)

    @pl.when(has_prev)
    def _():
        tail_first(late)
        tail_exchange(late)

    for g in range(1, len(groups)):
        main_counts(g)
        main_second(g)
    for u in range(late):
        tail_scores(u)

    @pl.when(tm == 0)
    def _():
        tail_scores(late)

    for g in range(len(groups) - 1):
        main_third(g)

    @pl.when(has_prev)
    def _():
        tail_scores(late)

    @pl.when(has_prev)
    def _():
        main_third(len(groups) - 1)

    for u in range(late):
        tail_last(u)

    @pl.when(has_prev)
    def _():
        for u in range(helped - 1):
            last_rolls(u)

    tail_last(late)

    @pl.when(tm == 0)
    def _():
        main_third(len(groups) - 1)

    @pl.when(has_prev)
    def _():
        for u in range(helped - 1, helped):
            last_rolls(u)
        head_count[...] = jnp.broadcast_to(counts[last, :1, :], head_count.shape)
        wait_for(advised.at[pl.ds(0, helped)], sent_sem.at[3])

    head_rows = pl.ds(0, WINDOW)

    @pl.when(has_prev)
    def _():
        wait_for(x.at[pl.ds(own, helped), head_rows, pl.ds(0, assets)], sent_sem.at[1])

    @pl.when(has_next)
    def _():
        wait_for(x.at[:, head_rows, pl.ds(0, assets)], sent_sem.at[0])
        wait_for(advice.at[pl.ds(0, helped)], sent_sem.at[2])

    wait_for(got.at[pl.ds(0, tail)], sent_sem.at[4])
    wait_for(got.at[pl.ds(tail, 2 * own), :, pl.ds(0, 2)], sent_sem.at[5])


def finisher(
    own, out, rolled, head_weight, advised, head_count, result, head, columns_of, sem,
):
    fields, rows, assets = out.shape
    helped = fields - own
    below = pl.ds(WINDOW, rows - WINDOW)
    tm = lax.axis_index("tm")
    copies = [
        pltpu.make_async_copy(out.at[f, below], result.at[f, below], sem)
        for f in range(fields)
    ]
    done = [
        pltpu.make_async_copy(out.at[f, :WINDOW], result.at[f, :WINDOW], sem)
        for f in range(fields)
    ]
    finished = [
        pltpu.make_async_copy(head.at[u], result.at[own + u, :WINDOW], sem)
        for u in range(helped)
    ]
    for copy in copies + done[:own]:
        copy.start()

    @pl.when(tm == 0)
    def _():
        for copy in done[own:]:
            copy.start()

    @pl.when(tm > 0)
    def _():
        for u in range(helped):
            spread(columns_of, advised[u], head_count[...], 2, 2 * u)
        for u in range(helped):
            center, scale = columns_of[2 * u, :WINDOW, :], columns_of[2 * u, WINDOW:, :]
            middle, factor = columns_of[2 * u + 1, :WINDOW, :], columns_of[2 * u + 1, WINDOW:, :]

            @pl.loop(0, assets // LANES, unroll=2)
            def chunk(c):
                cols = chunk_columns(c)
                scored = (rolled[u, :, cols] - center) * scale
                clipped = jnp.minimum(jnp.maximum(scored, -CLIP), CLIP)
                head[u, :, cols] = (clipped - middle) * head_weight[:, cols] * factor

            finished[u].start()

    pltpu.make_async_copy(out, out, sem).wait()


def per_device(n_tm, n_as, values, listed_from, listed_until):
    fields, rows, assets = values.shape
    blocks = rows // WINDOW
    groups = field_groups(fields)
    own = groups[0][1]
    stats = -(-max(own * blocks, blocks + 2) // SUBLANES) * SUBLANES
    slots = 1 + 2 * len(groups) + 2 * own
    cuts = len(halo_pieces(fields, own, assets // LANES))
    back_cuts = max(len(back_pieces(fields, own, assets // LANES)), 1)
    f32 = jnp.float32
    vmem = pltpu.VMEM
    dma = pltpu.SemaphoreType.DMA
    helped = max(fields - own, 1)
    parts = (
        vmem((fields, rows, assets), f32),
        vmem((helped, WINDOW, assets + LANES), f32),
        vmem((WINDOW, assets + LANES), f32),
        vmem((own, SUBLANES, LANES), f32),
        vmem((SUBLANES, LANES), f32),
    )
    in_vmem = [pl.BlockSpec(memory_space=vmem)] * len(parts)
    outputs = pl.pallas_call(
        functools.partial(kernel, n_tm, n_as),
        out_shape=parts,
        in_specs=[pl.BlockSpec(memory_space=pltpu.HBM)] * 3,
        out_specs=in_vmem,
        scratch_shapes=[
            vmem((fields, WINDOW + rows + WINDOW, assets + LANES), f32),
            vmem((fields, rows + WINDOW, assets + LANES), f32),
            vmem((WINDOW + rows + WINDOW, assets + LANES), f32),
            vmem((WINDOW + rows + WINDOW, assets + LANES), f32),
            vmem((1, assets), jnp.int32),
            vmem((1, assets), jnp.int32),
            vmem((stats + 2 * own, LANES, LANES), f32),
            vmem((stats + 2 * own, LANES, LANES), f32),
            vmem((slots, stats, LANES), f32),
            vmem((slots, n_as - 1, stats, LANES), f32),
            vmem((slots, stats, LANES), f32),
            vmem((len(groups) + 1, stats, LANES), f32),
            vmem((own, SUBLANES, LANES), f32),
            dma((len(groups) + 2,)),
            dma((6,)),
            dma((cuts,)),
            dma((back_cuts,)),
            dma((slots,)),
            pltpu.SemaphoreType.REGULAR((max(greeting_rounds(n_as), 1),)),
        ],
        compiler_params=pltpu.CompilerParams(
            collective_id=0, has_side_effects=True, vmem_limit_bytes=48 * 2**20
        ),
    )(values, listed_from[None], listed_until[None])
    return pl.pallas_call(
        functools.partial(finisher, own),
        out_shape=jax.ShapeDtypeStruct((fields, rows, assets), f32),
        in_specs=in_vmem,
        out_specs=pl.BlockSpec(memory_space=pltpu.HBM),
        scratch_shapes=[
            vmem((helped, WINDOW, assets), f32),
            vmem((2 * own, LANES, LANES), f32),
            dma(()),
        ],
        compiler_params=pltpu.CompilerParams(vmem_limit_bytes=4 * 2**20),
    )(*outputs)


def solution(mesh):
    in_specs = (P(None, "tm", "asset"), P("asset"), P("asset"))
    out_specs = P(None, "tm", "asset")
    body = functools.partial(per_device, mesh.shape["tm"], mesh.shape["asset"])
    return jax.shard_map(
        body, mesh=mesh, in_specs=in_specs, out_specs=out_specs, check_vma=False
    )
```

```python
import functools

import jax
import jax.numpy as jnp
from jax import lax
from jax.experimental import pallas as pl
from jax.experimental.pallas import tpu as pltpu
from jax.sharding import PartitionSpec as P

WINDOW = 64
LANES = 128
SUBLANES = 8
CLIP = 3.0
ROLL_UNROLL = 8
UNROLL = 4
CUTS = 4


def field_groups(fields):
    half = (fields + 1) // 2
    return [(start, min(half, fields - start)) for start in range(0, fields, half)]


def lane_pieces(fields, split, chunks):
    pieces = []
    for f in fields:
        cuts = CUTS if f in split and chunks % CUTS == 0 else 1
        size = chunks // cuts
        pieces += [(f, c * size, size) for c in range(cuts)]
    return pieces


def halo_pieces(fields, own, chunks):
    return lane_pieces(range(fields), (own - 1, fields - 1), chunks)


def back_pieces(fields, own, chunks):
    return lane_pieces(range(own, fields), (fields - 1,), chunks)


def greeting_rounds(n):
    if n % 2:
        return 0
    return max(n // 2 - 1, 0)


def spread(columns_of, sums, count, items, first=0):
    mean = sums / count
    other = pltpu.roll(mean, WINDOW, 1)
    scale = 1.0 / jnp.sqrt(jnp.maximum(mean - other * other, 0.0) + 0.1)
    lane = lax.broadcasted_iota(jnp.int32, mean.shape, 1)
    row = jnp.where(lane < WINDOW, mean, scale)
    for i in range(items):
        columns_of[first + i] = jnp.broadcast_to(row[i:i + 1], (LANES, LANES)).T


def chunk_columns(c):
    return pl.ds(pl.multiple_of(c * LANES, LANES), LANES)


def kernel(
    n_tm, n_as, values, opened_hbm, closed_hbm,
    out, rolled, head_weight, advised, head_count,
    x, rolling, weight, inverse, opened_ref, closed_ref,
    acc, columns_of, packed, part, got, totals, counts, advice,
    load_sem, sent_sem, halo_recv, top_recv, back_recv, recv_sem, hello,
):
    fields, rows, assets = values.shape
    blocks = rows // WINDOW
    chunks = assets // LANES
    tiles = WINDOW // SUBLANES
    groups = field_groups(fields)
    own = groups[0][1]
    helped = fields - own
    stats = part.shape[1]
    tail = 1 + 2 * len(groups)
    last = len(groups)
    tm = lax.axis_index("tm")
    me = lax.axis_index("asset")
    later = lax.rem(tm + 1, n_tm)
    before = lax.rem(tm + n_tm - 1, n_tm)
    has_next = tm < n_tm - 1
    has_prev = tm > 0

    def wait_for(ref, semaphore):
        pltpu.make_async_copy(ref, ref, semaphore).wait()

    dates = [
        pltpu.make_async_copy(opened_hbm, opened_ref, load_sem.at[len(groups)]),
        pltpu.make_async_copy(closed_hbm, closed_ref, load_sem.at[len(groups) + 1]),
    ]
    loads = [
        pltpu.make_async_copy(
            values.at[f], x.at[f, pl.ds(WINDOW, rows), pl.ds(0, assets)], load_sem.at[f // own]
        )
        for f in range(fields)
    ]

    barrier = pltpu.get_barrier_semaphore()
    rounds = greeting_rounds(n_as)

    @pl.when(has_next)
    def _():
        pl.semaphore_signal(barrier, inc=1, device_id={"tm": later})

    @pl.when(has_prev)
    def _():
        pl.semaphore_signal(barrier, inc=1, device_id={"tm": before})

    def greet(semaphore):
        if n_as % 2:
            for d in range(1, n_as):
                pl.semaphore_signal(semaphore, inc=1, device_id={"asset": lax.rem(me + d, n_as)})
            return n_as - 1
        beside = me + 1 - 2 * lax.rem(me, 2)
        pl.semaphore_signal(semaphore, inc=1, device_id={"asset": beside})

        @pl.when(me >= 2)
        def _():
            pl.semaphore_signal(semaphore, inc=1, device_id={"asset": me - 2})

        @pl.when(me + 2 < n_as)
        def _():
            pl.semaphore_signal(semaphore, inc=1, device_id={"asset": me + 2})

        return 1 + jnp.where(me >= 2, 1, 0) + jnp.where(me + 2 < n_as, 1, 0)

    near = greet(barrier)
    expected = near + jnp.where(has_next, 1, 0) + jnp.where(has_prev, 1, 0)
    for copy in dates + loads:
        copy.start()

    kept = packed.shape[2] // LANES
    landing = {f: [] for f in range(fields)}
    tops = {}
    for i, (f, first, size) in enumerate(halo_pieces(fields, own, chunks)):
        cols = pl.ds(first * LANES, size * LANES)
        skip = SUBLANES if f else 0
        copy = pltpu.make_async_remote_copy(
            src_ref=values.at[f, pl.ds(rows - WINDOW + skip, WINDOW - skip), cols],
            dst_ref=x.at[f, pl.ds(skip, WINDOW - skip), cols],
            send_sem=sent_sem.at[6 if f else 0],
            recv_sem=halo_recv.at[i],
            device_id={"tm": later},
        )
        landing[f].append((copy, first, size))
    for f in range(1, fields):
        tops[f] = pltpu.make_async_remote_copy(
            src_ref=packed.at[f - 1],
            dst_ref=x.at[f, pl.ds(0, SUBLANES), pl.ds(0, kept * LANES)],
            send_sem=sent_sem.at[7],
            recv_sem=top_recv.at[f - 1],
            device_id={"tm": later},
        )

    def tile_columns(c):
        return pl.ds(c * LANES, LANES)

    def pack_top(f):
        sublane = lax.broadcasted_iota(jnp.int32, (SUBLANES, LANES), 0)
        for c in range(kept):
            tile = x[f, pl.ds(rows, SUBLANES), tile_columns(c)]
            if kept < chunks:
                extra, row = kept + c // (SUBLANES - 1), 1 + c % (SUBLANES - 1)
                other = x[f, pl.ds(rows, SUBLANES), tile_columns(extra)][row:row + 1]
                tile = jnp.where(sublane == 0, jnp.broadcast_to(other, tile.shape), tile)
            packed[f - 1, :, tile_columns(c)] = tile

    def unpack_top(f):
        if f == 0:
            return
        tops[f].wait_recv()
        sublane = lax.broadcasted_iota(jnp.int32, (SUBLANES, LANES), 0)
        for extra in range(chunks - kept):
            tile = jnp.zeros((SUBLANES, LANES), jnp.float32)
            for k in range(SUBLANES - 1):
                from_tile = tile_columns((SUBLANES - 1) * extra + k)
                row = x[f, pl.ds(0, SUBLANES), from_tile][:1]
                tile = jnp.where(sublane == 1 + k, jnp.broadcast_to(row, tile.shape), tile)
            x[f, pl.ds(0, SUBLANES), tile_columns(kept + extra)] = tile

    def start_halo(f):
        if f > 0:
            tops[f].start()
        for copy, _, _ in landing[f]:
            copy.start()

    returning = {f: [] for f in range(own, fields)}
    backs = []
    for i, (f, first, size) in enumerate(back_pieces(fields, own, chunks)):
        cols = pl.ds(first * LANES, size * LANES)
        backs.append(pltpu.make_async_remote_copy(
            src_ref=values.at[f, pl.ds(0, WINDOW), cols],
            dst_ref=x.at[f, pl.ds(WINDOW + rows, WINDOW), cols],
            send_sem=sent_sem.at[1],
            recv_sem=back_recv.at[i],
            device_id={"tm": before},
        ))
        returning[f].append((backs[-1], first, size))
    advising = [
        pltpu.make_async_remote_copy(
            src_ref=advice.at[u],
            dst_ref=advised.at[u],
            send_sem=sent_sem.at[2],
            recv_sem=sent_sem.at[3],
            device_id={"tm": later},
        )
        for u in range(helped)
    ]
    odd = lax.rem(tm, 2) == 1

    def rows_of(slot):
        return pl.ds(0, 2 if slot >= tail else stats)

    def send(slot):
        for d in range(1, n_as):
            pltpu.make_async_remote_copy(
                src_ref=part.at[slot, rows_of(slot)],
                dst_ref=got.at[slot, d - 1, rows_of(slot)],
                send_sem=sent_sem.at[5 if slot >= tail else 4],
                recv_sem=recv_sem.at[slot],
                device_id={"asset": lax.rem(me + d, n_as)},
            ).start()

    def receive(slot):
        arrived = got.at[slot, :, rows_of(slot)]
        wait_for(arrived, recv_sem.at[slot])
        totals[slot] = part[slot] + jnp.sum(got[slot], axis=0)

    def reduce_items(slot, items, first=0):
        for i in range(items):
            part[slot, i:i + 1, :] = jnp.sum(acc[first + i].T, axis=0, keepdims=True)

    def spread_items(sums, count, items, first=0):
        spread(columns_of, sums, count, items, first)

    def column_pair(i):
        return columns_of[i, :WINDOW, :], columns_of[i, WINDOW:, :]

    zero = jnp.zeros((WINDOW, LANES), jnp.float32)
    first_stamp = tm * rows - WINDOW

    def start_listing():
        part[...] = jnp.zeros(part.shape, part.dtype)
        acc[...] = jnp.zeros(acc.shape, acc.dtype)
        for copy in dates:
            copy.wait()

        @pl.when(tm == 0)
        def _():
            @pl.loop(0, fields)
            def clear(f):
                x[f, pl.ds(0, WINDOW), pl.ds(0, assets)] = jnp.zeros((WINDOW, assets), jnp.float32)

    def listing(b):
        start = pl.multiple_of(b * WINDOW, WINDOW)
        row = lax.broadcasted_iota(jnp.int32, (WINDOW, LANES), 0)
        passed = (first_stamp + start + 1 + row).astype(jnp.float32)

        def chunk(c, total):
            cols = chunk_columns(c)
            opened = jnp.maximum(opened_ref[:, cols], 0).astype(jnp.float32)
            closed = closed_ref[:, cols].astype(jnp.float32)
            age = passed - opened
            listed = (age > 0.0) & (passed <= closed)
            ones = jnp.where(listed, 1.0, 0.0)
            weight[pl.ds(start, WINDOW), cols] = ones
            counted = jnp.minimum(jnp.maximum(age, 1.0), float(WINDOW))
            inverse[pl.ds(start, WINDOW), cols] = ones / counted
            return total + ones

        total = lax.fori_loop(0, chunks, chunk, zero, unroll=2)
        at = lax.rem(b + blocks + 1, blocks + 2)
        acc[at, :WINDOW, :] = total
        acc[at, WINDOW:, :] = total

    def listing_blocks(low, high):
        pl.loop(low, high)(listing)

    @pl.when(tm == 0)
    def _():
        start_listing()
        listing_blocks(0, blocks)

    pl.semaphore_wait(barrier, expected)

    @pl.when(has_prev & ~odd)
    def _():
        for copy in backs:
            copy.start()

    @pl.when(has_next)
    def _():
        start_halo(0)

    @pl.when(has_prev & odd)
    def _():
        for copy in backs:
            copy.start()

    if rounds:
        greet(hello.at[0])

    @pl.when(has_prev)
    def _():
        start_listing()
        listing_blocks(0, blocks)

    listing_blocks(blocks, blocks + 2)

    def next_round(r):
        pl.semaphore_wait(hello.at[r], near)
        if r + 1 < rounds:
            greet(hello.at[r + 1])

    for r in range(rounds - 2):
        next_round(r)
    reduce_items(0, blocks + 1)

    def window_means(f, b, c):
        top = pl.multiple_of(b * WINDOW, WINDOW)
        cols = chunk_columns(c)
        sublane = lax.broadcasted_iota(jnp.int32, (SUBLANES, LANES), 0)

        ends = range(2 * tiles)
        reach = pl.ds(top, 2 * WINDOW)
        masked = x[f, reach, cols] * weight[reach, cols]
        sums = {j: masked[SUBLANES * j:SUBLANES * (j + 1)] for j in ends}
        step = 1
        while step < tiles:
            sums = {j: sums[j] + sums[j - step] for j in ends if j - step in sums}
            step *= 2
        shift = 1
        while shift < SUBLANES:
            keep = sublane < SUBLANES - shift
            moved = {tiles - 1: sums[tiles - 1]}
            for j in range(tiles, 2 * tiles):
                moved[j] = jnp.where(keep, sums[j], sums[j - 1])
            sums = {j: sums[j] + pltpu.roll(moved[j], shift, 0) for j in moved}
            shift *= 2
        ending = jnp.concatenate([sums[j] for j in range(tiles, 2 * tiles)], axis=0)
        return ending * inverse[pl.ds(top + WINDOW, WINDOW), cols]

    def roll_window(f, b, i, low=0, size=chunks):
        top = pl.multiple_of(b * WINDOW, WINDOW)

        def chunk(c, carry):
            means = window_means(f, b, c)
            rolling[f, pl.ds(top, WINDOW), chunk_columns(c)] = means
            return carry[0] + means, carry[1] + means * means

        carry = (zero, zero) if low == 0 else (acc[i, :WINDOW, :], acc[i, WINDOW:, :])
        first, second = lax.fori_loop(
            low, low + size, chunk, carry, unroll=min(ROLL_UNROLL, size)
        )
        acc[i, :WINDOW, :] = first
        acc[i, WINDOW:, :] = second

    def clip_scores(f, b, i):
        top = pl.multiple_of(b * WINDOW, WINDOW)
        center, scale = column_pair(i)

        def chunk(c, carry):
            cols = chunk_columns(c)
            here = pl.ds(top, WINDOW)
            scored = (rolling[f, here, cols] - center) * scale
            clipped = jnp.minimum(jnp.maximum(scored, -CLIP), CLIP)
            rolling[f, here, cols] = clipped
            masked = clipped * weight[pl.ds(top + WINDOW, WINDOW), cols]
            return carry[0] + masked, carry[1] + masked * clipped

        first, second = lax.fori_loop(0, chunks, chunk, (zero, zero), unroll=UNROLL)
        acc[i, :WINDOW, :] = first
        acc[i, WINDOW:, :] = second

    def finish(f, b, i):
        top = pl.multiple_of(b * WINDOW, WINDOW)
        middle, factor = column_pair(i)

        @pl.loop(0, chunks, unroll=UNROLL)
        def chunk(c):
            cols = chunk_columns(c)
            here = pl.ds(top, WINDOW)
            deviate = (rolling[f, here, cols] - middle) * weight[pl.ds(top + WINDOW, WINDOW), cols]
            out[f, here, cols] = deviate * factor

    def roll_only(u, low, size):
        @pl.loop(low, low + size, unroll=min(2, size))
        def chunk(c):
            cols = chunk_columns(c)
            rolled[u, :, cols] = window_means(own + u, 0, c)
            if u == 0:
                head_weight[:, cols] = weight[WINDOW:2 * WINDOW, cols]

    def main_items(g):
        size = groups[g][1]
        return pl.loop(jnp.where(tm == 0, 0, size), size * blocks)

    def main_first(g):
        start, size = groups[g]
        block = x.at[pl.ds(start, size), pl.ds(WINDOW, rows), pl.ds(0, assets)]
        wait_for(block, load_sem.at[g])
        ahead = [f for f in range(start, start + size) if f > 0]

        @pl.when(has_next)
        def _():
            for f in ahead:
                pack_top(f)

        def middle():
            @pl.when(has_next)
            def _():
                for f in ahead:
                    start_halo(f)

            if g == 0 and rounds > 1:
                next_round(rounds - 2)

        @main_items(g)
        def item(i):
            roll_window(start + lax.rem(i, size), lax.div(i, size), i)
            pl.when(i == (size + size * blocks) // 2)(middle)

        reduce_items(1 + 2 * g, size * blocks)
        if g == 0:
            if rounds:
                next_round(rounds - 1)
            send(0)
        send(1 + 2 * g)

    def main_counts(g):
        size = groups[g][1]
        for i in range(size * blocks):
            b = i // size
            counts[g, i:i + 1, :] = jnp.maximum(totals[0, b:b + 1, :], 1.0)

    def main_second(g):
        start, size = groups[g]
        slot = 1 + 2 * g
        receive(slot)
        spread_items(totals[slot], counts[g], size * blocks)

        @main_items(g)
        def item(i):
            clip_scores(start + lax.rem(i, size), lax.div(i, size), i)

        reduce_items(slot + 1, size * blocks)
        send(slot + 1)

    def main_third(g):
        start, size = groups[g]
        slot = 2 + 2 * g
        receive(slot)
        spread_items(totals[slot], counts[g], size * blocks)

        @main_items(g)
        def item(i):
            finish(start + lax.rem(i, size), lax.div(i, size), i)

    def tail_own(u):
        unpack_top(u)
        for copy, low, size in landing[u]:
            copy.wait_recv()
            roll_window(u, 0, stats + 2 * u, low, size)

    def tail_help(u):
        for copy, low, size in returning[own + u]:
            copy.wait_recv()
            roll_window(own + u, blocks, stats + 2 * u + 1, low, size)

    def tail_first(u):
        pl.when(has_prev & odd)(functools.partial(tail_own, u))
        if u < helped:
            pl.when(has_next)(functools.partial(tail_help, u))
        pl.when(has_prev & ~odd)(functools.partial(tail_own, u))

    def tail_second(u):
        @pl.when(has_prev)
        def _():
            clip_scores(u, 0, stats + 2 * u)

        if u < helped:
            @pl.when(has_next)
            def _():
                clip_scores(own + u, blocks, stats + 2 * u + 1)

    def tail_exchange(u):
        reduce_items(tail + 2 * u, 2, stats + 2 * u)
        send(tail + 2 * u)

    def tail_scores(u):
        slot = tail + 2 * u
        receive(slot)
        spread_items(totals[slot], counts[last], 2, stats + 2 * u)
        tail_second(u)
        reduce_items(slot + 1, 2, stats + 2 * u)
        send(slot + 1)

    def tail_last(u):
        slot = tail + 2 * u
        receive(slot + 1)
        if u < helped:
            advice[u, :1, :] = totals[slot, 1:2, :]
            advice[u, 1:2, :] = totals[slot + 1, 1:2, :]

            @pl.when(has_next)
            def _():
                advising[u].start()

        @pl.when(has_prev)
        def _():
            spread_items(totals[slot + 1], counts[last], 1, stats + 2 * u)
            finish(u, 0, stats + 2 * u)

    def last_rolls(u):
        unpack_top(own + u)
        for copy, low, size in landing[own + u]:
            copy.wait_recv()
            roll_only(u, low, size)

    late = own - 1
    for g in range(len(groups)):
        main_first(g)
    for u in range(late):
        tail_first(u)
        tail_exchange(u)

    @pl.when(tm == 0)
    def _():
        tail_first(late)
        tail_exchange(late)

    receive(0)
    for i in range(2):
        b = 0 if i == 0 else blocks
        counts[last, i:i + 1, :] = jnp.maximum(totals[0, b:b + 1, :], 1.0)
    main_counts(0)
    main_second(0)

    @pl.when(has_prev)
    def _():
        tail_first(late)
        tail_exchange(late)

    for g in range(1, len(groups)):
        main_counts(g)
        main_second(g)
    for u in range(late):
        tail_scores(u)

    @pl.when(tm == 0)
    def _():
        tail_scores(late)

    for g in range(len(groups) - 1):
        main_third(g)

    @pl.when(has_prev)
    def _():
        tail_scores(late)

    @pl.when(has_prev)
    def _():
        main_third(len(groups) - 1)

    for u in range(late):
        tail_last(u)

    @pl.when(has_prev)
    def _():
        for u in range(helped - 1):
            last_rolls(u)

    tail_last(late)

    @pl.when(tm == 0)
    def _():
        main_third(len(groups) - 1)

    @pl.when(has_prev)
    def _():
        for u in range(helped - 1, helped):
            last_rolls(u)
        head_count[...] = jnp.broadcast_to(counts[last, :1, :], head_count.shape)
        wait_for(advised.at[pl.ds(0, helped)], sent_sem.at[3])

    head_rows = pl.ds(0, WINDOW)

    @pl.when(has_prev)
    def _():
        wait_for(x.at[pl.ds(own, helped), head_rows, pl.ds(0, assets)], sent_sem.at[1])

    @pl.when(has_next)
    def _():
        wait_for(x.at[0, head_rows, pl.ds(0, assets)], sent_sem.at[0])
        if fields > 1:
            later_rows = pl.ds(SUBLANES, WINDOW - SUBLANES)
            wait_for(x.at[pl.ds(1, fields - 1), later_rows, pl.ds(0, assets)], sent_sem.at[6])
            wait_for(packed, sent_sem.at[7])
        wait_for(advice.at[pl.ds(0, helped)], sent_sem.at[2])

    wait_for(got.at[pl.ds(0, tail)], sent_sem.at[4])
    wait_for(got.at[pl.ds(tail, 2 * own), :, pl.ds(0, 2)], sent_sem.at[5])


def finisher(
    own, out, rolled, head_weight, advised, head_count, result, head, columns_of, sem,
):
    fields, rows, assets = out.shape
    helped = fields - own
    below = pl.ds(WINDOW, rows - WINDOW)
    tm = lax.axis_index("tm")
    copies = [
        pltpu.make_async_copy(out.at[f, below], result.at[f, below], sem)
        for f in range(fields)
    ]
    done = [
        pltpu.make_async_copy(out.at[f, :WINDOW], result.at[f, :WINDOW], sem)
        for f in range(fields)
    ]
    finished = [
        pltpu.make_async_copy(head.at[u], result.at[own + u, :WINDOW], sem)
        for u in range(helped)
    ]
    for copy in copies + done[:own]:
        copy.start()

    @pl.when(tm == 0)
    def _():
        for copy in done[own:]:
            copy.start()

    @pl.when(tm > 0)
    def _():
        for u in range(helped):
            spread(columns_of, advised[u], head_count[...], 2, 2 * u)
        for u in range(helped):
            center, scale = columns_of[2 * u, :WINDOW, :], columns_of[2 * u, WINDOW:, :]
            middle, factor = columns_of[2 * u + 1, :WINDOW, :], columns_of[2 * u + 1, WINDOW:, :]

            @pl.loop(0, assets // LANES, unroll=2)
            def chunk(c):
                cols = chunk_columns(c)
                scored = (rolled[u, :, cols] - center) * scale
                clipped = jnp.minimum(jnp.maximum(scored, -CLIP), CLIP)
                head[u, :, cols] = (clipped - middle) * head_weight[:, cols] * factor

            finished[u].start()

    pltpu.make_async_copy(out, out, sem).wait()


def per_device(n_tm, n_as, values, listed_from, listed_until):
    fields, rows, assets = values.shape
    blocks = rows // WINDOW
    groups = field_groups(fields)
    own = groups[0][1]
    stats = -(-max(own * blocks, blocks + 2) // SUBLANES) * SUBLANES
    slots = 1 + 2 * len(groups) + 2 * own
    cuts = len(halo_pieces(fields, own, assets // LANES))
    back_cuts = max(len(back_pieces(fields, own, assets // LANES)), 1)
    f32 = jnp.float32
    vmem = pltpu.VMEM
    dma = pltpu.SemaphoreType.DMA
    helped = max(fields - own, 1)
    chunks = assets // LANES
    kept = chunks - (chunks // SUBLANES if chunks % SUBLANES == 0 else 0)
    parts = (
        vmem((fields, rows, assets), f32),
        vmem((helped, WINDOW, assets + LANES), f32),
        vmem((WINDOW, assets + LANES), f32),
        vmem((own, SUBLANES, LANES), f32),
        vmem((SUBLANES, LANES), f32),
    )
    in_vmem = [pl.BlockSpec(memory_space=vmem)] * len(parts)
    outputs = pl.pallas_call(
        functools.partial(kernel, n_tm, n_as),
        out_shape=parts,
        in_specs=[pl.BlockSpec(memory_space=pltpu.HBM)] * 3,
        out_specs=in_vmem,
        scratch_shapes=[
            vmem((fields, WINDOW + rows + WINDOW, assets + LANES), f32),
            vmem((fields, rows + WINDOW, assets + LANES), f32),
            vmem((WINDOW + rows + WINDOW, assets + LANES), f32),
            vmem((WINDOW + rows + WINDOW, assets + LANES), f32),
            vmem((1, assets), jnp.int32),
            vmem((1, assets), jnp.int32),
            vmem((stats + 2 * own, LANES, LANES), f32),
            vmem((stats + 2 * own, LANES, LANES), f32),
            vmem((max(fields - 1, 1), SUBLANES, kept * LANES), f32),
            vmem((slots, stats, LANES), f32),
            vmem((slots, n_as - 1, stats, LANES), f32),
            vmem((slots, stats, LANES), f32),
            vmem((len(groups) + 1, stats, LANES), f32),
            vmem((own, SUBLANES, LANES), f32),
            dma((len(groups) + 2,)),
            dma((8,)),
            dma((cuts,)),
            dma((max(fields - 1, 1),)),
            dma((back_cuts,)),
            dma((slots,)),
            pltpu.SemaphoreType.REGULAR((max(greeting_rounds(n_as), 1),)),
        ],
        compiler_params=pltpu.CompilerParams(
            collective_id=0, has_side_effects=True, vmem_limit_bytes=48 * 2**20
        ),
    )(values, listed_from[None], listed_until[None])
    return pl.pallas_call(
        functools.partial(finisher, own),
        out_shape=jax.ShapeDtypeStruct((fields, rows, assets), f32),
        in_specs=in_vmem,
        out_specs=pl.BlockSpec(memory_space=pltpu.HBM),
        scratch_shapes=[
            vmem((helped, WINDOW, assets), f32),
            vmem((2 * own, LANES, LANES), f32),
            dma(()),
        ],
        compiler_params=pltpu.CompilerParams(vmem_limit_bytes=4 * 2**20),
    )(*outputs)


def solution(mesh):
    in_specs = (P(None, "tm", "asset"), P("asset"), P("asset"))
    out_specs = P(None, "tm", "asset")
    body = functools.partial(per_device, mesh.shape["tm"], mesh.shape["asset"])
    return jax.shard_map(
        body, mesh=mesh, in_specs=in_specs, out_specs=out_specs, check_vma=False
    )
```

```python
import functools

import jax
import jax.numpy as jnp
from jax import lax
from jax.experimental import pallas as pl
from jax.experimental.pallas import tpu as pltpu
from jax.sharding import PartitionSpec as P

WINDOW = 64
LANES = 128
SUBLANES = 8
CLIP = 3.0
ROLL_UNROLL = 8
UNROLL = 4
CUTS = 4


def field_groups(fields):
    half = (fields + 1) // 2
    return [(start, min(half, fields - start)) for start in range(0, fields, half)]


def lane_pieces(fields, split, chunks):
    pieces = []
    for f in fields:
        cuts = CUTS if f in split and chunks % CUTS == 0 else 1
        size = chunks // cuts
        pieces += [(f, c * size, size) for c in range(cuts)]
    return pieces


def halo_pieces(fields, own, chunks):
    return lane_pieces(range(fields), (own - 1, fields - 1), chunks)


def back_pieces(fields, own, chunks):
    return lane_pieces(range(own, fields), (fields - 1,), chunks)


def greeting_rounds(n):
    if n % 2:
        return 0
    return max(n // 2 - 1, 0)


def spread(columns_of, sums, count, items, first=0):
    mean = sums / count
    other = pltpu.roll(mean, WINDOW, 1)
    scale = 1.0 / jnp.sqrt(jnp.maximum(mean - other * other, 0.0) + 0.1)
    lane = lax.broadcasted_iota(jnp.int32, mean.shape, 1)
    row = jnp.where(lane < WINDOW, mean, scale)
    for i in range(items):
        columns_of[first + i] = jnp.broadcast_to(row[i:i + 1], (LANES, LANES)).T


def chunk_columns(c):
    return pl.ds(pl.multiple_of(c * LANES, LANES), LANES)


def kernel(
    n_tm, n_as, values, opened_hbm, closed_hbm,
    out, rolled, head_weight, advised, head_count,
    x, rolling, weight, inverse, opened_ref, closed_ref,
    acc, columns_of, packed, part, got, totals, counts, advice,
    load_sem, sent_sem, halo_recv, top_recv, back_recv, recv_sem, hello,
):
    fields, rows, assets = values.shape
    blocks = rows // WINDOW
    chunks = assets // LANES
    tiles = WINDOW // SUBLANES
    groups = field_groups(fields)
    own = groups[0][1]
    helped = fields - own
    stats = part.shape[1]
    tail = 1 + 2 * len(groups)
    last = len(groups)
    tm = lax.axis_index("tm")
    me = lax.axis_index("asset")
    later = lax.rem(tm + 1, n_tm)
    before = lax.rem(tm + n_tm - 1, n_tm)
    has_next = tm < n_tm - 1
    has_prev = tm > 0

    def wait_for(ref, semaphore):
        pltpu.make_async_copy(ref, ref, semaphore).wait()

    dates = [
        pltpu.make_async_copy(opened_hbm, opened_ref, load_sem.at[len(groups)]),
        pltpu.make_async_copy(closed_hbm, closed_ref, load_sem.at[len(groups) + 1]),
    ]
    loads = [
        pltpu.make_async_copy(
            values.at[f], x.at[f, pl.ds(WINDOW, rows), pl.ds(0, assets)], load_sem.at[f // own]
        )
        for f in range(fields)
    ]

    barrier = pltpu.get_barrier_semaphore()
    rounds = greeting_rounds(n_as)

    @pl.when(has_next)
    def _():
        pl.semaphore_signal(barrier, inc=1, device_id={"tm": later})

    @pl.when(has_prev)
    def _():
        pl.semaphore_signal(barrier, inc=1, device_id={"tm": before})

    def greet(semaphore):
        if n_as % 2:
            for d in range(1, n_as):
                pl.semaphore_signal(semaphore, inc=1, device_id={"asset": lax.rem(me + d, n_as)})
            return n_as - 1
        beside = me + 1 - 2 * lax.rem(me, 2)
        pl.semaphore_signal(semaphore, inc=1, device_id={"asset": beside})

        @pl.when(me >= 2)
        def _():
            pl.semaphore_signal(semaphore, inc=1, device_id={"asset": me - 2})

        @pl.when(me + 2 < n_as)
        def _():
            pl.semaphore_signal(semaphore, inc=1, device_id={"asset": me + 2})

        return 1 + jnp.where(me >= 2, 1, 0) + jnp.where(me + 2 < n_as, 1, 0)

    near = greet(barrier)
    expected = near + jnp.where(has_next, 1, 0) + jnp.where(has_prev, 1, 0)
    for copy in dates + loads:
        copy.start()

    kept = packed.shape[2] // LANES
    landing = {f: [] for f in range(fields)}
    tops = {}
    for i, (f, first, size) in enumerate(halo_pieces(fields, own, chunks)):
        cols = pl.ds(first * LANES, size * LANES)
        skip = SUBLANES if f else 0
        copy = pltpu.make_async_remote_copy(
            src_ref=values.at[f, pl.ds(rows - WINDOW + skip, WINDOW - skip), cols],
            dst_ref=x.at[f, pl.ds(skip, WINDOW - skip), cols],
            send_sem=sent_sem.at[6 if f else 0],
            recv_sem=halo_recv.at[i],
            device_id={"tm": later},
        )
        landing[f].append((copy, first, size))
    for f in range(1, fields):
        tops[f] = pltpu.make_async_remote_copy(
            src_ref=packed.at[f - 1],
            dst_ref=x.at[f, pl.ds(0, SUBLANES), pl.ds(0, kept * LANES)],
            send_sem=sent_sem.at[7],
            recv_sem=top_recv.at[f - 1],
            device_id={"tm": later},
        )

    def tile_columns(c):
        return pl.ds(c * LANES, LANES)

    def pack_top(f):
        sublane = lax.broadcasted_iota(jnp.int32, (SUBLANES, LANES), 0)
        for c in range(kept):
            tile = x[f, pl.ds(rows, SUBLANES), tile_columns(c)]
            if kept < chunks:
                extra, row = kept + c // (SUBLANES - 1), 1 + c % (SUBLANES - 1)
                other = x[f, pl.ds(rows, SUBLANES), tile_columns(extra)][row:row + 1]
                tile = jnp.where(sublane == 0, jnp.broadcast_to(other, tile.shape), tile)
            packed[f - 1, :, tile_columns(c)] = tile

    def unpack_top(f):
        if f == 0:
            return
        tops[f].wait_recv()
        sublane = lax.broadcasted_iota(jnp.int32, (SUBLANES, LANES), 0)
        for extra in range(chunks - kept):
            tile = jnp.zeros((SUBLANES, LANES), jnp.float32)
            for k in range(SUBLANES - 1):
                from_tile = tile_columns((SUBLANES - 1) * extra + k)
                row = x[f, pl.ds(0, SUBLANES), from_tile][:1]
                tile = jnp.where(sublane == 1 + k, jnp.broadcast_to(row, tile.shape), tile)
            x[f, pl.ds(0, SUBLANES), tile_columns(kept + extra)] = tile

    def start_halo(f):
        if f > 0:
            tops[f].start()
        for copy, _, _ in landing[f]:
            copy.start()

    returning = {f: [] for f in range(own, fields)}
    backs = []
    for i, (f, first, size) in enumerate(back_pieces(fields, own, chunks)):
        cols = pl.ds(first * LANES, size * LANES)
        backs.append(pltpu.make_async_remote_copy(
            src_ref=values.at[f, pl.ds(0, WINDOW), cols],
            dst_ref=x.at[f, pl.ds(WINDOW + rows, WINDOW), cols],
            send_sem=sent_sem.at[1],
            recv_sem=back_recv.at[i],
            device_id={"tm": before},
        ))
        returning[f].append((backs[-1], first, size))
    advising = [
        pltpu.make_async_remote_copy(
            src_ref=advice.at[u],
            dst_ref=advised.at[u],
            send_sem=sent_sem.at[2],
            recv_sem=sent_sem.at[3],
            device_id={"tm": later},
        )
        for u in range(helped)
    ]
    odd = lax.rem(tm, 2) == 1

    def rows_of(slot):
        return pl.ds(0, 2 if slot >= tail else stats)

    def send(slot):
        for d in range(1, n_as):
            pltpu.make_async_remote_copy(
                src_ref=part.at[slot, rows_of(slot)],
                dst_ref=got.at[slot, d - 1, rows_of(slot)],
                send_sem=sent_sem.at[5 if slot >= tail else 4],
                recv_sem=recv_sem.at[slot],
                device_id={"asset": lax.rem(me + d, n_as)},
            ).start()

    def receive(slot):
        arrived = got.at[slot, :, rows_of(slot)]
        wait_for(arrived, recv_sem.at[slot])
        totals[slot] = part[slot] + jnp.sum(got[slot], axis=0)

    def reduce_items(slot, items, first=0):
        for i in range(items):
            part[slot, i:i + 1, :] = jnp.sum(acc[first + i].T, axis=0, keepdims=True)

    def spread_items(sums, count, items, first=0):
        spread(columns_of, sums, count, items, first)

    def column_pair(i):
        return columns_of[i, :WINDOW, :], columns_of[i, WINDOW:, :]

    zero = jnp.zeros((WINDOW, LANES), jnp.float32)
    first_stamp = tm * rows - WINDOW

    def start_listing():
        part[...] = jnp.zeros(part.shape, part.dtype)
        acc[...] = jnp.zeros(acc.shape, acc.dtype)
        for copy in dates:
            copy.wait()

        @pl.when(tm == 0)
        def _():
            @pl.loop(0, fields)
            def clear(f):
                x[f, pl.ds(0, WINDOW), pl.ds(0, assets)] = jnp.zeros((WINDOW, assets), jnp.float32)

    def listing(b):
        start = pl.multiple_of(b * WINDOW, WINDOW)
        row = lax.broadcasted_iota(jnp.int32, (WINDOW, LANES), 0)
        passed = (first_stamp + start + 1 + row).astype(jnp.float32)

        def chunk(c, total):
            cols = chunk_columns(c)
            opened = jnp.maximum(opened_ref[:, cols], 0).astype(jnp.float32)
            closed = closed_ref[:, cols].astype(jnp.float32)
            age = passed - opened
            listed = (age > 0.0) & (passed <= closed)
            ones = jnp.where(listed, 1.0, 0.0)
            weight[pl.ds(start, WINDOW), cols] = ones
            counted = jnp.minimum(jnp.maximum(age, 1.0), float(WINDOW))
            inverse[pl.ds(start, WINDOW), cols] = ones / counted
            return total + ones

        total = lax.fori_loop(0, chunks, chunk, zero, unroll=2)
        at = lax.rem(b + blocks + 1, blocks + 2)
        acc[at, :WINDOW, :] = total
        acc[at, WINDOW:, :] = total

    def listing_blocks(low, high):
        pl.loop(low, high)(listing)

    @pl.when(tm == 0)
    def _():
        start_listing()
        listing_blocks(0, blocks)

    pl.semaphore_wait(barrier, expected)

    @pl.when(has_prev & ~odd)
    def _():
        for copy in backs:
            copy.start()

    @pl.when(has_next)
    def _():
        start_halo(0)

    @pl.when(has_prev & odd)
    def _():
        for copy in backs:
            copy.start()

    if rounds:
        greet(hello.at[0])

    @pl.when(has_prev)
    def _():
        start_listing()
        listing_blocks(0, blocks)

    listing_blocks(blocks, blocks + 2)

    def next_round(r):
        pl.semaphore_wait(hello.at[r], near)
        if r + 1 < rounds:
            greet(hello.at[r + 1])

    for r in range(rounds - 2):
        next_round(r)
    reduce_items(0, blocks + 1)

    def window_means(f, b, c):
        top = pl.multiple_of(b * WINDOW, WINDOW)
        cols = chunk_columns(c)
        sublane = lax.broadcasted_iota(jnp.int32, (SUBLANES, LANES), 0)

        ends = range(2 * tiles)
        reach = pl.ds(top, 2 * WINDOW)
        masked = x[f, reach, cols] * weight[reach, cols]
        sums = {j: masked[SUBLANES * j:SUBLANES * (j + 1)] for j in ends}
        step = 1
        while step < tiles:
            sums = {j: sums[j] + sums[j - step] for j in ends if j - step in sums}
            step *= 2
        shift = 1
        while shift < SUBLANES:
            keep = sublane < SUBLANES - shift
            moved = {tiles - 1: sums[tiles - 1]}
            for j in range(tiles, 2 * tiles):
                moved[j] = jnp.where(keep, sums[j], sums[j - 1])
            sums = {j: sums[j] + pltpu.roll(moved[j], shift, 0) for j in moved}
            shift *= 2
        ending = jnp.concatenate([sums[j] for j in range(tiles, 2 * tiles)], axis=0)
        return ending * inverse[pl.ds(top + WINDOW, WINDOW), cols]

    def roll_window(f, b, i, low=0, size=chunks):
        top = pl.multiple_of(b * WINDOW, WINDOW)

        def chunk(c, carry):
            means = window_means(f, b, c)
            rolling[f, pl.ds(top, WINDOW), chunk_columns(c)] = means
            return carry[0] + means, carry[1] + means * means

        carry = (zero, zero) if low == 0 else (acc[i, :WINDOW, :], acc[i, WINDOW:, :])
        first, second = lax.fori_loop(
            low, low + size, chunk, carry, unroll=min(ROLL_UNROLL, size)
        )
        acc[i, :WINDOW, :] = first
        acc[i, WINDOW:, :] = second

    def clip_scores(f, b, i):
        top = pl.multiple_of(b * WINDOW, WINDOW)
        center, scale = column_pair(i)

        def chunk(c, carry):
            cols = chunk_columns(c)
            here = pl.ds(top, WINDOW)
            scored = (rolling[f, here, cols] - center) * scale
            clipped = jnp.minimum(jnp.maximum(scored, -CLIP), CLIP)
            rolling[f, here, cols] = clipped
            masked = clipped * weight[pl.ds(top + WINDOW, WINDOW), cols]
            return carry[0] + masked, carry[1] + masked * clipped

        first, second = lax.fori_loop(0, chunks, chunk, (zero, zero), unroll=UNROLL)
        acc[i, :WINDOW, :] = first
        acc[i, WINDOW:, :] = second

    def finish(f, b, i):
        top = pl.multiple_of(b * WINDOW, WINDOW)
        middle, factor = column_pair(i)

        @pl.loop(0, chunks, unroll=UNROLL)
        def chunk(c):
            cols = chunk_columns(c)
            here = pl.ds(top, WINDOW)
            deviate = (rolling[f, here, cols] - middle) * weight[pl.ds(top + WINDOW, WINDOW), cols]
            out[f, here, cols] = deviate * factor

    def roll_only(u, low, size):
        @pl.loop(low, low + size, unroll=min(UNROLL, size))
        def chunk(c):
            cols = chunk_columns(c)
            rolled[u, :, cols] = window_means(own + u, 0, c)
            if u == 0:
                head_weight[:, cols] = weight[WINDOW:2 * WINDOW, cols]

    def main_items(g):
        size = groups[g][1]
        return pl.loop(jnp.where(tm == 0, 0, size), size * blocks)

    def main_first(g):
        start, size = groups[g]
        block = x.at[pl.ds(start, size), pl.ds(WINDOW, rows), pl.ds(0, assets)]
        wait_for(block, load_sem.at[g])
        ahead = [f for f in range(start, start + size) if f > 0]

        @pl.when(has_next)
        def _():
            for f in ahead:
                pack_top(f)

        def middle():
            @pl.when(has_next)
            def _():
                for f in ahead:
                    start_halo(f)

            if g == 0 and rounds > 1:
                next_round(rounds - 2)

        @main_items(g)
        def item(i):
            roll_window(start + lax.rem(i, size), lax.div(i, size), i)
            pl.when(i == (size + size * blocks) // 2)(middle)

        reduce_items(1 + 2 * g, size * blocks)
        if g == 0:
            if rounds:
                next_round(rounds - 1)
            send(0)
        send(1 + 2 * g)

    def main_counts(g):
        size = groups[g][1]
        for i in range(size * blocks):
            b = i // size
            counts[g, i:i + 1, :] = jnp.maximum(totals[0, b:b + 1, :], 1.0)

    def main_second(g):
        start, size = groups[g]
        slot = 1 + 2 * g
        receive(slot)
        spread_items(totals[slot], counts[g], size * blocks)

        @main_items(g)
        def item(i):
            clip_scores(start + lax.rem(i, size), lax.div(i, size), i)

        reduce_items(slot + 1, size * blocks)
        send(slot + 1)

    def main_third(g):
        start, size = groups[g]
        slot = 2 + 2 * g
        receive(slot)
        spread_items(totals[slot], counts[g], size * blocks)

        @main_items(g)
        def item(i):
            finish(start + lax.rem(i, size), lax.div(i, size), i)

    def tail_own(u):
        unpack_top(u)
        for copy, low, size in landing[u]:
            copy.wait_recv()
            roll_window(u, 0, stats + 2 * u, low, size)

    def tail_help(u):
        for copy, low, size in returning[own + u]:
            copy.wait_recv()
            roll_window(own + u, blocks, stats + 2 * u + 1, low, size)

    def tail_first(u):
        pl.when(has_prev & odd)(functools.partial(tail_own, u))
        if u < helped:
            pl.when(has_next)(functools.partial(tail_help, u))
        pl.when(has_prev & ~odd)(functools.partial(tail_own, u))

    def tail_second(u):
        @pl.when(has_prev)
        def _():
            clip_scores(u, 0, stats + 2 * u)

        if u < helped:
            @pl.when(has_next)
            def _():
                clip_scores(own + u, blocks, stats + 2 * u + 1)

    def tail_exchange(u):
        reduce_items(tail + 2 * u, 2, stats + 2 * u)
        send(tail + 2 * u)

    def tail_scores(u):
        slot = tail + 2 * u
        receive(slot)
        spread_items(totals[slot], counts[last], 2, stats + 2 * u)
        tail_second(u)
        reduce_items(slot + 1, 2, stats + 2 * u)
        send(slot + 1)

    def tail_last(u):
        slot = tail + 2 * u
        receive(slot + 1)
        if u < helped:
            advice[u, :1, :] = totals[slot, 1:2, :]
            advice[u, 1:2, :] = totals[slot + 1, 1:2, :]

            @pl.when(has_next)
            def _():
                advising[u].start()

        @pl.when(has_prev)
        def _():
            spread_items(totals[slot + 1], counts[last], 1, stats + 2 * u)
            finish(u, 0, stats + 2 * u)

    def last_rolls(u):
        unpack_top(own + u)
        for copy, low, size in landing[own + u]:
            copy.wait_recv()
            roll_only(u, low, size)

    late = own - 1
    for g in range(len(groups)):
        main_first(g)
    for u in range(late):
        tail_first(u)
        tail_exchange(u)

    @pl.when(tm == 0)
    def _():
        tail_first(late)
        tail_exchange(late)

    receive(0)
    for i in range(2):
        b = 0 if i == 0 else blocks
        counts[last, i:i + 1, :] = jnp.maximum(totals[0, b:b + 1, :], 1.0)
    main_counts(0)
    main_second(0)

    @pl.when(has_prev)
    def _():
        tail_first(late)
        tail_exchange(late)

    for g in range(1, len(groups)):
        main_counts(g)
        main_second(g)
    for u in range(late):
        tail_scores(u)

    @pl.when(tm == 0)
    def _():
        tail_scores(late)

    for g in range(len(groups) - 1):
        main_third(g)

    @pl.when(has_prev)
    def _():
        tail_scores(late)

    @pl.when(has_prev)
    def _():
        main_third(len(groups) - 1)

    for u in range(late):
        tail_last(u)

    @pl.when(has_prev)
    def _():
        for u in range(helped - 1):
            last_rolls(u)

    tail_last(late)

    @pl.when(tm == 0)
    def _():
        main_third(len(groups) - 1)

    @pl.when(has_prev)
    def _():
        for u in range(helped - 1, helped):
            last_rolls(u)
        head_count[...] = jnp.broadcast_to(counts[last, :1, :], head_count.shape)
        wait_for(advised.at[pl.ds(0, helped)], sent_sem.at[3])

    head_rows = pl.ds(0, WINDOW)

    @pl.when(has_prev)
    def _():
        wait_for(x.at[pl.ds(own, helped), head_rows, pl.ds(0, assets)], sent_sem.at[1])

    @pl.when(has_next)
    def _():
        wait_for(x.at[0, head_rows, pl.ds(0, assets)], sent_sem.at[0])
        if fields > 1:
            later_rows = pl.ds(SUBLANES, WINDOW - SUBLANES)
            wait_for(x.at[pl.ds(1, fields - 1), later_rows, pl.ds(0, assets)], sent_sem.at[6])
            wait_for(packed, sent_sem.at[7])
        wait_for(advice.at[pl.ds(0, helped)], sent_sem.at[2])

    wait_for(got.at[pl.ds(0, tail)], sent_sem.at[4])
    wait_for(got.at[pl.ds(tail, 2 * own), :, pl.ds(0, 2)], sent_sem.at[5])


def finisher(
    own, out, rolled, head_weight, advised, head_count, result, head, columns_of, sem,
):
    fields, rows, assets = out.shape
    helped = fields - own
    below = pl.ds(WINDOW, rows - WINDOW)
    tm = lax.axis_index("tm")
    copies = [
        pltpu.make_async_copy(out.at[f, below], result.at[f, below], sem)
        for f in range(fields)
    ]
    done = [
        pltpu.make_async_copy(out.at[f, :WINDOW], result.at[f, :WINDOW], sem)
        for f in range(fields)
    ]
    finished = [
        pltpu.make_async_copy(head.at[u], result.at[own + u, :WINDOW], sem)
        for u in range(helped)
    ]
    whole = [pltpu.make_async_copy(out.at[f], result.at[f], sem) for f in range(own)]
    for copy in whole + copies[own:]:
        copy.start()

    @pl.when(tm == 0)
    def _():
        for copy in done[own:]:
            copy.start()

    @pl.when(tm > 0)
    def _():
        for u in range(helped):
            spread(columns_of, advised[u], head_count[...], 2, 2 * u)
        for u in range(helped):
            center, scale = columns_of[2 * u, :WINDOW, :], columns_of[2 * u, WINDOW:, :]
            middle, factor = columns_of[2 * u + 1, :WINDOW, :], columns_of[2 * u + 1, WINDOW:, :]

            @pl.loop(0, assets // LANES, unroll=2)
            def chunk(c):
                cols = chunk_columns(c)
                scored = (rolled[u, :, cols] - center) * scale
                clipped = jnp.minimum(jnp.maximum(scored, -CLIP), CLIP)
                head[u, :, cols] = (clipped - middle) * head_weight[:, cols] * factor

            finished[u].start()

    pltpu.make_async_copy(out, out, sem).wait()


def per_device(n_tm, n_as, values, listed_from, listed_until):
    fields, rows, assets = values.shape
    blocks = rows // WINDOW
    groups = field_groups(fields)
    own = groups[0][1]
    stats = -(-max(own * blocks, blocks + 2) // SUBLANES) * SUBLANES
    slots = 1 + 2 * len(groups) + 2 * own
    cuts = len(halo_pieces(fields, own, assets // LANES))
    back_cuts = max(len(back_pieces(fields, own, assets // LANES)), 1)
    f32 = jnp.float32
    vmem = pltpu.VMEM
    dma = pltpu.SemaphoreType.DMA
    helped = max(fields - own, 1)
    chunks = assets // LANES
    kept = chunks - (chunks // SUBLANES if chunks % SUBLANES == 0 else 0)
    parts = (
        vmem((fields, rows, assets), f32),
        vmem((helped, WINDOW, assets + LANES), f32),
        vmem((WINDOW, assets + LANES), f32),
        vmem((own, SUBLANES, LANES), f32),
        vmem((SUBLANES, LANES), f32),
    )
    in_vmem = [pl.BlockSpec(memory_space=vmem)] * len(parts)
    outputs = pl.pallas_call(
        functools.partial(kernel, n_tm, n_as),
        out_shape=parts,
        in_specs=[pl.BlockSpec(memory_space=pltpu.HBM)] * 3,
        out_specs=in_vmem,
        scratch_shapes=[
            vmem((fields, WINDOW + rows + WINDOW, assets + LANES), f32),
            vmem((fields, rows + WINDOW, assets + LANES), f32),
            vmem((WINDOW + rows + WINDOW, assets + LANES), f32),
            vmem((WINDOW + rows + WINDOW, assets + LANES), f32),
            vmem((1, assets), jnp.int32),
            vmem((1, assets), jnp.int32),
            vmem((stats + 2 * own, LANES, LANES), f32),
            vmem((stats + 2 * own, LANES, LANES), f32),
            vmem((max(fields - 1, 1), SUBLANES, kept * LANES), f32),
            vmem((slots, stats, LANES), f32),
            vmem((slots, n_as - 1, stats, LANES), f32),
            vmem((slots, stats, LANES), f32),
            vmem((len(groups) + 1, stats, LANES), f32),
            vmem((own, SUBLANES, LANES), f32),
            dma((len(groups) + 2,)),
            dma((8,)),
            dma((cuts,)),
            dma((max(fields - 1, 1),)),
            dma((back_cuts,)),
            dma((slots,)),
            pltpu.SemaphoreType.REGULAR((max(greeting_rounds(n_as), 1),)),
        ],
        compiler_params=pltpu.CompilerParams(
            collective_id=0, has_side_effects=True, vmem_limit_bytes=48 * 2**20
        ),
    )(values, listed_from[None], listed_until[None])
    return pl.pallas_call(
        functools.partial(finisher, own),
        out_shape=jax.ShapeDtypeStruct((fields, rows, assets), f32),
        in_specs=in_vmem,
        out_specs=pl.BlockSpec(memory_space=pltpu.HBM),
        scratch_shapes=[
            vmem((helped, WINDOW, assets), f32),
            vmem((2 * own, LANES, LANES), f32),
            dma(()),
        ],
        compiler_params=pltpu.CompilerParams(vmem_limit_bytes=4 * 2**20),
    )(*outputs)


def solution(mesh):
    in_specs = (P(None, "tm", "asset"), P("asset"), P("asset"))
    out_specs = P(None, "tm", "asset")
    body = functools.partial(per_device, mesh.shape["tm"], mesh.shape["asset"])
    return jax.shard_map(
        body, mesh=mesh, in_specs=in_specs, out_specs=out_specs, check_vma=False
    )
```

```python
import functools

import jax
import jax.numpy as jnp
from jax import lax
from jax.experimental import pallas as pl
from jax.experimental.pallas import tpu as pltpu
from jax.sharding import PartitionSpec as P

WINDOW = 64
LANES = 128
SUBLANES = 8
CLIP = 3.0
ROLL_UNROLL = 8
UNROLL = 4
CUTS = 4


def field_groups(fields):
    half = (fields + 1) // 2
    return [(start, min(half, fields - start)) for start in range(0, fields, half)]


def lane_pieces(fields, split, chunks):
    pieces = []
    for f in fields:
        cuts = CUTS if f in split and chunks % CUTS == 0 else 1
        size = chunks // cuts
        pieces += [(f, c * size, size) for c in range(cuts)]
    return pieces


def halo_pieces(fields, own, chunks):
    return lane_pieces(range(fields), (own - 1, fields - 1), chunks)


def back_pieces(fields, own, chunks):
    return lane_pieces(range(own, fields), (fields - 1,), chunks)


def greeting_rounds(n):
    if n % 2:
        return 0
    return max(n // 2 - 1, 0)


def spread(columns_of, sums, count, items, first=0):
    mean = sums / count
    other = pltpu.roll(mean, WINDOW, 1)
    scale = 1.0 / jnp.sqrt(jnp.maximum(mean - other * other, 0.0) + 0.1)
    lane = lax.broadcasted_iota(jnp.int32, mean.shape, 1)
    row = jnp.where(lane < WINDOW, mean, scale)
    for i in range(items):
        columns_of[first + i] = jnp.broadcast_to(row[i:i + 1], (LANES, LANES)).T


def chunk_columns(c):
    return pl.ds(pl.multiple_of(c * LANES, LANES), LANES)


def kernel(
    n_tm, n_as, values, opened_hbm, closed_hbm,
    out, rolled, head_weight, advised, head_count,
    x, rolling, weight, inverse, opened_ref, closed_ref,
    acc, columns_of, packed, part, got, totals, counts, advice,
    load_sem, sent_sem, halo_recv, top_recv, back_recv, recv_sem, hello,
):
    fields, rows, assets = values.shape
    blocks = rows // WINDOW
    chunks = assets // LANES
    tiles = WINDOW // SUBLANES
    groups = field_groups(fields)
    own = groups[0][1]
    helped = fields - own
    stats = part.shape[1]
    tail = 1 + 2 * len(groups)
    last = len(groups)
    tm = lax.axis_index("tm")
    me = lax.axis_index("asset")
    later = lax.rem(tm + 1, n_tm)
    before = lax.rem(tm + n_tm - 1, n_tm)
    has_next = tm < n_tm - 1
    has_prev = tm > 0

    def wait_for(ref, semaphore):
        pltpu.make_async_copy(ref, ref, semaphore).wait()

    dates = [
        pltpu.make_async_copy(opened_hbm, opened_ref, load_sem.at[len(groups)]),
        pltpu.make_async_copy(closed_hbm, closed_ref, load_sem.at[len(groups) + 1]),
    ]
    loads = [
        pltpu.make_async_copy(
            values.at[f], x.at[f, pl.ds(WINDOW, rows), pl.ds(0, assets)], load_sem.at[f // own]
        )
        for f in range(fields)
    ]

    barrier = pltpu.get_barrier_semaphore()
    rounds = greeting_rounds(n_as)

    @pl.when(has_next)
    def _():
        pl.semaphore_signal(barrier, inc=1, device_id={"tm": later})

    @pl.when(has_prev)
    def _():
        pl.semaphore_signal(barrier, inc=1, device_id={"tm": before})

    def greet(semaphore):
        if n_as % 2:
            for d in range(1, n_as):
                pl.semaphore_signal(semaphore, inc=1, device_id={"asset": lax.rem(me + d, n_as)})
            return n_as - 1
        beside = me + 1 - 2 * lax.rem(me, 2)
        pl.semaphore_signal(semaphore, inc=1, device_id={"asset": beside})

        @pl.when(me >= 2)
        def _():
            pl.semaphore_signal(semaphore, inc=1, device_id={"asset": me - 2})

        @pl.when(me + 2 < n_as)
        def _():
            pl.semaphore_signal(semaphore, inc=1, device_id={"asset": me + 2})

        return 1 + jnp.where(me >= 2, 1, 0) + jnp.where(me + 2 < n_as, 1, 0)

    near = greet(barrier)
    expected = near + jnp.where(has_next, 1, 0) + jnp.where(has_prev, 1, 0)
    for copy in dates + loads:
        copy.start()

    kept = packed.shape[2] // LANES
    landing = {f: [] for f in range(fields)}
    tops = {}
    for i, (f, first, size) in enumerate(halo_pieces(fields, own, chunks)):
        cols = pl.ds(first * LANES, size * LANES)
        skip = SUBLANES if f else 0
        copy = pltpu.make_async_remote_copy(
            src_ref=values.at[f, pl.ds(rows - WINDOW + skip, WINDOW - skip), cols],
            dst_ref=x.at[f, pl.ds(skip, WINDOW - skip), cols],
            send_sem=sent_sem.at[6 if f else 0],
            recv_sem=halo_recv.at[i],
            device_id={"tm": later},
        )
        landing[f].append((copy, first, size))
    for f in range(1, fields):
        tops[f] = pltpu.make_async_remote_copy(
            src_ref=packed.at[f - 1],
            dst_ref=x.at[f, pl.ds(0, SUBLANES), pl.ds(0, kept * LANES)],
            send_sem=sent_sem.at[7],
            recv_sem=top_recv.at[f - 1],
            device_id={"tm": later},
        )

    def tile_columns(c):
        return pl.ds(c * LANES, LANES)

    def pack_top(f):
        sublane = lax.broadcasted_iota(jnp.int32, (SUBLANES, LANES), 0)
        for c in range(kept):
            tile = x[f, pl.ds(rows, SUBLANES), tile_columns(c)]
            if kept < chunks:
                extra, row = kept + c // (SUBLANES - 1), 1 + c % (SUBLANES - 1)
                other = x[f, pl.ds(rows, SUBLANES), tile_columns(extra)][row:row + 1]
                tile = jnp.where(sublane == 0, jnp.broadcast_to(other, tile.shape), tile)
            packed[f - 1, :, tile_columns(c)] = tile

    def unpack_top(f):
        if f == 0:
            return
        tops[f].wait_recv()
        sublane = lax.broadcasted_iota(jnp.int32, (SUBLANES, LANES), 0)
        for extra in range(chunks - kept):
            tile = jnp.zeros((SUBLANES, LANES), jnp.float32)
            for k in range(SUBLANES - 1):
                from_tile = tile_columns((SUBLANES - 1) * extra + k)
                row = x[f, pl.ds(0, SUBLANES), from_tile][:1]
                tile = jnp.where(sublane == 1 + k, jnp.broadcast_to(row, tile.shape), tile)
            x[f, pl.ds(0, SUBLANES), tile_columns(kept + extra)] = tile

    def start_halo(f):
        if f > 0:
            tops[f].start()
        for copy, _, _ in landing[f]:
            copy.start()

    returning = {f: [] for f in range(own, fields)}
    backs = []
    for i, (f, first, size) in enumerate(back_pieces(fields, own, chunks)):
        cols = pl.ds(first * LANES, size * LANES)
        backs.append(pltpu.make_async_remote_copy(
            src_ref=values.at[f, pl.ds(0, WINDOW), cols],
            dst_ref=x.at[f, pl.ds(WINDOW + rows, WINDOW), cols],
            send_sem=sent_sem.at[1],
            recv_sem=back_recv.at[i],
            device_id={"tm": before},
        ))
        returning[f].append((backs[-1], first, size))
    advising = [
        pltpu.make_async_remote_copy(
            src_ref=advice.at[u],
            dst_ref=advised.at[u],
            send_sem=sent_sem.at[2],
            recv_sem=sent_sem.at[3],
            device_id={"tm": later},
        )
        for u in range(helped)
    ]
    odd = lax.rem(tm, 2) == 1

    def rows_of(slot):
        return pl.ds(0, 2 if slot >= tail else stats)

    def send(slot):
        for d in range(1, n_as):
            pltpu.make_async_remote_copy(
                src_ref=part.at[slot, rows_of(slot)],
                dst_ref=got.at[slot, d - 1, rows_of(slot)],
                send_sem=sent_sem.at[5 if slot >= tail else 4],
                recv_sem=recv_sem.at[slot],
                device_id={"asset": lax.rem(me + d, n_as)},
            ).start()

    def receive(slot):
        arrived = got.at[slot, :, rows_of(slot)]
        wait_for(arrived, recv_sem.at[slot])
        totals[slot] = part[slot] + jnp.sum(got[slot], axis=0)

    def reduce_items(slot, items, first=0):
        for i in range(items):
            part[slot, i:i + 1, :] = jnp.sum(acc[first + i].T, axis=0, keepdims=True)

    def spread_items(sums, count, items, first=0):
        spread(columns_of, sums, count, items, first)

    def column_pair(i):
        return columns_of[i, :WINDOW, :], columns_of[i, WINDOW:, :]

    zero = jnp.zeros((WINDOW, LANES), jnp.float32)
    first_stamp = tm * rows - WINDOW

    def start_listing():
        part[...] = jnp.zeros(part.shape, part.dtype)
        acc[...] = jnp.zeros(acc.shape, acc.dtype)
        for copy in dates:
            copy.wait()

        @pl.when(tm == 0)
        def _():
            @pl.loop(0, fields)
            def clear(f):
                x[f, pl.ds(0, WINDOW), pl.ds(0, assets)] = jnp.zeros((WINDOW, assets), jnp.float32)

    def listing(b):
        start = pl.multiple_of(b * WINDOW, WINDOW)
        row = lax.broadcasted_iota(jnp.int32, (WINDOW, LANES), 0)
        passed = (first_stamp + start + 1 + row).astype(jnp.float32)

        def chunk(c, total):
            cols = chunk_columns(c)
            opened = jnp.maximum(opened_ref[:, cols], 0).astype(jnp.float32)
            closed = closed_ref[:, cols].astype(jnp.float32)
            age = passed - opened
            listed = (age > 0.0) & (passed <= closed)
            ones = jnp.where(listed, 1.0, 0.0)
            weight[pl.ds(start, WINDOW), cols] = ones
            counted = jnp.minimum(jnp.maximum(age, 1.0), float(WINDOW))
            inverse[pl.ds(start, WINDOW), cols] = ones / counted
            return total + ones

        total = lax.fori_loop(0, chunks, chunk, zero, unroll=2)
        at = lax.rem(b + blocks + 1, blocks + 2)
        acc[at, :WINDOW, :] = total
        acc[at, WINDOW:, :] = total

    def listing_blocks(low, high):
        pl.loop(low, high)(listing)

    @pl.when(tm == 0)
    def _():
        start_listing()
        listing_blocks(0, blocks)

    pl.semaphore_wait(barrier, expected)

    @pl.when(has_prev & ~odd)
    def _():
        for copy in backs:
            copy.start()

    @pl.when(has_next)
    def _():
        start_halo(0)

    @pl.when(has_prev & odd)
    def _():
        for copy in backs:
            copy.start()

    if rounds:
        greet(hello.at[0])

    @pl.when(has_prev)
    def _():
        start_listing()
        listing_blocks(0, blocks)

    listing_blocks(blocks, blocks + 2)

    def next_round(r):
        pl.semaphore_wait(hello.at[r], near)
        if r + 1 < rounds:
            greet(hello.at[r + 1])

    for r in range(rounds - 2):
        next_round(r)
    reduce_items(0, blocks + 1)

    def window_means(f, b, c):
        top = pl.multiple_of(b * WINDOW, WINDOW)
        cols = chunk_columns(c)
        sublane = lax.broadcasted_iota(jnp.int32, (SUBLANES, LANES), 0)

        ends = range(2 * tiles)
        reach = pl.ds(top, 2 * WINDOW)
        masked = x[f, reach, cols] * weight[reach, cols]
        sums = {j: masked[SUBLANES * j:SUBLANES * (j + 1)] for j in ends}
        step = 1
        while step < tiles:
            sums = {j: sums[j] + sums[j - step] for j in ends if j - step in sums}
            step *= 2
        shift = 1
        while shift < SUBLANES:
            keep = sublane < SUBLANES - shift
            moved = {tiles - 1: sums[tiles - 1]}
            for j in range(tiles, 2 * tiles):
                moved[j] = jnp.where(keep, sums[j], sums[j - 1])
            sums = {j: sums[j] + pltpu.roll(moved[j], shift, 0) for j in moved}
            shift *= 2
        ending = jnp.concatenate([sums[j] for j in range(tiles, 2 * tiles)], axis=0)
        return ending * inverse[pl.ds(top + WINDOW, WINDOW), cols]

    def roll_window(f, b, i, low=0, size=chunks):
        top = pl.multiple_of(b * WINDOW, WINDOW)

        def chunk(c, carry):
            means = window_means(f, b, c)
            rolling[f, pl.ds(top, WINDOW), chunk_columns(c)] = means
            return carry[0] + means, carry[1] + means * means

        carry = (zero, zero) if low == 0 else (acc[i, :WINDOW, :], acc[i, WINDOW:, :])
        first, second = lax.fori_loop(
            low, low + size, chunk, carry, unroll=min(ROLL_UNROLL, size)
        )
        acc[i, :WINDOW, :] = first
        acc[i, WINDOW:, :] = second

    def clip_scores(f, b, i):
        top = pl.multiple_of(b * WINDOW, WINDOW)
        center, scale = column_pair(i)

        def chunk(c, carry):
            cols = chunk_columns(c)
            here = pl.ds(top, WINDOW)
            scored = (rolling[f, here, cols] - center) * scale
            clipped = jnp.minimum(jnp.maximum(scored, -CLIP), CLIP)
            rolling[f, here, cols] = clipped
            masked = clipped * weight[pl.ds(top + WINDOW, WINDOW), cols]
            return carry[0] + masked, carry[1] + masked * clipped

        first, second = lax.fori_loop(0, chunks, chunk, (zero, zero), unroll=UNROLL)
        acc[i, :WINDOW, :] = first
        acc[i, WINDOW:, :] = second

    def finish(f, b, i):
        top = pl.multiple_of(b * WINDOW, WINDOW)
        middle, factor = column_pair(i)

        @pl.loop(0, chunks, unroll=UNROLL)
        def chunk(c):
            cols = chunk_columns(c)
            here = pl.ds(top, WINDOW)
            deviate = (rolling[f, here, cols] - middle) * weight[pl.ds(top + WINDOW, WINDOW), cols]
            out[f, here, cols] = deviate * factor

    def roll_only(u, low, size):
        @pl.loop(low, low + size, unroll=min(UNROLL, size))
        def chunk(c):
            cols = chunk_columns(c)
            rolled[u, :, cols] = window_means(own + u, 0, c)
            if u == 0:
                head_weight[:, cols] = weight[WINDOW:2 * WINDOW, cols]

    def main_items(g):
        size = groups[g][1]
        return pl.loop(jnp.where(tm == 0, 0, size), size * blocks)

    def main_first(g):
        start, size = groups[g]
        block = x.at[pl.ds(start, size), pl.ds(WINDOW, rows), pl.ds(0, assets)]
        wait_for(block, load_sem.at[g])
        ahead = [f for f in range(start, start + size) if f > 0]

        @pl.when(has_next)
        def _():
            for f in ahead:
                pack_top(f)

        def middle():
            @pl.when(has_next)
            def _():
                for f in ahead:
                    start_halo(f)

            if g == 0 and rounds > 1:
                next_round(rounds - 2)

        @main_items(g)
        def item(i):
            roll_window(start + lax.rem(i, size), lax.div(i, size), i)
            pl.when(i == (size + size * blocks) // 2)(middle)

        reduce_items(1 + 2 * g, size * blocks)
        if g == 0:
            if rounds:
                next_round(rounds - 1)
            send(0)
        send(1 + 2 * g)

    def main_counts(g):
        size = groups[g][1]
        for i in range(size * blocks):
            b = i // size
            counts[g, i:i + 1, :] = jnp.maximum(totals[0, b:b + 1, :], 1.0)

    def main_second(g):
        start, size = groups[g]
        slot = 1 + 2 * g
        receive(slot)
        spread_items(totals[slot], counts[g], size * blocks)

        @main_items(g)
        def item(i):
            clip_scores(start + lax.rem(i, size), lax.div(i, size), i)

        reduce_items(slot + 1, size * blocks)
        send(slot + 1)

    def main_third(g):
        start, size = groups[g]
        slot = 2 + 2 * g
        receive(slot)
        spread_items(totals[slot], counts[g], size * blocks)

        @main_items(g)
        def item(i):
            finish(start + lax.rem(i, size), lax.div(i, size), i)

    def tail_own(u):
        unpack_top(u)
        for copy, low, size in landing[u]:
            copy.wait_recv()
            roll_window(u, 0, stats + 2 * u, low, size)

    def tail_help(u):
        for copy, low, size in returning[own + u]:
            copy.wait_recv()
            roll_window(own + u, blocks, stats + 2 * u + 1, low, size)

    def tail_first(u):
        pl.when(has_prev & odd)(functools.partial(tail_own, u))
        if u < helped:
            pl.when(has_next)(functools.partial(tail_help, u))
        pl.when(has_prev & ~odd)(functools.partial(tail_own, u))

    def tail_second(u):
        @pl.when(has_prev)
        def _():
            clip_scores(u, 0, stats + 2 * u)

        if u < helped:
            @pl.when(has_next)
            def _():
                clip_scores(own + u, blocks, stats + 2 * u + 1)

    def tail_exchange(u):
        reduce_items(tail + 2 * u, 2, stats + 2 * u)
        send(tail + 2 * u)

    def tail_scores(u):
        slot = tail + 2 * u
        receive(slot)
        spread_items(totals[slot], counts[last], 2, stats + 2 * u)
        tail_second(u)
        reduce_items(slot + 1, 2, stats + 2 * u)
        send(slot + 1)

    def tail_last(u):
        slot = tail + 2 * u
        receive(slot + 1)
        if u < helped:
            advice[u, :1, :] = totals[slot, 1:2, :]
            advice[u, 1:2, :] = totals[slot + 1, 1:2, :]

            @pl.when(has_next)
            def _():
                advising[u].start()

        @pl.when(has_prev)
        def _():
            spread_items(totals[slot + 1], counts[last], 1, stats + 2 * u)
            finish(u, 0, stats + 2 * u)

    def last_rolls(u):
        unpack_top(own + u)
        for copy, low, size in landing[own + u]:
            copy.wait_recv()
            roll_only(u, low, size)

    late = own - 1
    for g in range(len(groups)):
        main_first(g)
    for u in range(late):
        tail_first(u)
        tail_exchange(u)

    @pl.when(tm == 0)
    def _():
        tail_first(late)
        tail_exchange(late)

    receive(0)
    for i in range(2):
        b = 0 if i == 0 else blocks
        counts[last, i:i + 1, :] = jnp.maximum(totals[0, b:b + 1, :], 1.0)
    main_counts(0)
    main_second(0)

    @pl.when(has_prev)
    def _():
        tail_first(late)
        tail_exchange(late)

    for g in range(1, len(groups)):
        main_counts(g)
        main_second(g)
    for u in range(late):
        tail_scores(u)

    @pl.when(tm == 0)
    def _():
        tail_scores(late)

    for g in range(len(groups) - 1):
        main_third(g)

    @pl.when(has_prev)
    def _():
        tail_scores(late)

    @pl.when(has_prev)
    def _():
        main_third(len(groups) - 1)

    for u in range(late):
        tail_last(u)

    @pl.when(has_prev)
    def _():
        for u in range(helped - 1):
            last_rolls(u)

    tail_last(late)

    @pl.when(tm == 0)
    def _():
        main_third(len(groups) - 1)

    @pl.when(has_prev)
    def _():
        for u in range(helped - 1, helped):
            last_rolls(u)
        head_count[...] = jnp.broadcast_to(counts[last, :1, :], head_count.shape)
        wait_for(advised.at[pl.ds(0, helped)], sent_sem.at[3])

    head_rows = pl.ds(0, WINDOW)

    @pl.when(has_prev)
    def _():
        wait_for(x.at[pl.ds(own, helped), head_rows, pl.ds(0, assets)], sent_sem.at[1])

    @pl.when(has_next)
    def _():
        wait_for(x.at[0, head_rows, pl.ds(0, assets)], sent_sem.at[0])
        if fields > 1:
            later_rows = pl.ds(SUBLANES, WINDOW - SUBLANES)
            wait_for(x.at[pl.ds(1, fields - 1), later_rows, pl.ds(0, assets)], sent_sem.at[6])
            wait_for(packed, sent_sem.at[7])
        wait_for(advice.at[pl.ds(0, helped)], sent_sem.at[2])

    wait_for(got.at[pl.ds(0, tail)], sent_sem.at[4])
    wait_for(got.at[pl.ds(tail, 2 * own), :, pl.ds(0, 2)], sent_sem.at[5])


def finisher(
    own, out, rolled, head_weight, advised, head_count, result, head, columns_of, sem,
):
    fields, rows, assets = out.shape
    helped = fields - own
    below = pl.ds(WINDOW, rows - WINDOW)
    tm = lax.axis_index("tm")
    copies = [
        pltpu.make_async_copy(out.at[f, below], result.at[f, below], sem)
        for f in range(fields)
    ]
    done = [
        pltpu.make_async_copy(out.at[f, :WINDOW], result.at[f, :WINDOW], sem)
        for f in range(fields)
    ]
    finished = [
        pltpu.make_async_copy(head.at[u], result.at[own + u, :WINDOW], sem)
        for u in range(helped)
    ]
    whole = [pltpu.make_async_copy(out.at[f], result.at[f], sem) for f in range(own)]
    for copy in whole + copies[own:]:
        copy.start()

    @pl.when(tm == 0)
    def _():
        for copy in done[own:]:
            copy.start()

    @pl.when(tm > 0)
    def _():
        for u in range(helped):
            spread(columns_of, advised[u], head_count[...], 2, 2 * u)
        for u in range(helped):
            center, scale = columns_of[2 * u, :WINDOW, :], columns_of[2 * u, WINDOW:, :]
            middle, factor = columns_of[2 * u + 1, :WINDOW, :], columns_of[2 * u + 1, WINDOW:, :]

            @pl.loop(0, assets // LANES, unroll=UNROLL)
            def chunk(c):
                cols = chunk_columns(c)
                scored = (rolled[u, :, cols] - center) * scale
                clipped = jnp.minimum(jnp.maximum(scored, -CLIP), CLIP)
                head[u, :, cols] = (clipped - middle) * head_weight[:, cols] * factor

            finished[u].start()

    pltpu.make_async_copy(out, out, sem).wait()


def per_device(n_tm, n_as, values, listed_from, listed_until):
    fields, rows, assets = values.shape
    blocks = rows // WINDOW
    groups = field_groups(fields)
    own = groups[0][1]
    stats = -(-max(own * blocks, blocks + 2) // SUBLANES) * SUBLANES
    slots = 1 + 2 * len(groups) + 2 * own
    cuts = len(halo_pieces(fields, own, assets // LANES))
    back_cuts = max(len(back_pieces(fields, own, assets // LANES)), 1)
    f32 = jnp.float32
    vmem = pltpu.VMEM
    dma = pltpu.SemaphoreType.DMA
    helped = max(fields - own, 1)
    chunks = assets // LANES
    kept = chunks - (chunks // SUBLANES if chunks % SUBLANES == 0 else 0)
    parts = (
        vmem((fields, rows, assets), f32),
        vmem((helped, WINDOW, assets + LANES), f32),
        vmem((WINDOW, assets + LANES), f32),
        vmem((own, SUBLANES, LANES), f32),
        vmem((SUBLANES, LANES), f32),
    )
    in_vmem = [pl.BlockSpec(memory_space=vmem)] * len(parts)
    outputs = pl.pallas_call(
        functools.partial(kernel, n_tm, n_as),
        out_shape=parts,
        in_specs=[pl.BlockSpec(memory_space=pltpu.HBM)] * 3,
        out_specs=in_vmem,
        scratch_shapes=[
            vmem((fields, WINDOW + rows + WINDOW, assets + LANES), f32),
            vmem((fields, rows + WINDOW, assets + LANES), f32),
            vmem((WINDOW + rows + WINDOW, assets + LANES), f32),
            vmem((WINDOW + rows + WINDOW, assets + LANES), f32),
            vmem((1, assets), jnp.int32),
            vmem((1, assets), jnp.int32),
            vmem((stats + 2 * own, LANES, LANES), f32),
            vmem((stats + 2 * own, LANES, LANES), f32),
            vmem((max(fields - 1, 1), SUBLANES, kept * LANES), f32),
            vmem((slots, stats, LANES), f32),
            vmem((slots, n_as - 1, stats, LANES), f32),
            vmem((slots, stats, LANES), f32),
            vmem((len(groups) + 1, stats, LANES), f32),
            vmem((own, SUBLANES, LANES), f32),
            dma((len(groups) + 2,)),
            dma((8,)),
            dma((cuts,)),
            dma((max(fields - 1, 1),)),
            dma((back_cuts,)),
            dma((slots,)),
            pltpu.SemaphoreType.REGULAR((max(greeting_rounds(n_as), 1),)),
        ],
        compiler_params=pltpu.CompilerParams(
            collective_id=0, has_side_effects=True, vmem_limit_bytes=48 * 2**20
        ),
    )(values, listed_from[None], listed_until[None])
    return pl.pallas_call(
        functools.partial(finisher, own),
        out_shape=jax.ShapeDtypeStruct((fields, rows, assets), f32),
        in_specs=in_vmem,
        out_specs=pl.BlockSpec(memory_space=pltpu.HBM),
        scratch_shapes=[
            vmem((helped, WINDOW, assets), f32),
            vmem((2 * own, LANES, LANES), f32),
            dma(()),
        ],
        compiler_params=pltpu.CompilerParams(vmem_limit_bytes=4 * 2**20),
    )(*outputs)


def solution(mesh):
    in_specs = (P(None, "tm", "asset"), P("asset"), P("asset"))
    out_specs = P(None, "tm", "asset")
    body = functools.partial(per_device, mesh.shape["tm"], mesh.shape["asset"])
    return jax.shard_map(
        body, mesh=mesh, in_specs=in_specs, out_specs=out_specs, check_vma=False
    )
```
